32 devices in a mesh: seq: 8 (over z, core), tp: 4 (over y, x).
Axes of the slice: x: 2, y: 2, z: 4, core: 2. Of those that a mesh axis runs over, the one named last changes fastest.
Arguments:
- hidden: bfloat16 [4096, 2048], P(('seq', 'tp')), may hold values from -5 to 5
- w_qkv: bfloat16 [2048, 3, 2048], P(None, None, 'tp'), may hold values from -0.125 to 0.125
- w_gate: bfloat16 [2048, 2048], P(None, 'tp'), may hold values from -0.125 to 0.125
- w_decay_beta: bfloat16 [2048, 2, 16], P(None, None, 'tp'), may hold values from -0.7 to 0.7
- conv_weight: bfloat16 [4, 3, 2048], P(None, None, 'tp'), may hold values from -2 to 2
- decay_rate: float32 [16], P('tp'), may hold values from 2e-05 to 0.05
- dt_bias: float32 [16], P('tp'), may hold values from -1 to 1
- norm_gain: float32 [128], replicated, may hold values from 0.1 to 1.9
Outputs:
- core: bfloat16 [4096, 2048], P('seq', 'tp')
The draws below stay inside these ranges and needn't reach their ends.
All inputs are finite; a program needn't handle non-finite values.
Results may differ from the reference program's by a relative error of at most 0.01.
Values may be sent and summed in bfloat16 or wider, within the bound.
No kernel may reach another device: no remote copies, remote signals or barrier semaphores. Data moves between devices by JAX's collectives and lax.ppermute only.
A program may use at most 64 MiB of HBM per device.

```python
import math
import jax
import jax.numpy as jnp
from jax import lax

D = 2048
H = 16
DH = 128
KERNEL = 4
SEQ = 4096


def direction_signs(key):
    return jax.random.rademacher(jax.random.fold_in(key, 71), (D,), dtype=jnp.float32)


def slow_heads(key):
    order = jax.random.permutation(jax.random.fold_in(key, 72), H)
    count = 3 * H // 8
    return (order < count).astype(jnp.float32)


def draw_hidden(key, part):
    signs = direction_signs(key)
    noise_key = jax.random.fold_in(key, 73)
    noise = 0.9 * jax.random.truncated_normal(noise_key, -5.0, 5.0, (SEQ, D), jnp.float32)
    offset = 0.4
    return (noise + offset * signs[None, :]).astype(jnp.bfloat16)


def draw_w_decay_beta(key, part):
    signs = direction_signs(key)
    slow = slow_heads(key)
    base = jax.random.truncated_normal(jax.random.fold_in(key, 74), -5.0, 5.0, (D, 2, H), jnp.float32)
    base = base * (1.0 / math.sqrt(D))
    strength = jax.random.uniform(jax.random.fold_in(key, 75), (H,), jnp.float32, 10.0, 13.0)
    slow_column = -strength[None, :] * signs[:, None] * (1.0 / D) + 0.3 * base[:, 1, :]
    beta_column = slow[None, :] * slow_column + (1.0 - slow[None, :]) * base[:, 1, :]
    return jnp.stack([base[:, 0, :], beta_column], axis=1).astype(jnp.bfloat16)


def draw_decay_rate(key, part):
    slow = slow_heads(key)
    fraction = jax.random.uniform(jax.random.fold_in(key, 76), (H,), jnp.float32, 0.0, 1.0)
    slow_rate = jnp.exp(math.log(2e-05) + fraction * (math.log(0.00015) - math.log(2e-05)))
    fast_rate = jnp.exp(math.log(0.002) + fraction * (math.log(0.05) - math.log(0.002)))
    return jnp.where(slow > 0.5, slow_rate, fast_rate).astype(jnp.float32)


def levels(own_key, dims, shards, low, high):
    level = 1.0
    for axis_at, shards_of in shards:
        draws = jax.random.uniform(jax.random.fold_in(jax.random.fold_in(own_key, 6), axis_at), (shards_of,), jnp.float32, low / len(shards), high / len(shards))
        level = level * jnp.repeat(jnp.exp(draws), dims[axis_at] // shards_of).reshape((-1,) + (1,) * (len(dims) - 1 - axis_at))
    return level


def scatter_about(stream_key, extent, deviation, limit, shards=(), held_as=jnp.bfloat16):
    loudness = levels(stream_key, extent, shards, -0.22, 0.18) if shards else 1.0
    entries = jax.random.normal(stream_key, extent, jnp.float32) * deviation * loudness
    return jnp.minimum(jnp.maximum(entries, -limit), limit).astype(held_as)


def setup_inputs(seed: int = 0) -> dict:
    arg_keys = jax.random.split(jax.random.key(seed), 9)
    return {
        "hidden": draw_hidden(jax.random.fold_in(arg_keys[8], 71), 0),
        "w_qkv": scatter_about(arg_keys[1], (D, 3, H * DH), D ** -0.5, 0.125, ((2, 4),)),
        "w_gate": scatter_about(arg_keys[2], (D, H * DH), D ** -0.5, 0.125, ((1, 4),)),
        "w_decay_beta": draw_w_decay_beta(jax.random.fold_in(arg_keys[8], 71), 0),
        "conv_weight": scatter_about(arg_keys[4], (KERNEL, 3, H * DH), 0.5, 2.0, ((2, 4),)),
        "decay_rate": draw_decay_rate(jax.random.fold_in(arg_keys[8], 71), 0),
        "dt_bias": jnp.clip(jax.random.uniform(arg_keys[6], (H,), jnp.float32, -1.0, 1.0) * levels(arg_keys[6], (H,), ((0, 4),), -0.4, 0.0), -1.0, 1.0),
        "norm_gain": jnp.clip(1.0 + 0.18 * jax.random.normal(arg_keys[7], (DH,), jnp.float32), 0.1, 1.9),
    }


def unit_rows(matrix):
    return matrix * lax.rsqrt(lax.optimization_barrier(jnp.sum(matrix * matrix, axis=-1, keepdims=True)) + 1e-06)

def reference(hidden, w_qkv, w_gate, w_decay_beta, conv_weight, decay_rate, dt_bias, norm_gain):
    seq_total = hidden.shape[0]
    columns = H * DH
    projected = jnp.dot(hidden, w_qkv.reshape(D, 3 * columns), preferred_element_type=jnp.float32)
    projected = projected.astype(jnp.bfloat16).reshape(seq_total, 3, columns)
    padded = jnp.concatenate([jnp.zeros((KERNEL - 1, 3, columns), jnp.bfloat16), projected], axis=0)
    convolved = jnp.zeros((seq_total, 3, columns), jnp.float32)
    for offset in range(KERNEL):
        convolved = convolved + padded[offset:offset + seq_total].astype(jnp.float32) * conv_weight[offset].astype(jnp.float32)
    activated = jax.nn.silu(convolved).astype(jnp.bfloat16)
    scalars = jnp.dot(hidden, w_decay_beta.reshape(D, 2 * H), preferred_element_type=jnp.float32).reshape(seq_total, 2, H)
    log_decay = -decay_rate * jax.nn.softplus(scalars[:, 0] + dt_bias)
    write_rate = jax.nn.sigmoid(scalars[:, 1])
    branches = activated.astype(jnp.float32).reshape(seq_total, 3, H, DH)
    inv_root = 1.0 / math.sqrt(DH)
    queries = unit_rows(branches[:, 0]) * inv_root
    keys_in = unit_rows(branches[:, 1])
    values_in = branches[:, 2]

    def advance(state_history, inputs):
        single_query, single_key, value_row, decay_row, rate_row = inputs
        state_history = jnp.exp(decay_row)[:, None, None] * state_history
        retrieved_value = jnp.einsum('cd,cdn->cn', single_key, state_history, precision=lax.Precision.HIGHEST)
        state_history = state_history + rate_row[:, None, None] * single_key[:, :, None] * (value_row - retrieved_value)[:, None, :]
        return (state_history, jnp.einsum('cd,cdn->cn', single_query, state_history, precision=lax.Precision.HIGHEST))
    start_state = jnp.zeros((H, DH, DH), jnp.float32)
    _, state_output = lax.scan(advance, start_state, (queries, keys_in, values_in, log_decay, write_rate))
    gate_linear = jnp.dot(hidden, w_gate, preferred_element_type=jnp.float32).reshape(seq_total, H, DH)
    rms_scale = lax.rsqrt(lax.optimization_barrier(jnp.mean(state_output * state_output, axis=-1, keepdims=True)) + 1e-06)
    core = state_output * rms_scale * norm_gain * jax.nn.silu(gate_linear)
    return core.reshape(seq_total, columns).astype(jnp.bfloat16)
```

```python
import functools
import math

import jax
import jax.numpy as jnp
from jax import lax
from jax.experimental import pallas as pl
from jax.experimental.pallas import tpu as pltpu
from jax.sharding import PartitionSpec as P

CHUNK = 128
LANES = 128
RIM = 8
EPS = 1e-6

f32 = jnp.float32
bf16 = jnp.bfloat16


def dot(left, right, contract=(1, 0), precision=None):
    dims = (((contract[0],), (contract[1],)), ((), ()))
    return lax.dot_general(left, right, dims, precision=precision, preferred_element_type=f32)


def whole(memory=pltpu.VMEM):
    return pl.BlockSpec(memory_space=memory)


def gather_blocks(block, axis):
    count = lax.axis_size(axis)
    bits = count.bit_length() - 1
    rows = block.shape[0]
    half = rows // 2

    def swap(value, bit):
        step = 1 << bit
        return lax.ppermute(value, axis, [(i, i ^ step) for i in range(count)])

    parts = [{0: block[:half]}, {0: block[half:]}]
    found = {0: block}
    for bit in range(bits):
        found[1 << bit] = swap(block, bit)
        parts[0][1 << bit] = found[1 << bit][:half]
        parts[1][1 << bit] = found[1 << bit][half:]
    for order, part in ((range(bits), parts[0]), (range(bits - 1, -1, -1), parts[1])):
        for bit in order:
            for mask in list(part):
                if mask | (1 << bit) not in part and not mask & (1 << bit):
                    part[mask | (1 << bit)] = swap(part[mask], bit)
    return [
        found[m] if m in found else jnp.concatenate([parts[0][m], parts[1][m]])
        for m in range(count)
    ]


def silu(x):
    return x / (1.0 + jnp.exp(-x))


def delta_kernel(
    heads, blocks, me_ref, p_ref, rim_ref, taps_ref, sc_ref, vec_ref,
    x_ref, qp_ref, o_ref, xp, act, sc, cols, masks,
):
    seq_rows, width = p_ref.shape
    columns = width // 3
    rows = seq_rows // blocks
    chunks = seq_rows // CHUNK
    taps = taps_ref.shape[0]
    me = me_ref[0]

    xp[:RIM] = rim_ref[...].astype(f32)
    for m in range(blocks):
        at = lax.bitwise_xor(me, m) * rows
        xp[pl.ds(pl.multiple_of(RIM + at, 8), rows)] = p_ref[m * rows:(m + 1) * rows].astype(f32)
        sc[pl.ds(pl.multiple_of(at, 8), rows)] = sc_ref[m * rows:(m + 1) * rows]

    ri = lax.broadcasted_iota(jnp.int32, (CHUNK, CHUNK), 0)
    ci = lax.broadcasted_iota(jnp.int32, (CHUNK, CHUNK), 1)
    strict = ri > ci
    upto = ri >= ci
    lower = upto.astype(f32)
    levels = CHUNK.bit_length() - 1
    for level in range(levels):
        hit = ((ri >> (level + 1)) == (ci >> (level + 1))) & ((ri >> level) > (ci >> level))
        masks[level] = hit.astype(f32).astype(bf16)

    root = 1.0 / math.sqrt(columns // heads)
    for chunk in range(chunks):
        base = chunk * CHUNK
        raw = sc[base:base + CHUNK]
        shifted = raw + vec_ref[1:2]
        soft = jnp.maximum(shifted, 0.0) + jnp.log1p(jnp.exp(-jnp.abs(shifted)))
        decay = dot(lower, vec_ref[0:1] * soft, precision=lax.Precision.HIGHEST)
        beta = 1.0 / (1.0 + jnp.exp(-raw))
        comb = jnp.where(ci < heads, decay, 0.0)
        for head in range(heads):
            norms = []
            for branch in range(3):
                lane = branch * columns + head * LANES
                total = None
                for i in range(taps):
                    start = RIM - taps + 1 + base + i
                    term = xp[start:start + CHUNK, lane:lane + LANES] * taps_ref[i:i + 1, lane:lane + LANES]
                    total = term if total is None else total + term
                value = silu(total).astype(bf16)
                act[branch, head, base:base + CHUNK] = value
                if branch < 2:
                    wide = value.astype(f32)
                    norms.append(lax.rsqrt(jnp.sum(wide * wide, axis=-1, keepdims=True) + EPS))
            scaled = beta[:, heads + head:heads + head + 1] * norms[1]
            comb = jnp.where(ci == heads + head, scaled, comb)
            comb = jnp.where(ci == 2 * heads + head, norms[0] * root, comb)
            comb = jnp.where(ci == 3 * heads + head, norms[1], comb)
        cols[chunk] = comb

    pairs = [(head, chunk) for head in range(heads) for chunk in range(chunks)]
    for head in range(heads):
        todo = list(range(chunks))
        turned = {}
        state = {}
        for chunk in todo:
            at = slice(chunk * CHUNK, (chunk + 1) * CHUNK)
            col = cols[chunk]
            row = col.T
            k = act[1, head, at]
            q = act[0, head, at]
            gap = col[:, head:head + 1] - row[head:head + 1]
            weight = jnp.exp(jnp.where(upto, gap, 0.0)) * row[heads + head:heads + head + 1]
            gram = dot(k, k, (1, 1))
            score = dot(q, k, (1, 1))
            key_norm = col[:, 3 * heads + head:3 * heads + head + 1]
            mix = (weight * gram * key_norm).astype(bf16)
            attend = jnp.where(upto, weight * score * col[:, 2 * heads + head:2 * heads + head + 1], 0.0)
            x = jnp.where(ri == ci, 1.0, 0.0) - (mix * masks[0]).astype(f32)
            state[chunk] = [mix, x, attend.astype(bf16), col, row]
        for level in range(1, levels):
            low = {c: state[c][1].astype(bf16) for c in todo}
            mid = {c: dot(state[c][0] * masks[level], low[c]).astype(bf16) for c in todo}
            for c in todo:
                state[c][1] = state[c][1] - dot(low[c], mid[c])
        p_run, r_run = None, None
        for chunk in todo:
            mix, x, attend, col, row = state[chunk]
            at = slice(chunk * CHUNK, (chunk + 1) * CHUNK)
            k, q, v = act[1, head, at], act[0, head, at], act[2, head, at]
            decay = col[:, head:head + 1]
            last = col[CHUNK - 1:CHUNK, head:head + 1]
            key_norm_row = row[3 * heads + head:3 * heads + head + 1]
            grown = jnp.exp(row[head:head + 1]) * key_norm_row
            new = dot(x.astype(bf16), v)
            back = dot((x * grown).astype(bf16), k)
            tail = col[:, heads + head:heads + head + 1] * jnp.exp(last - decay)
            both = jnp.concatenate([back, new], axis=1)
            change = dot(k, (both * tail).astype(bf16), (0, 0))
            inner = dot(attend, both.astype(bf16))
            eff = (jnp.exp(decay) * col[:, 2 * heads + head:2 * heads + head + 1]) * q.astype(f32) - inner[:, :LANES]
            if chunk == 0:
                qp_ref[head, at] = eff.astype(bf16)
                o_ref[head, at] = inner[:, LANES:]
                p_run = jnp.where(ri == ci, jnp.exp(last), 0.0) - change[:, :LANES]
                r_run = change[:, LANES:]
            else:
                run = jnp.concatenate([p_run, r_run], axis=1)
                low_run = run.astype(bf16)
                ahead = dot(eff.astype(bf16), low_run)
                qp_ref[head, at] = ahead[:, :LANES].astype(bf16)
                o_ref[head, at] = inner[:, LANES:] + ahead[:, LANES:]
                run = jnp.exp(last) * run - dot(change[:, :LANES].astype(bf16), low_run)
                p_run = run[:, :LANES]
                r_run = run[:, LANES:] + change[:, LANES:]
        x_ref[head] = jnp.concatenate([p_run, r_run], axis=1).astype(bf16)


def join_kernel(mine_ref, earlier_ref, out_ref):
    for head in range(mine_ref.shape[0]):
        mine = mine_ref[head]
        both = dot(mine[:, :LANES], earlier_ref[head])
        out_ref[head, :, :LANES] = both[:, :LANES].astype(bf16)
        out_ref[head, :, LANES:] = (both[:, LANES:] + mine[:, LANES:].astype(f32)).astype(bf16)


def final_kernel(blocks, me_ref, qp_ref, o_ref, near_ref, far_ref, gate_ref, gain_ref, out_ref):
    heads, seq_rows, dim = qp_ref.shape
    rows = seq_rows // blocks
    me = me_ref[0]
    for head in range(heads):
        near = near_ref[head]
        start = near[:, dim:].astype(f32) + dot(near[:, :dim], far_ref[head])
        start = start.astype(bf16)
        lanes = slice(head * dim, (head + 1) * dim)
        for m in range(blocks):
            at = pl.multiple_of(lax.bitwise_xor(me, m) * rows, 8)
            y = o_ref[head, pl.ds(at, rows)] + dot(qp_ref[head, pl.ds(at, rows)], start)
            scale = lax.rsqrt(jnp.mean(y * y, axis=-1, keepdims=True) + EPS)
            gate = gate_ref[m * rows:(m + 1) * rows, lanes]
            y = y * scale * gain_ref[...] * silu(gate)
            out_ref[pl.ds(at, rows), lanes] = y.astype(bf16)


def shifted(value, axis, distance):
    count = lax.axis_size(axis)
    return lax.ppermute(value, axis, [(i, i + distance) for i in range(count - distance)])


def per_device(hidden, w_qkv, w_gate, w_decay_beta, conv_weight, decay_rate, dt_bias, norm_gain):
    model_width = hidden.shape[1]
    heads = decay_rate.shape[0]
    dim = norm_gain.shape[0]
    columns = heads * dim
    blocks = lax.axis_size("tp")
    seq_count = lax.axis_size("seq")
    me = lax.axis_index("tp")
    index = jnp.full((1,), me, jnp.int32)
    qkv_matrix = w_qkv.reshape(model_width, 3 * columns)
    small = jnp.pad(
        w_decay_beta.reshape(model_width, 2 * heads), ((0, 0), (0, LANES - 2 * heads))
    )
    tokens = jnp.concatenate(gather_blocks(hidden, "tp"), axis=0)
    rows = hidden.shape[0]
    seq_rows = tokens.shape[0]
    projected = jnp.dot(tokens, qkv_matrix, preferred_element_type=f32).astype(bf16)
    last = lax.bitwise_xor(me, blocks - 1)
    rim = lax.dynamic_slice(projected, (last * rows + rows - RIM, 0), (RIM, 3 * columns))
    rim = shifted(rim, "seq", 1)
    scalars = jnp.dot(tokens, small, preferred_element_type=f32)
    gate = jnp.dot(tokens, w_gate, preferred_element_type=f32)
    taps = conv_weight.reshape(conv_weight.shape[0], 3 * columns).astype(f32)
    vectors = jnp.pad(jnp.stack([-decay_rate, dt_bias]), ((0, 6), (0, LANES - heads)))
    chunks = seq_rows // CHUNK
    cost = functools.partial(pl.CostEstimate, transcendentals=0, bytes_accessed=4 << 20)
    own, reach, base = pl.pallas_call(
        functools.partial(delta_kernel, heads, blocks),
        out_shape=(
            jax.ShapeDtypeStruct((heads, dim, 2 * dim), bf16),
            jax.ShapeDtypeStruct((heads, seq_rows, dim), bf16),
            jax.ShapeDtypeStruct((heads, seq_rows, dim), f32),
        ),
        in_specs=[whole(pltpu.SMEM)] + [whole()] * 5,
        out_specs=(whole(),) * 3,
        scratch_shapes=[
            pltpu.VMEM((seq_rows + RIM, 3 * columns), f32),
            pltpu.VMEM((3, heads, seq_rows, dim), bf16),
            pltpu.VMEM((seq_rows, LANES), f32),
            pltpu.VMEM((chunks, CHUNK, LANES), f32),
            pltpu.VMEM((CHUNK.bit_length() - 1, CHUNK, CHUNK), bf16),
        ],
        cost_estimate=cost(flops=2000000000),
        name="delta",
    )(index, projected, rim, taps, scalars, vectors)

    def join(mine, earlier):
        return pl.pallas_call(
            join_kernel,
            out_shape=jax.ShapeDtypeStruct(mine.shape, bf16),
            in_specs=[whole()] * 2,
            out_specs=whole(),
            cost_estimate=cost(flops=50000000),
            name="join",
        )(mine, earlier)

    run = own
    distance = 1
    while distance * 2 < seq_count:
        run = join(run, shifted(run, "seq", distance))
        distance *= 2
    near = shifted(run, "seq", 1)
    far = shifted(run[:, :, dim:], "seq", distance + 1)
    return pl.pallas_call(
        functools.partial(final_kernel, blocks),
        out_shape=jax.ShapeDtypeStruct((seq_rows, columns), bf16),
        in_specs=[whole(pltpu.SMEM)] + [whole()] * 6,
        out_specs=whole(),
        cost_estimate=cost(flops=200000000),
        name="final",
    )(index, reach, base, near, far, gate, norm_gain.reshape(1, dim))


def solution(mesh):
    return jax.shard_map(
        per_device,
        mesh=mesh,
        in_specs=(
            P(("seq", "tp"), None),
            P(None, None, "tp"),
            P(None, "tp"),
            P(None, None, "tp"),
            P(None, None, "tp"),
            P("tp"),
            P("tp"),
            P(),
        ),
        out_specs=P("seq", "tp"),
        check_vma=False,
    )
```

```python
import functools
import math

import jax
import jax.numpy as jnp
from jax import lax
from jax.experimental import pallas as pl
from jax.experimental.pallas import tpu as pltpu
from jax.sharding import PartitionSpec as P

CHUNK = 128
LANES = 128
RIM = 8
EPS = 1e-6

f32 = jnp.float32
bf16 = jnp.bfloat16


def dot(left, right, contract=(1, 0), precision=None):
    dims = (((contract[0],), (contract[1],)), ((), ()))
    return lax.dot_general(left, right, dims, precision=precision, preferred_element_type=f32)


def whole(memory=pltpu.VMEM):
    return pl.BlockSpec(memory_space=memory)


def gather_blocks(block, axis):
    count = lax.axis_size(axis)
    bits = count.bit_length() - 1
    rows = block.shape[0]
    half = rows // 2

    def swap(value, bit):
        step = 1 << bit
        return lax.ppermute(value, axis, [(i, i ^ step) for i in range(count)])

    parts = [{0: block[:half]}, {0: block[half:]}]
    found = {0: block}
    for bit in range(bits):
        found[1 << bit] = swap(block, bit)
        parts[0][1 << bit] = found[1 << bit][:half]
        parts[1][1 << bit] = found[1 << bit][half:]
    for order, part in ((range(bits), parts[0]), (range(bits - 1, -1, -1), parts[1])):
        for bit in order:
            for mask in list(part):
                if mask | (1 << bit) not in part and not mask & (1 << bit):
                    part[mask | (1 << bit)] = swap(part[mask], bit)
    return [
        found[m] if m in found else jnp.concatenate([parts[0][m], parts[1][m]])
        for m in range(count)
    ]


def silu(x):
    return x / (1.0 + jnp.exp(-x))


def block_diagonal(left, right):
    hole = jnp.zeros_like(left)
    return jnp.concatenate(
        [jnp.concatenate([left, hole], axis=1), jnp.concatenate([hole, right], axis=1)], axis=0
    )


def beside(left, right):
    return jnp.concatenate([left, right], axis=1)


def delta_kernel(
    heads, blocks, me_ref, p_ref, rim_ref, taps_ref, sc_ref, vec_ref,
    x_ref, qp_ref, o_ref, xp, act, sc, cols, rows_of, masks, mixes, solves, attends,
):
    seq_rows, width = p_ref.shape
    tiles = width // LANES
    rows = seq_rows // blocks
    chunks = seq_rows // CHUNK
    taps = taps_ref.shape[1]
    me = me_ref[0]

    for tile in range(tiles):
        lanes = slice(tile * LANES, (tile + 1) * LANES)
        xp[tile, :RIM] = rim_ref[:, lanes].astype(f32)
        for m in range(blocks):
            at = pl.multiple_of(RIM + lax.bitwise_xor(me, m) * rows, 8)
            xp[tile, pl.ds(at, rows)] = p_ref[m * rows:(m + 1) * rows, lanes].astype(f32)
    for m in range(blocks):
        at = pl.multiple_of(lax.bitwise_xor(me, m) * rows, 8)
        sc[pl.ds(at, rows)] = sc_ref[m * rows:(m + 1) * rows]

    ri = lax.broadcasted_iota(jnp.int32, (CHUNK, CHUNK), 0)
    ci = lax.broadcasted_iota(jnp.int32, (CHUNK, CHUNK), 1)
    upto = ri >= ci
    lower = upto.astype(f32)
    levels = CHUNK.bit_length() - 1
    for level in range(levels):
        hit = ((ri >> (level + 1)) == (ci >> (level + 1))) & ((ri >> level) > (ci >> level))
        hit = hit.astype(f32).astype(bf16)
        masks[level] = beside(hit, hit)

    root = 1.0 / math.sqrt(LANES)

    def prepare(chunk, carry):
        base = pl.multiple_of(chunk * CHUNK, CHUNK)
        raw = sc[pl.ds(base, CHUNK)]
        shifted = raw + vec_ref[1:2]
        soft = jnp.maximum(shifted, 0.0) + jnp.log1p(jnp.exp(-jnp.abs(shifted)))
        decay = dot(lower, vec_ref[0:1] * soft, precision=lax.Precision.HIGHEST)
        beta = 1.0 / (1.0 + jnp.exp(-raw))
        comb = jnp.where(ci < heads, decay, 0.0)
        for head in range(heads):
            norms = []
            for branch in range(3):
                tile = branch * heads + head
                total = None
                for i in range(taps):
                    term = xp[tile, pl.ds(base + (RIM - taps + 1 + i), CHUNK)] * taps_ref[tile, i:i + 1]
                    total = term if total is None else total + term
                value = silu(total).astype(bf16)
                act[tile, pl.ds(base, CHUNK)] = value
                if branch < 2:
                    wide = value.astype(f32)
                    norms.append(lax.rsqrt(jnp.sum(wide * wide, axis=-1, keepdims=True) + EPS))
            scaled = beta[:, heads + head:heads + head + 1] * norms[1]
            comb = jnp.where(ci == heads + head, scaled, comb)
            comb = jnp.where(ci == 2 * heads + head, norms[0] * root, comb)
            comb = jnp.where(ci == 3 * heads + head, norms[1], comb)
        cols[chunk] = comb
        rows_of[chunk] = comb.T
        return carry

    lax.fori_loop(0, chunks, prepare, 0)

    def part(branch, head, chunk):
        return act[branch * heads + head, chunk * CHUNK:(chunk + 1) * CHUNK]

    def col(kind, head, chunk):
        lane = kind * heads + head
        return cols[chunk, :, lane:lane + 1]

    def row(kind, head, chunk):
        lane = kind * heads + head
        return rows_of[chunk, lane:lane + 1, :]

    sets = [(head, chunk) for head in range(heads) for chunk in range(0, chunks, 2)]
    for s, (head, first) in enumerate(sets):
        two = (first, first + 1)
        keys = [part(1, head, c) for c in two]
        turned = block_diagonal(*[k.T for k in keys])
        gram = dot(beside(*keys), turned)
        score = dot(beside(*[part(0, head, c) for c in two]), turned)
        mix, solve = [], []
        for i, c in enumerate(two):
            lanes = slice(i * LANES, (i + 1) * LANES)
            gap = col(0, head, c) - row(0, head, c)
            weight = jnp.where(upto, jnp.exp(jnp.minimum(gap, 0.0)) * row(1, head, c), 0.0)
            mix.append((weight * gram[:, lanes] * col(3, head, c)).astype(bf16))
            attends[head, c] = (weight * score[:, lanes] * col(2, head, c)).astype(bf16)
        mix = beside(*mix)
        mixes[s] = mix
        eye = jnp.where(ri == ci, 1.0, 0.0)
        solves[s] = beside(eye, eye) - (mix * masks[0]).astype(f32)
    for level in range(1, levels):
        lows, mids = [], []
        for s in range(len(sets)):
            lows.append(solves[s].astype(bf16))
            low = lows[s]
            mids.append(dot(mixes[s] * masks[level], block_diagonal(low[:, :LANES], low[:, LANES:])).astype(bf16))
        for s in range(len(sets)):
            mid = mids[s]
            solves[s] = solves[s] - dot(lows[s], block_diagonal(mid[:, :LANES], mid[:, LANES:]))
    change, inner = {}, {}
    for s, (head, first) in enumerate(sets):
        two = (first, first + 1)
        solve = solves[s]
        new = dot(solve.astype(bf16), block_diagonal(*[part(2, head, c) for c in two]))
        grown = beside(*[jnp.exp(row(0, head, c)) * row(3, head, c) for c in two])
        back = dot((solve * grown).astype(bf16), block_diagonal(*[part(1, head, c) for c in two]))
        for i, c in enumerate(two):
            lanes = slice(i * LANES, (i + 1) * LANES)
            both = beside(back[:, lanes], new[:, lanes])
            decay = col(0, head, c)
            tail = col(1, head, c) * jnp.exp(decay[CHUNK - 1:] - decay)
            change[head, c] = dot(part(1, head, c), (both * tail).astype(bf16), (0, 0))
            inner[head, c] = dot(attends[head, c], both.astype(bf16))
    runs = {}
    for c in range(chunks):
        at = slice(c * CHUNK, (c + 1) * CHUNK)
        for head in range(heads):
            decay = col(0, head, c)
            last = jnp.exp(decay[CHUNK - 1:])
            eff = (jnp.exp(decay) * col(2, head, c)) * part(0, head, c).astype(f32) - inner[head, c][:, :LANES]
            if c == 0:
                qp_ref[head, at] = eff.astype(bf16)
                o_ref[head, at] = inner[head, c][:, LANES:]
                runs[head] = beside(
                    jnp.where(ri == ci, last, 0.0) - change[head, c][:, :LANES], change[head, c][:, LANES:]
                )
            else:
                low = runs[head].astype(bf16)
                ahead = dot(eff.astype(bf16), low)
                qp_ref[head, at] = ahead[:, :LANES].astype(bf16)
                o_ref[head, at] = inner[head, c][:, LANES:] + ahead[:, LANES:]
                run = last * runs[head] - dot(change[head, c][:, :LANES].astype(bf16), low)
                runs[head] = beside(run[:, :LANES], run[:, LANES:] + change[head, c][:, LANES:])
    for head in range(heads):
        x_ref[head] = runs[head].astype(bf16)


def join_kernel(mine_ref, earlier_ref, out_ref):
    for head in range(mine_ref.shape[0]):
        mine = mine_ref[head]
        both = dot(mine[:, :LANES], earlier_ref[head])
        out_ref[head, :, :LANES] = both[:, :LANES].astype(bf16)
        out_ref[head, :, LANES:] = (both[:, LANES:] + mine[:, LANES:].astype(f32)).astype(bf16)


def final_kernel(blocks, me_ref, qp_ref, o_ref, near_ref, far_ref, gate_ref, gain_ref, out_ref):
    heads, seq_rows, dim = qp_ref.shape
    rows = seq_rows // blocks
    me = me_ref[0]
    for head in range(heads):
        near = near_ref[head]
        start = near[:, dim:].astype(f32) + dot(near[:, :dim], far_ref[head])
        start = start.astype(bf16)
        lanes = slice(head * dim, (head + 1) * dim)
        for m in range(blocks):
            at = pl.multiple_of(lax.bitwise_xor(me, m) * rows, 8)
            y = o_ref[head, pl.ds(at, rows)] + dot(qp_ref[head, pl.ds(at, rows)], start)
            scale = lax.rsqrt(jnp.mean(y * y, axis=-1, keepdims=True) + EPS)
            gate = gate_ref[m * rows:(m + 1) * rows, lanes]
            y = y * scale * gain_ref[...] * silu(gate)
            out_ref[pl.ds(at, rows), lanes] = y.astype(bf16)


def shifted(value, axis, distance):
    count = lax.axis_size(axis)
    return lax.ppermute(value, axis, [(i, i + distance) for i in range(count - distance)])


def per_device(hidden, w_qkv, w_gate, w_decay_beta, conv_weight, decay_rate, dt_bias, norm_gain):
    model_width = hidden.shape[1]
    heads = decay_rate.shape[0]
    dim = norm_gain.shape[0]
    columns = heads * dim
    blocks = lax.axis_size("tp")
    seq_count = lax.axis_size("seq")
    me = lax.axis_index("tp")
    index = jnp.full((1,), me, jnp.int32)
    qkv_matrix = w_qkv.reshape(model_width, 3 * columns)
    small = jnp.pad(
        w_decay_beta.reshape(model_width, 2 * heads), ((0, 0), (0, LANES - 2 * heads))
    )
    tokens = jnp.concatenate(gather_blocks(hidden, "tp"), axis=0)
    rows = hidden.shape[0]
    seq_rows = tokens.shape[0]
    projected = jnp.dot(tokens, qkv_matrix, preferred_element_type=f32).astype(bf16)
    last = lax.bitwise_xor(me, blocks - 1)
    rim = lax.dynamic_slice(projected, (last * rows + rows - RIM, 0), (RIM, 3 * columns))
    rim = shifted(rim, "seq", 1)
    scalars = jnp.dot(tokens, small, preferred_element_type=f32)
    gate = jnp.dot(tokens, w_gate, preferred_element_type=f32)
    count = conv_weight.shape[0]
    taps = conv_weight.reshape(count, 3 * heads, dim).transpose(1, 0, 2).astype(f32)
    vectors = jnp.pad(jnp.stack([-decay_rate, dt_bias]), ((0, 6), (0, LANES - heads)))
    chunks = seq_rows // CHUNK
    cost = functools.partial(pl.CostEstimate, transcendentals=0, bytes_accessed=4 << 20)
    own, reach, base = pl.pallas_call(
        functools.partial(delta_kernel, heads, blocks),
        out_shape=(
            jax.ShapeDtypeStruct((heads, dim, 2 * dim), bf16),
            jax.ShapeDtypeStruct((heads, seq_rows, dim), bf16),
            jax.ShapeDtypeStruct((heads, seq_rows, dim), f32),
        ),
        in_specs=[whole(pltpu.SMEM)] + [whole()] * 5,
        out_specs=(whole(),) * 3,
        scratch_shapes=[
            pltpu.VMEM((3 * heads, seq_rows + RIM, dim), f32),
            pltpu.VMEM((3 * heads, seq_rows, dim), bf16),
            pltpu.VMEM((seq_rows, LANES), f32),
            pltpu.VMEM((chunks, CHUNK, LANES), f32),
            pltpu.VMEM((chunks, CHUNK, LANES), f32),
            pltpu.VMEM((CHUNK.bit_length() - 1, CHUNK, 2 * CHUNK), bf16),
            pltpu.VMEM((heads * chunks // 2, CHUNK, 2 * CHUNK), bf16),
            pltpu.VMEM((heads * chunks // 2, CHUNK, 2 * CHUNK), f32),
            pltpu.VMEM((heads, chunks, CHUNK, CHUNK), bf16),
        ],
        cost_estimate=cost(flops=2000000000),
        name="delta",
    )(index, projected, rim, taps, scalars, vectors)

    def join(mine, earlier):
        return pl.pallas_call(
            join_kernel,
            out_shape=jax.ShapeDtypeStruct(mine.shape, bf16),
            in_specs=[whole()] * 2,
            out_specs=whole(),
            cost_estimate=cost(flops=50000000),
            name="join",
        )(mine, earlier)

    run = own
    distance = 1
    while distance * 2 < seq_count:
        run = join(run, shifted(run, "seq", distance))
        distance *= 2
    near = shifted(run, "seq", 1)
    far = shifted(run[:, :, dim:], "seq", distance + 1)
    return pl.pallas_call(
        functools.partial(final_kernel, blocks),
        out_shape=jax.ShapeDtypeStruct((seq_rows, columns), bf16),
        in_specs=[whole(pltpu.SMEM)] + [whole()] * 6,
        out_specs=whole(),
        cost_estimate=cost(flops=200000000),
        name="final",
    )(index, reach, base, near, far, gate, norm_gain.reshape(1, dim))


def solution(mesh):
    return jax.shard_map(
        per_device,
        mesh=mesh,
        in_specs=(
            P(("seq", "tp"), None),
            P(None, None, "tp"),
            P(None, "tp"),
            P(None, None, "tp"),
            P(None, None, "tp"),
            P("tp"),
            P("tp"),
            P(),
        ),
        out_specs=P("seq", "tp"),
        check_vma=False,
    )
```

```python
import functools
import math

import jax
import jax.numpy as jnp
from jax import lax
from jax.experimental import pallas as pl
from jax.experimental.pallas import tpu as pltpu
from jax.sharding import PartitionSpec as P

CHUNK = 128
LANES = 128
RIM = 16
EPS = 1e-6
PROJECT_FLOPS = 3000000000
DELTA_FLOPS = 3000000000
REACH_FLOPS = 2000000000
SMALL_FLOPS = 50000000

f32 = jnp.float32
bf16 = jnp.bfloat16


def dot(left, right, contract=(1, 0), precision=None):
    dims = (((contract[0],), (contract[1],)), ((), ()))
    return lax.dot_general(left, right, dims, precision=precision, preferred_element_type=f32)


def whole(memory=pltpu.VMEM):
    return pl.BlockSpec(memory_space=memory)


def gather_blocks(block, axis):
    count = lax.axis_size(axis)
    bits = count.bit_length() - 1
    half = block.shape[0] // 2

    def swap(value, bit):
        step = 1 << bit
        return lax.ppermute(value, axis, [(i, i ^ step) for i in range(count)])

    found = {0: block}
    for bit in range(bits):
        found[1 << bit] = swap(block, bit)
    halves = []
    for number, order in enumerate((range(bits), range(bits - 1, -1, -1))):
        part = {m: value[number * half:(number + 1) * half] for m, value in found.items()}
        for bit in order:
            for mask in list(part):
                if mask | (1 << bit) not in part:
                    part[mask | (1 << bit)] = swap(part[mask], bit)
        halves.append(part)
    early = [found[m] if m in found else (halves[0][m], halves[1][m]) for m in range(count - 1)]
    flat = []
    for item in early:
        flat.extend(item if isinstance(item, tuple) else (item,))
    return flat, [halves[0][count - 1], halves[1][count - 1]]


def rim_rows(block, count):
    seq_count, tp_count = lax.axis_size("seq"), lax.axis_size("tp")
    tail = block[-count:]
    total = None
    for j in range(tp_count):
        route = [(s * tp_count - 1, s * tp_count + j) for s in range(1, seq_count)]
        part = lax.ppermute(tail, ("seq", "tp"), route)
        total = part if total is None else total + part
    return total


def silu(x):
    return x / (1.0 + jnp.exp(-x))


def block_diagonal(left, right):
    hole = jnp.zeros_like(left)
    return jnp.concatenate(
        [jnp.concatenate([left, hole], axis=1), jnp.concatenate([hole, right], axis=1)], axis=0
    )


def beside(left, right):
    return jnp.concatenate([left, right], axis=1)


def project_kernel(count, *refs):
    blocks, rim_ref, w_ref, small_ref = refs[:count], *refs[count:count + 3]
    p_ref, rim_out, sc_ref = refs[count + 3:]
    rows = p_ref.shape[1]
    tokens = jnp.concatenate([ref[...] for ref in blocks] + [rim_ref[...]], axis=0)
    sc_ref[...] = dot(tokens, small_ref[...])[:rows]

    def one(branch, carry):
        out = dot(tokens, w_ref[branch]).astype(bf16)
        p_ref[branch] = out[:rows]
        rim_out[branch] = out[rows:]
        return carry

    lax.fori_loop(0, w_ref.shape[0], one, 0)


def block_diagonal(left, right):
    hole = jnp.zeros_like(left)
    return jnp.concatenate(
        [jnp.concatenate([left, hole], axis=1), jnp.concatenate([hole, right], axis=1)], axis=0
    )


def beside(left, right):
    return jnp.concatenate([left, right], axis=1)


def grid_index(shape):
    return lax.broadcasted_iota(jnp.int32, shape, 0), lax.broadcasted_iota(jnp.int32, shape, 1)


def delta_kernel(
    heads, blocks, me_ref, p_ref, rim_ref, sc_ref, late0_ref, late1_ref, w_ref, small_ref,
    taps_ref, vec_ref, x_ref, both_ref, low_ref, act, cols, rows_of,
    xp, sc, masks, mixes, solves,
):
    seq_rows = act.shape[1]
    rows = seq_rows // blocks
    chunks = seq_rows // CHUNK
    taps = taps_ref.shape[1]
    me = me_ref[0]

    def place(m, offset=0):
        return pl.multiple_of(offset + lax.bitwise_xor(me, m) * rows, 8)

    late = jnp.concatenate([late0_ref[...], late1_ref[...]], axis=0)
    sc[pl.ds(place(blocks - 1), rows)] = dot(late, small_ref[...])
    for m in range(blocks - 1):
        sc[pl.ds(place(m), rows)] = sc_ref[m * rows:(m + 1) * rows]

    def fill(branch, carry):
        made = dot(late, w_ref[branch]).astype(bf16).astype(f32)
        for head in range(heads):
            tile = branch * heads + head
            lanes = slice(head * LANES, (head + 1) * LANES)
            xp[tile, :RIM] = rim_ref[branch, :, lanes].astype(f32)
            xp[tile, pl.ds(place(blocks - 1, RIM), rows)] = made[:, lanes]
            for m in range(blocks - 1):
                xp[tile, pl.ds(place(m, RIM), rows)] = p_ref[branch, m * rows:(m + 1) * rows, lanes].astype(f32)
        return carry

    lax.fori_loop(0, 3, fill, 0)

    ri, ci = grid_index((CHUNK, CHUNK))
    upto = ri >= ci
    lower = upto.astype(f32)
    levels = CHUNK.bit_length() - 1
    for level in range(levels):
        hit = ((ri >> (level + 1)) == (ci >> (level + 1))) & ((ri >> level) > (ci >> level))
        hit = hit.astype(f32).astype(bf16)
        masks[level] = beside(hit, hit)

    root = 1.0 / math.sqrt(LANES)

    def prepare(chunk, carry):
        base = pl.multiple_of(chunk * CHUNK, CHUNK)
        raw = sc[pl.ds(base, CHUNK)]
        shifted = raw + vec_ref[1:2]
        soft = jnp.maximum(shifted, 0.0) + jnp.log1p(jnp.exp(-jnp.abs(shifted)))
        decay = dot(lower, vec_ref[0:1] * soft, precision=lax.Precision.HIGHEST)
        beta = 1.0 / (1.0 + jnp.exp(-raw))
        comb = jnp.where(ci < heads, decay, 0.0)
        for head in range(heads):
            norms = []
            for branch in range(3):
                tile = branch * heads + head
                total = None
                for i in range(taps):
                    term = xp[tile, pl.ds(base + (RIM - taps + 1 + i), CHUNK)] * taps_ref[tile, i:i + 1]
                    total = term if total is None else total + term
                value = silu(total).astype(bf16)
                act[tile, pl.ds(base, CHUNK)] = value
                if branch < 2:
                    wide = value.astype(f32)
                    norms.append(lax.rsqrt(jnp.sum(wide * wide, axis=-1, keepdims=True) + EPS))
            scaled = beta[:, heads + head:heads + head + 1] * norms[1]
            comb = jnp.where(ci == heads + head, scaled, comb)
            comb = jnp.where(ci == 2 * heads + head, norms[0] * root, comb)
            comb = jnp.where(ci == 3 * heads + head, norms[1], comb)
        cols[chunk] = comb
        rows_of[chunk] = comb.T
        return carry

    lax.fori_loop(0, chunks, prepare, 0)

    def part(branch, head, chunk):
        return act[branch * heads + head, chunk * CHUNK:(chunk + 1) * CHUNK]

    def col(kind, head, chunk):
        lane = kind * heads + head
        return cols[chunk, :, lane:lane + 1]

    def row(kind, head, chunk):
        lane = kind * heads + head
        return rows_of[chunk, lane:lane + 1, :]

    sets = [(head, chunk) for head in range(heads) for chunk in range(0, chunks, 2)]
    for s, (head, first) in enumerate(sets):
        two = (first, first + 1)
        keys = [part(1, head, c) for c in two]
        gram = dot(beside(*keys), block_diagonal(*[k.T for k in keys]))
        mix = []
        for i, c in enumerate(two):
            lanes = slice(i * LANES, (i + 1) * LANES)
            gap = col(0, head, c) - row(0, head, c)
            weight = jnp.exp(jnp.minimum(gap, 0.0)) * row(1, head, c)
            mix.append((weight * gram[:, lanes] * col(3, head, c)).astype(bf16))
        mix = beside(*mix)
        mixes[s] = mix
        eye = jnp.where(ri == ci, 1.0, 0.0)
        solves[s] = beside(eye, eye) - (mix * masks[0]).astype(f32)
    for level in range(1, levels):
        lows, mids = [], []
        for s in range(len(sets)):
            low = solves[s].astype(bf16)
            lows.append(low)
            mids.append(dot(mixes[s] * masks[level], block_diagonal(low[:, :LANES], low[:, LANES:])).astype(bf16))
        for s in range(len(sets)):
            mid = mids[s]
            solves[s] = solves[s] - dot(lows[s], block_diagonal(mid[:, :LANES], mid[:, LANES:]))
    change = {}
    for s, (head, first) in enumerate(sets):
        two = (first, first + 1)
        solve = solves[s]
        new = dot(solve.astype(bf16), block_diagonal(*[part(2, head, c) for c in two]))
        grown = beside(*[jnp.exp(row(0, head, c)) * row(3, head, c) for c in two])
        back = dot((solve * grown).astype(bf16), block_diagonal(*[part(1, head, c) for c in two]))
        for i, c in enumerate(two):
            lanes = slice(i * LANES, (i + 1) * LANES)
            both = beside(back[:, lanes], new[:, lanes])
            decay = col(0, head, c)
            tail = col(1, head, c) * jnp.exp(decay[CHUNK - 1:] - decay)
            change[head, c] = dot(part(1, head, c), (both * tail).astype(bf16), (0, 0))
            both_ref[head, c] = both.astype(bf16)
    runs = {}
    for c in range(chunks):
        for head in range(heads):
            last = jnp.exp(col(0, head, c)[CHUNK - 1:])
            if c == 0:
                runs[head] = beside(
                    jnp.where(ri == ci, last, 0.0) - change[head, c][:, :LANES], change[head, c][:, LANES:]
                )
            else:
                low = runs[head].astype(bf16)
                low_ref[head, c - 1] = low
                run = last * runs[head] - dot(change[head, c][:, :LANES].astype(bf16), low)
                runs[head] = beside(run[:, :LANES], run[:, LANES:] + change[head, c][:, LANES:])
    for head in range(heads):
        x_ref[head] = runs[head].astype(bf16)


def reach_kernel(
    heads, blocks, count, me_ref, both_ref, low_ref, act, cols, rows_of, w_ref, *refs
):
    tokens_refs, (qp_ref, o_ref, gate_ref) = refs[:count], refs[count:]
    seq_rows = act.shape[1]
    rows = seq_rows // blocks
    chunks = seq_rows // CHUNK
    me = me_ref[0]
    tokens = jnp.concatenate([ref[...] for ref in tokens_refs], axis=0)
    gate = silu(dot(tokens, w_ref[...]))
    for m in range(blocks):
        at = pl.multiple_of(lax.bitwise_xor(me, m) * rows, 8)
        gate_ref[pl.ds(at, rows)] = gate[m * rows:(m + 1) * rows]
    ri, ci = grid_index((CHUNK, CHUNK))
    upto = ri >= ci
    for head in range(heads):
        for c in range(chunks):
            at = slice(c * CHUNK, (c + 1) * CHUNK)

            def col(kind):
                lane = kind * heads + head
                return cols[c, :, lane:lane + 1]

            def row(kind):
                lane = kind * heads + head
                return rows_of[c, lane:lane + 1, :]

            q = act[head, at]
            score = dot(q, act[heads + head, at], (1, 1))
            weight = jnp.exp(jnp.minimum(col(0) - row(0), 0.0)) * row(1)
            attend = jnp.where(upto, weight * score * col(2), 0.0).astype(bf16)
            inner = dot(attend, both_ref[head, c])
            eff = (jnp.exp(col(0)) * col(2)) * q.astype(f32) - inner[:, :LANES]
            if c == 0:
                qp_ref[head, at] = eff.astype(bf16)
                o_ref[head, at] = inner[:, LANES:]
            else:
                ahead = dot(eff.astype(bf16), low_ref[head, c - 1])
                qp_ref[head, at] = ahead[:, :LANES].astype(bf16)
                o_ref[head, at] = inner[:, LANES:] + ahead[:, LANES:]


def pair_kernel(share, core_ref, mine_ref, other_ref, out_ref):
    core = core_ref[0]
    heads = mine_ref.shape[0]
    for j in range(out_ref.shape[0]):
        head = core * out_ref.shape[0] + j if share else j
        mine, other = mine_ref[head], other_ref[head]
        first = jnp.where(core == 0, mine, other)
        second = jnp.where(core == 0, other, mine)
        both = dot(second[:, :LANES], first)
        out_ref[j, :, :LANES] = both[:, :LANES].astype(bf16)
        out_ref[j, :, LANES:] = (both[:, LANES:] + second[:, LANES:].astype(f32)).astype(bf16)


def fold_kernel(*refs):
    out_ref = refs[-1]
    for j in range(out_ref.shape[0]):
        state = refs[0][j].astype(f32)
        for ref in refs[1:-1]:
            step = ref[j]
            state = step[:, LANES:].astype(f32) + dot(step[:, :LANES], state.astype(bf16))
        out_ref[j] = state.astype(bf16)


def final_kernel(share, core_ref, qp_ref, o_ref, pair_ref, mine_ref, other_ref, gate_ref, gain_ref, out_ref):
    heads, seq_rows, dim = qp_ref.shape
    core = core_ref[0]
    part = mine_ref.shape[0]
    for head in range(heads):
        start = mine_ref[head % part]
        if share:
            start = jnp.where(core == head // part, start, other_ref[head % part])
        pair = pair_ref[head]
        moved = pair[:, dim:].astype(f32) + dot(pair[:, :dim], start)
        start = jnp.where(core == 0, start.astype(f32), moved).astype(bf16)
        lanes = slice(head * dim, (head + 1) * dim)
        y = o_ref[head] + dot(qp_ref[head], start)
        scale = lax.rsqrt(jnp.mean(y * y, axis=-1, keepdims=True) + EPS)
        out_ref[:, lanes] = (y * scale * gain_ref[...] * gate_ref[:, lanes]).astype(bf16)


def call(kernel, name, out, operands, scalars=1, flops=0, scratch=(), limit=24):
    single = not isinstance(out, tuple)
    return pl.pallas_call(
        kernel,
        out_shape=out,
        in_specs=[whole(pltpu.SMEM)] * scalars + [whole()] * (len(operands) - scalars),
        out_specs=whole() if single else (whole(),) * len(out),
        scratch_shapes=scratch,
        cost_estimate=pl.CostEstimate(flops=flops, transcendentals=0, bytes_accessed=1 << 20),
        compiler_params=pltpu.CompilerParams(vmem_limit_bytes=limit << 20),
        name=name,
    )(*operands)


def per_device(hidden, w_qkv, w_gate, w_decay_beta, conv_weight, decay_rate, dt_bias, norm_gain):
    model_width = hidden.shape[1]
    heads = decay_rate.shape[0]
    dim = norm_gain.shape[0]
    columns = heads * dim
    blocks = lax.axis_size("tp")
    seq_count = lax.axis_size("seq")
    rows = hidden.shape[0]
    seq_rows = rows * blocks
    chunks = seq_rows // CHUNK
    me = jnp.full((1,), lax.axis_index("tp"), jnp.int32)
    core = jnp.full((1,), lax.axis_index("seq") % 2, jnp.int32)
    shape = jax.ShapeDtypeStruct

    w_three = w_qkv.transpose(1, 0, 2)
    small = jnp.pad(
        w_decay_beta.reshape(model_width, 2 * heads), ((0, 0), (0, LANES - 2 * heads))
    )
    taps = conv_weight.reshape(conv_weight.shape[0], 3 * heads, dim).transpose(1, 0, 2).astype(f32)
    vectors = jnp.pad(jnp.stack([-decay_rate, dt_bias]), ((0, 6), (0, LANES - heads)))

    early, late = gather_blocks(hidden, "tp")
    rim = rim_rows(hidden, RIM)
    early_rows = seq_rows - rows
    projected, rim, scalars = call(
        functools.partial(project_kernel, len(early)), "project",
        (
            shape((3, early_rows, columns), bf16),
            shape((3, RIM, columns), bf16),
            shape((early_rows, LANES), f32),
        ),
        [*early, rim, w_three, small], scalars=0, flops=PROJECT_FLOPS,
    )
    own, both, low, act, cols, rows_of = call(
        functools.partial(delta_kernel, heads, blocks), "delta",
        (
            shape((heads, dim, 2 * dim), bf16),
            shape((heads, chunks, CHUNK, 2 * dim), bf16),
            shape((heads, chunks - 1, dim, 2 * dim), bf16),
            shape((3 * heads, seq_rows, dim), bf16),
            shape((chunks, CHUNK, LANES), f32),
            shape((chunks, CHUNK, LANES), f32),
        ),
        [me, projected, rim, scalars, *late, w_three, small, taps, vectors],
        flops=DELTA_FLOPS, limit=32,
        scratch=[
            pltpu.VMEM((3 * heads, seq_rows + RIM, dim), f32),
            pltpu.VMEM((seq_rows, LANES), f32),
            pltpu.VMEM((CHUNK.bit_length() - 1, CHUNK, 2 * CHUNK), bf16),
            pltpu.VMEM((heads * chunks // 2, CHUNK, 2 * CHUNK), bf16),
            pltpu.VMEM((heads * chunks // 2, CHUNK, 2 * CHUNK), f32),
        ],
    )
    tokens = [*early, *late]
    reach, base, gate = call(
        functools.partial(reach_kernel, heads, blocks, len(tokens)), "reach",
        (
            shape((heads, seq_rows, dim), bf16),
            shape((heads, seq_rows, dim), f32),
            shape((seq_rows, columns), f32),
        ),
        [me, both, low, act, cols, rows_of, w_gate, *tokens], flops=REACH_FLOPS,
    )

    share = heads % 2 == 0
    part = heads // 2 if share else heads
    swap = [(i, i ^ 1) for i in range(seq_count)]
    other = lax.ppermute(own, "seq", swap)
    joined = call(
        functools.partial(pair_kernel, share), "pair",
        shape((part, dim, 2 * dim), bf16), [core, own, other], flops=SMALL_FLOPS, limit=4,
    )
    steps = []
    for distance in range(seq_count // 2 - 1, 0, -1):
        sent = joined if steps else joined[:, :, dim:]
        route = [(i, i + 2 * distance) for i in range(seq_count - 2 * distance)]
        steps.append(lax.ppermute(sent, "seq", route))
    state = call(
        fold_kernel, "fold", shape((part, dim, dim), bf16), steps,
        scalars=0, flops=SMALL_FLOPS, limit=4,
    )
    back = lax.ppermute(state, "seq", swap) if share else state
    return call(
        functools.partial(final_kernel, share), "final", shape((seq_rows, columns), bf16),
        [core, reach, base, other, state, back, gate, norm_gain.reshape(1, dim)],
        flops=SMALL_FLOPS, limit=12,
    )


def solution(mesh):
    return jax.shard_map(
        per_device,
        mesh=mesh,
        in_specs=(
            P(("seq", "tp"), None),
            P(None, None, "tp"),
            P(None, "tp"),
            P(None, None, "tp"),
            P(None, None, "tp"),
            P("tp"),
            P("tp"),
            P(),
        ),
        out_specs=P("seq", "tp"),
        check_vma=False,
    )
```

```python
import functools
import math

import jax
import jax.numpy as jnp
from jax import lax
from jax.experimental import pallas as pl
from jax.experimental.pallas import tpu as pltpu
from jax.sharding import PartitionSpec as P


CHUNK = 128
LANES = 128
RIM = 16
EPS = 1e-6
PROJECT_FLOPS = 3000000000
DELTA_FLOPS = 3000000000
REACH_FLOPS = 2000000000
SMALL_FLOPS = 50000000

f32 = jnp.float32
bf16 = jnp.bfloat16


def dot(left, right, contract=(1, 0), precision=None):
    dims = (((contract[0],), (contract[1],)), ((), ()))
    return lax.dot_general(left, right, dims, precision=precision, preferred_element_type=f32)


def whole(memory=pltpu.VMEM):
    return pl.BlockSpec(memory_space=memory)


def gather_blocks(block, axis):
    count = lax.axis_size(axis)
    bits = count.bit_length() - 1
    half = block.shape[0] // 2

    def swap(value, bit):
        step = 1 << bit
        return lax.ppermute(value, axis, [(i, i ^ step) for i in range(count)])

    found = {0: block}
    for bit in range(bits):
        found[1 << bit] = swap(block, bit)
    halves = []
    for number, order in enumerate((range(bits), range(bits - 1, -1, -1))):
        part = {m: value[number * half:(number + 1) * half] for m, value in found.items()}
        for bit in order:
            for mask in list(part):
                if mask | (1 << bit) not in part:
                    part[mask | (1 << bit)] = swap(part[mask], bit)
        halves.append(part)
    early = [found[m] if m in found else (halves[0][m], halves[1][m]) for m in range(count - 1)]
    flat = []
    for item in early[1:]:
        flat.extend(item if isinstance(item, tuple) else (item,))
    return flat, [halves[0][count - 1], halves[1][count - 1]]


def rim_rows(block, count):
    seq_count, tp_count = lax.axis_size("seq"), lax.axis_size("tp")
    tail = block[-count:]
    total = None
    for j in range(tp_count):
        route = [(s * tp_count - 1, s * tp_count + j) for s in range(1, seq_count)]
        part = lax.ppermute(tail, ("seq", "tp"), route)
        total = part if total is None else total + part
    return total


def silu(x):
    return x / (1.0 + jnp.exp(-x))


def project_kernel(count, *refs):
    blocks = refs[:count]
    w_ref, gate_w_ref, small_ref = refs[count:count + 3]
    p_ref, gate_ref, sc_ref = refs[count + 3:count + 6]
    rows = sc_ref.shape[0]
    tokens = jnp.concatenate([ref[...] for ref in blocks], axis=0)
    sc_ref[...] = dot(tokens, small_ref[...])[:rows]
    gate_ref[...] = silu(dot(tokens, gate_w_ref[...])[:rows])

    def one(branch, carry):
        p_ref[branch] = dot(tokens, w_ref[branch]).astype(bf16)
        return carry

    lax.fori_loop(0, w_ref.shape[0], one, 0)


def block_diagonal(left, right):
    hole = jnp.zeros_like(left)
    return jnp.concatenate(
        [jnp.concatenate([left, hole], axis=1), jnp.concatenate([hole, right], axis=1)], axis=0
    )


def beside(left, right):
    return jnp.concatenate([left, right], axis=1)


def grid_index(shape):
    return lax.broadcasted_iota(jnp.int32, shape, 0), lax.broadcasted_iota(jnp.int32, shape, 1)


def delta_kernel(
    heads, blocks, own_ref, own_sc_ref, p_ref, sc_ref, late0_ref, late1_ref, w_ref,
    gate_w_ref, small_ref, taps_ref, vec_ref, x_ref, both_ref, low_ref, act, cols, rows_of, gate_ref,
    xp, sc, masks, mixes, solves,
):
    seq_rows = act.shape[1]
    rows = seq_rows // blocks
    chunks = seq_rows // CHUNK
    taps = taps_ref.shape[1]
    me = lax.axis_index("tp")

    def place(m, offset=0):
        return pl.multiple_of(offset + lax.bitwise_xor(me, m) * rows, 8)

    late = jnp.concatenate([late0_ref[...], late1_ref[...]], axis=0)
    sc[pl.ds(place(blocks - 1), rows)] = dot(late, small_ref[...])
    gate_ref[...] = silu(dot(late, gate_w_ref[...]))
    sc[pl.ds(place(0), rows)] = own_sc_ref[...]
    for m in range(1, blocks - 1):
        sc[pl.ds(place(m), rows)] = sc_ref[(m - 1) * rows:m * rows]

    def fill(branch, carry):
        made = dot(late, w_ref[branch]).astype(bf16).astype(f32)
        for head in range(heads):
            tile = branch * heads + head
            lanes = slice(head * LANES, (head + 1) * LANES)
            xp[tile, :RIM] = p_ref[branch, (blocks - 2) * rows:, lanes].astype(f32)
            xp[tile, pl.ds(place(0, RIM), rows)] = own_ref[branch, :, lanes].astype(f32)
            xp[tile, pl.ds(place(blocks - 1, RIM), rows)] = made[:, lanes]
            for m in range(1, blocks - 1):
                block = p_ref[branch, (m - 1) * rows:m * rows, lanes]
                xp[tile, pl.ds(place(m, RIM), rows)] = block.astype(f32)
        return carry

    lax.fori_loop(0, 3, fill, 0)

    ri, ci = grid_index((CHUNK, CHUNK))
    upto = ri >= ci
    lower = upto.astype(f32)
    levels = CHUNK.bit_length() - 1
    for level in range(levels):
        hit = ((ri >> (level + 1)) == (ci >> (level + 1))) & ((ri >> level) > (ci >> level))
        hit = hit.astype(f32).astype(bf16)
        masks[level] = beside(hit, hit)

    root = 1.0 / math.sqrt(LANES)

    def prepare(chunk, carry):
        base = pl.multiple_of(chunk * CHUNK, CHUNK)
        raw = sc[pl.ds(base, CHUNK)]
        shifted = raw + vec_ref[1:2]
        soft = jnp.maximum(shifted, 0.0) + jnp.log1p(jnp.exp(-jnp.abs(shifted)))
        decay = dot(lower, vec_ref[0:1] * soft, precision=lax.Precision.HIGHEST)
        beta = 1.0 / (1.0 + jnp.exp(-raw))
        comb = jnp.where(ci < heads, decay, 0.0)
        for head in range(heads):
            norms = []
            for branch in range(3):
                tile = branch * heads + head
                total = None
                for i in range(taps):
                    term = xp[tile, pl.ds(base + (RIM - taps + 1 + i), CHUNK)] * taps_ref[tile, i:i + 1]
                    total = term if total is None else total + term
                value = silu(total).astype(bf16)
                act[tile, pl.ds(base, CHUNK)] = value
                if branch < 2:
                    wide = value.astype(f32)
                    norms.append(lax.rsqrt(jnp.sum(wide * wide, axis=-1, keepdims=True) + EPS))
            scaled = beta[:, heads + head:heads + head + 1] * norms[1]
            comb = jnp.where(ci == heads + head, scaled, comb)
            comb = jnp.where(ci == 2 * heads + head, norms[0] * root, comb)
            comb = jnp.where(ci == 3 * heads + head, norms[1], comb)
        cols[chunk] = comb
        rows_of[chunk] = comb.T
        return carry

    lax.fori_loop(0, chunks, prepare, 0)

    def part(branch, head, chunk):
        return act[branch * heads + head, chunk * CHUNK:(chunk + 1) * CHUNK]

    def col(kind, head, chunk):
        lane = kind * heads + head
        return cols[chunk, :, lane:lane + 1]

    def row(kind, head, chunk):
        lane = kind * heads + head
        return rows_of[chunk, lane:lane + 1, :]

    sets = [(head, chunk) for head in range(heads) for chunk in range(0, chunks, 2)]
    for s, (head, first) in enumerate(sets):
        two = (first, first + 1)
        keys = [part(1, head, c) for c in two]
        gram = dot(beside(*keys), block_diagonal(*[k.T for k in keys]))
        mix = []
        for i, c in enumerate(two):
            lanes = slice(i * LANES, (i + 1) * LANES)
            gap = col(0, head, c) - row(0, head, c)
            weight = jnp.exp(jnp.minimum(gap, 0.0)) * row(1, head, c)
            mix.append((weight * gram[:, lanes] * col(3, head, c)).astype(bf16))
        mix = beside(*mix)
        mixes[s] = mix
        eye = jnp.where(ri == ci, 1.0, 0.0)
        solves[s] = beside(eye, eye) - (mix * masks[0]).astype(f32)
    for level in range(1, levels):
        lows, mids = [], []
        for s in range(len(sets)):
            low = solves[s].astype(bf16)
            lows.append(low)
            mids.append(dot(mixes[s] * masks[level], block_diagonal(low[:, :LANES], low[:, LANES:])).astype(bf16))
        for s in range(len(sets)):
            mid = mids[s]
            solves[s] = solves[s] - dot(lows[s], block_diagonal(mid[:, :LANES], mid[:, LANES:]))
    change = {}
    for s, (head, first) in enumerate(sets):
        two = (first, first + 1)
        solve = solves[s]
        new = dot(solve.astype(bf16), block_diagonal(*[part(2, head, c) for c in two]))
        grown = beside(*[jnp.exp(row(0, head, c)) * row(3, head, c) for c in two])
        back = dot((solve * grown).astype(bf16), block_diagonal(*[part(1, head, c) for c in two]))
        for i, c in enumerate(two):
            lanes = slice(i * LANES, (i + 1) * LANES)
            both = beside(back[:, lanes], new[:, lanes])
            decay = col(0, head, c)
            tail = col(1, head, c) * jnp.exp(decay[CHUNK - 1:] - decay)
            change[head, c] = dot(part(1, head, c), (both * tail).astype(bf16), (0, 0))
            both_ref[head, c] = both.astype(bf16)
    runs = {}
    for c in range(chunks):
        for head in range(heads):
            last = jnp.exp(col(0, head, c)[CHUNK - 1:])
            if c == 0:
                runs[head] = beside(
                    jnp.where(ri == ci, last, 0.0) - change[head, c][:, :LANES], change[head, c][:, LANES:]
                )
            else:
                low = runs[head].astype(bf16)
                low_ref[head, c - 1] = low
                run = last * runs[head] - dot(change[head, c][:, :LANES].astype(bf16), low)
                runs[head] = beside(run[:, :LANES], run[:, LANES:] + change[head, c][:, LANES:])
    for head in range(heads):
        x_ref[head] = runs[head].astype(bf16)


def reach_kernel(heads, both_ref, low_ref, act, cols, rows_of, qp_ref, o_ref):
    chunks = act.shape[1] // CHUNK
    ri, ci = grid_index((CHUNK, CHUNK))
    upto = ri >= ci
    for head in range(heads):
        for c in range(chunks):
            at = slice(c * CHUNK, (c + 1) * CHUNK)

            def col(kind):
                lane = kind * heads + head
                return cols[c, :, lane:lane + 1]

            def row(kind):
                lane = kind * heads + head
                return rows_of[c, lane:lane + 1, :]

            q = act[head, at]
            score = dot(q, act[heads + head, at], (1, 1))
            weight = jnp.exp(jnp.minimum(col(0) - row(0), 0.0)) * row(1)
            attend = jnp.where(upto, weight * score * col(2), 0.0).astype(bf16)
            inner = dot(attend, both_ref[head, c])
            eff = (jnp.exp(col(0)) * col(2)) * q.astype(f32) - inner[:, :LANES]
            if c == 0:
                qp_ref[head, at] = eff.astype(bf16)
                o_ref[head, at] = inner[:, LANES:]
            else:
                ahead = dot(eff.astype(bf16), low_ref[head, c - 1])
                qp_ref[head, at] = ahead[:, :LANES].astype(bf16)
                o_ref[head, at] = inner[:, LANES:] + ahead[:, LANES:]


def pair_kernel(share, mine_ref, other_ref, out_ref):
    core = lax.axis_index("seq") & 1
    for j in range(out_ref.shape[0]):
        head = core * out_ref.shape[0] + j if share else j
        mine, other = mine_ref[head], other_ref[head]
        first = jnp.where(core == 0, mine, other)
        second = jnp.where(core == 0, other, mine)
        both = dot(second[:, :LANES], first)
        out_ref[j, :, :LANES] = both[:, :LANES].astype(bf16)
        out_ref[j, :, LANES:] = (both[:, LANES:] + second[:, LANES:].astype(f32)).astype(bf16)


def climb_kernel(bit, inside_ref, block_ref, sent_ref, inside_out, block_out):
    upper = (lax.axis_index("seq") >> (bit + 1)) & 1
    for j in range(block_ref.shape[0]):
        sent = sent_ref[j]
        for ref, out in ((inside_ref, inside_out), (block_ref, block_out)):
            mine = ref[j]
            both = dot(mine[:, :LANES], sent)
            left = jnp.where(upper == 1, both[:, :LANES], mine[:, :LANES].astype(f32))
            right = mine[:, LANES:].astype(f32) + both[:, LANES:]
            out[j] = jnp.concatenate([left, right], axis=1).astype(bf16)


def first_kernel(block_ref, sent_ref, inside_out, block_out):
    upper = (lax.axis_index("seq") >> 1) & 1
    ri, ci = grid_index((LANES, LANES))
    eye = jnp.where(ri == ci, 1.0, 0.0)
    for j in range(block_ref.shape[0]):
        sent, mine = sent_ref[j], block_ref[j]
        both = dot(mine[:, :LANES], sent)
        left = jnp.where(upper == 1, both[:, :LANES], mine[:, :LANES].astype(f32))
        right = mine[:, LANES:].astype(f32) + both[:, LANES:]
        block_out[j] = jnp.concatenate([left, right], axis=1).astype(bf16)
        inside = jnp.where(upper == 1, sent[:, :LANES].astype(f32), eye)
        inside_out[j] = jnp.concatenate([inside.astype(bf16), sent[:, LANES:]], axis=1)


def fold_kernel(inside_ref, *refs):
    out_ref = refs[-1]
    for j in range(out_ref.shape[0]):
        state = refs[0][j]
        for ref in refs[1:-1]:
            state = state + ref[j]
        inside = inside_ref[j]
        state = inside[:, LANES:].astype(f32) + dot(inside[:, :LANES], state)
        out_ref[j] = state.astype(bf16)


def final_kernel(
    share, blocks, qp_ref, o_ref, pair_ref, mine_ref, other_ref,
    own_gate_ref, gate_ref, late_gate_ref, gain_ref, out_ref,
):
    heads, seq_rows, dim = qp_ref.shape
    rows = seq_rows // blocks
    core, me = lax.axis_index("seq") & 1, lax.axis_index("tp")
    part = mine_ref.shape[0]
    for head in range(heads):
        start = mine_ref[head % part]
        if share:
            start = jnp.where(core == head // part, start, other_ref[head % part])
        pair = pair_ref[head]
        moved = pair[:, dim:].astype(f32) + dot(pair[:, :dim], start)
        start = jnp.where(core == 0, start.astype(f32), moved).astype(bf16)
        lanes = slice(head * dim, (head + 1) * dim)
        for m in range(blocks):
            if m == 0:
                gate = own_gate_ref[:, lanes]
            elif m < blocks - 1:
                gate = gate_ref[(m - 1) * rows:m * rows, lanes]
            else:
                gate = late_gate_ref[:, lanes]
            at = pl.ds(pl.multiple_of(lax.bitwise_xor(me, m) * rows, 8), rows)
            y = o_ref[head, at] + dot(qp_ref[head, at], start)
            scale = lax.rsqrt(jnp.mean(y * y, axis=-1, keepdims=True) + EPS)
            out_ref[at, lanes] = (y * scale * gain_ref[...] * gate).astype(bf16)


def call(kernel, out, operands, flops=0, scratch=(), limit=24):
    single = not isinstance(out, tuple)
    return pl.pallas_call(
        kernel,
        out_shape=out,
        in_specs=[whole()] * len(operands),
        out_specs=whole() if single else (whole(),) * len(out),
        scratch_shapes=scratch,
        cost_estimate=pl.CostEstimate(flops=flops, transcendentals=0, bytes_accessed=1 << 20),
        compiler_params=pltpu.CompilerParams(vmem_limit_bytes=limit << 20),
    )(*operands)


def per_device(hidden, w_qkv, w_gate, w_decay_beta, conv_weight, decay_rate, dt_bias, norm_gain):
    model_width = hidden.shape[1]
    heads = decay_rate.shape[0]
    dim = norm_gain.shape[0]
    columns = heads * dim
    blocks = lax.axis_size("tp")
    seq_count = lax.axis_size("seq")
    rows = hidden.shape[0]
    seq_rows = rows * blocks
    chunks = seq_rows // CHUNK
    shape = jax.ShapeDtypeStruct

    w_three = w_qkv.transpose(1, 0, 2)
    small = jnp.pad(
        w_decay_beta.reshape(model_width, 2 * heads), ((0, 0), (0, LANES - 2 * heads))
    )
    taps = conv_weight.reshape(conv_weight.shape[0], 3 * heads, dim).transpose(1, 0, 2).astype(f32)
    vectors = jnp.pad(jnp.stack([-decay_rate, dt_bias]), ((0, 6), (0, LANES - heads)))

    early, late = gather_blocks(hidden, "tp")
    rim = rim_rows(hidden, RIM)
    weights = [w_three, w_gate, small]

    def project(tokens, count, extra=0):
        return call(
            functools.partial(project_kernel, len(tokens)),
            (
                shape((3, count + extra, columns), bf16),
                shape((count, columns), f32),
                shape((count, LANES), f32),
            ),
            [*tokens, *weights], flops=PROJECT_FLOPS, limit=20,
        )

    own_p, own_gate, own_sc = project([hidden], rows)
    mid_p, mid_gate, mid_sc = project([*early, rim], seq_rows - 2 * rows, RIM)
    own, both, low, act, cols, rows_of, late_gate = call(
        functools.partial(delta_kernel, heads, blocks),
        (
            shape((heads, dim, 2 * dim), bf16),
            shape((heads, chunks, CHUNK, 2 * dim), bf16),
            shape((heads, chunks - 1, dim, 2 * dim), bf16),
            shape((3 * heads, seq_rows, dim), bf16),
            shape((chunks, CHUNK, LANES), f32),
            shape((chunks, CHUNK, LANES), f32),
            shape((rows, columns), f32),
        ),
        [own_p, own_sc, mid_p, mid_sc, *late, *weights, taps, vectors],
        flops=DELTA_FLOPS, limit=32,
        scratch=[
            pltpu.VMEM((3 * heads, seq_rows + RIM, dim), f32),
            pltpu.VMEM((seq_rows, LANES), f32),
            pltpu.VMEM((CHUNK.bit_length() - 1, CHUNK, 2 * CHUNK), bf16),
            pltpu.VMEM((heads * chunks // 2, CHUNK, 2 * CHUNK), bf16),
            pltpu.VMEM((heads * chunks // 2, CHUNK, 2 * CHUNK), f32),
        ],
    )
    reach, base = call(
        functools.partial(reach_kernel, heads),
        (shape((heads, seq_rows, dim), bf16), shape((heads, seq_rows, dim), f32)),
        [both, low, act, cols, rows_of], flops=REACH_FLOPS, limit=12,
    )

    share = heads % 2 == 0
    part = heads // 2 if share else heads
    swap = [(i, i ^ 1) for i in range(seq_count)]
    other = lax.ppermute(own, "seq", swap)
    block = call(
        functools.partial(pair_kernel, share),
        shape((part, dim, 2 * dim), bf16), [own, other], flops=SMALL_FLOPS, limit=4,
    )
    chips = seq_count // 2
    levels = chips.bit_length() - 1
    inside = None
    for level in range(levels):
        size = 1 << level
        sent = block if level < levels - 1 or level == 0 else block[:, :, dim:]
        parts = []
        for target in range(size):
            route = []
            for top in range(size - 1, chips, 2 * size):
                for c in range(2):
                    route.append((2 * top + c, 2 * (top + 1 + target) + c))
            parts.append(lax.ppermute(sent, "seq", route))
        if level == levels - 1 and level > 0:
            break
        sent = sum(parts[1:], parts[0])
        kernel, operands = first_kernel, [block, sent]
        if level > 0:
            kernel, operands = functools.partial(climb_kernel, level), [inside, block, sent]
        inside, block = call(
            kernel, (shape(block.shape, bf16),) * 2, operands, flops=SMALL_FLOPS, limit=4,
        )
    state = call(
        fold_kernel, shape((part, dim, dim), bf16), [inside, *parts],
        flops=SMALL_FLOPS, limit=4,
    )
    back = lax.ppermute(state, "seq", swap) if share else state
    return call(
        functools.partial(final_kernel, share, blocks), shape((seq_rows, columns), bf16),
        [reach, base, other, state, back, own_gate, mid_gate, late_gate, norm_gain.reshape(1, dim)],
        flops=SMALL_FLOPS, limit=12,
    )


def solution(mesh):
    return jax.shard_map(
        per_device,
        mesh=mesh,
        in_specs=(
            P(("seq", "tp"), None),
            P(None, None, "tp"),
            P(None, "tp"),
            P(None, None, "tp"),
            P(None, None, "tp"),
            P("tp"),
            P("tp"),
            P(),
        ),
        out_specs=P("seq", "tp"),
        check_vma=False,
    )
```

```python
import functools
import math

import jax
import jax.numpy as jnp
from jax import lax
from jax.experimental import pallas as pl
from jax.experimental.pallas import tpu as pltpu
from jax.sharding import PartitionSpec as P


CHUNK = 128
LANES = 128
RIM = 16
EPS = 1e-6
PROJECT_FLOPS = 3000000000
DELTA_FLOPS = 3000000000
REACH_FLOPS = 2000000000
SMALL_FLOPS = 50000000


f32 = jnp.float32
bf16 = jnp.bfloat16


def dot(left, right, contract=(1, 0), precision=None):
    dims = (((contract[0],), (contract[1],)), ((), ()))
    return lax.dot_general(left, right, dims, precision=precision, preferred_element_type=f32)


def whole(memory=pltpu.VMEM):
    return pl.BlockSpec(memory_space=memory)


def gather_blocks(block, axis):
    count = lax.axis_size(axis)
    bits = count.bit_length() - 1
    half = block.shape[0] // 2

    def swap(value, bit):
        step = 1 << bit
        return lax.ppermute(value, axis, [(i, i ^ step) for i in range(count)])

    found = {0: block}
    for bit in range(bits):
        found[1 << bit] = swap(block, bit)
    halves = []
    for number, order in enumerate((range(bits), range(bits - 1, -1, -1))):
        part = {m: value[number * half:(number + 1) * half] for m, value in found.items()}
        for bit in order:
            for mask in list(part):
                if mask | (1 << bit) not in part:
                    part[mask | (1 << bit)] = swap(part[mask], bit)
        halves.append(part)
    early = [found[m] if m in found else (halves[0][m], halves[1][m]) for m in range(count - 1)]
    flat = []
    for item in early[1:]:
        flat.extend(item if isinstance(item, tuple) else (item,))
    return flat, [halves[0][count - 1], halves[1][count - 1]]


def rim_rows(block, count):
    seq_count, tp_count = lax.axis_size("seq"), lax.axis_size("tp")
    tail = block[-count:]
    total = None
    for j in range(tp_count):
        route = [(s * tp_count - 1, s * tp_count + j) for s in range(1, seq_count)]
        part = lax.ppermute(tail, ("seq", "tp"), route)
        total = part if total is None else total + part
    return total


def silu(x):
    return x / (1.0 + jnp.exp(-x))


def scalar_weights(ref):
    kinds, heads, width = ref.shape
    rows = [ref[kind].astype(f32) for kind in range(kinds)]
    rows.append(jnp.zeros((LANES - kinds * heads, width), f32))
    return jnp.concatenate(rows, axis=0).astype(bf16)


def lane_row(ref):
    lane = lax.broadcasted_iota(jnp.int32, (1, LANES), 1)
    row = jnp.zeros((1, LANES), f32)
    for head in range(ref.shape[1]):
        row = jnp.where(lane == head, ref[:, head:head + 1], row)
    return row


def project_kernel(count, *refs):
    blocks = refs[:count]
    w_ref, gate_w_ref, small_ref = refs[count:count + 3]
    p_ref, gate_ref, sc_ref = refs[count + 3:count + 6]
    rows = sc_ref.shape[0]
    tokens = jnp.concatenate([ref[...] for ref in blocks], axis=0)
    sc_ref[...] = dot(tokens, scalar_weights(small_ref), (1, 1))[:rows]
    gate_ref[...] = silu(dot(tokens, gate_w_ref[...])[:rows])

    def one(branch, carry):
        p_ref[branch] = dot(tokens, w_ref[branch]).astype(bf16)
        return carry

    lax.fori_loop(0, w_ref.shape[0], one, 0)


def block_diagonal(left, right):
    hole = jnp.zeros_like(left)
    return jnp.concatenate(
        [jnp.concatenate([left, hole], axis=1), jnp.concatenate([hole, right], axis=1)], axis=0
    )


def beside(left, right):
    return jnp.concatenate([left, right], axis=1)


def grid_index(shape):
    return lax.broadcasted_iota(jnp.int32, shape, 0), lax.broadcasted_iota(jnp.int32, shape, 1)


def delta_kernel(
    heads, blocks, own_ref, own_sc_ref, p_ref, sc_ref, late0_ref, late1_ref, w_ref,
    small_ref, taps_ref, rate_ref, bias_ref, x_ref, both_ref, low_ref, act, cols, rows_of,
    xp, sc, masks, mixes, solves,
):
    seq_rows = act.shape[1]
    rows = seq_rows // blocks
    chunks = seq_rows // CHUNK
    taps = taps_ref.shape[1]
    me = lax.axis_index("tp")

    def place(m, offset=0):
        return pl.multiple_of(offset + lax.bitwise_xor(me, m) * rows, 8)

    late = jnp.concatenate([late0_ref[...], late1_ref[...]], axis=0)
    sc[pl.ds(place(blocks - 1), rows)] = dot(late, scalar_weights(small_ref), (1, 1))
    sc[pl.ds(place(0), rows)] = own_sc_ref[...]
    for m in range(1, blocks - 1):
        sc[pl.ds(place(m), rows)] = sc_ref[(m - 1) * rows:m * rows]

    def fill(branch, carry):
        made = dot(late, w_ref[branch]).astype(bf16).astype(f32)
        for head in range(heads):
            tile = branch * heads + head
            lanes = slice(head * LANES, (head + 1) * LANES)
            xp[tile, :RIM] = p_ref[branch, (blocks - 2) * rows:, lanes].astype(f32)
            xp[tile, pl.ds(place(0, RIM), rows)] = own_ref[branch, :, lanes].astype(f32)
            xp[tile, pl.ds(place(blocks - 1, RIM), rows)] = made[:, lanes]
            for m in range(1, blocks - 1):
                block = p_ref[branch, (m - 1) * rows:m * rows, lanes]
                xp[tile, pl.ds(place(m, RIM), rows)] = block.astype(f32)
        return carry

    lax.fori_loop(0, 3, fill, 0)

    ri, ci = grid_index((CHUNK, CHUNK))
    upto = ri >= ci
    lower = upto.astype(f32)
    levels = CHUNK.bit_length() - 1
    for level in range(levels):
        hit = ((ri >> (level + 1)) == (ci >> (level + 1))) & ((ri >> level) > (ci >> level))
        hit = hit.astype(f32).astype(bf16)
        masks[level] = beside(hit, hit)

    root = 1.0 / math.sqrt(LANES)
    rate, bias = -lane_row(rate_ref), lane_row(bias_ref)

    def prepare(chunk, carry):
        base = pl.multiple_of(chunk * CHUNK, CHUNK)
        raw = sc[pl.ds(base, CHUNK)]
        shifted = raw + bias
        soft = jnp.maximum(shifted, 0.0) + jnp.log1p(jnp.exp(-jnp.abs(shifted)))
        decay = dot(lower, rate * soft, precision=lax.Precision.HIGHEST)
        beta = 1.0 / (1.0 + jnp.exp(-raw))
        comb = jnp.where(ci < heads, decay, 0.0)
        for head in range(heads):
            norms = []
            for branch in range(3):
                tile = branch * heads + head
                weights = taps_ref[branch, :, head * LANES:(head + 1) * LANES].astype(f32)
                total = None
                for i in range(taps):
                    term = xp[tile, pl.ds(base + (RIM - taps + 1 + i), CHUNK)] * weights[i:i + 1]
                    total = term if total is None else total + term
                value = silu(total).astype(bf16)
                act[tile, pl.ds(base, CHUNK)] = value
                if branch < 2:
                    wide = value.astype(f32)
                    norms.append(lax.rsqrt(jnp.sum(wide * wide, axis=-1, keepdims=True) + EPS))
            scaled = beta[:, heads + head:heads + head + 1] * norms[1]
            comb = jnp.where(ci == heads + head, scaled, comb)
            comb = jnp.where(ci == 2 * heads + head, norms[0] * root, comb)
            comb = jnp.where(ci == 3 * heads + head, norms[1], comb)
        cols[chunk] = comb
        rows_of[chunk] = comb.T
        return carry

    lax.fori_loop(0, chunks, prepare, 0)

    def part(branch, head, chunk):
        return act[branch * heads + head, chunk * CHUNK:(chunk + 1) * CHUNK]

    def col(kind, head, chunk):
        lane = kind * heads + head
        return cols[chunk, :, lane:lane + 1]

    def row(kind, head, chunk):
        lane = kind * heads + head
        return rows_of[chunk, lane:lane + 1, :]

    sets = [(head, chunk) for head in range(heads) for chunk in range(0, chunks, 2)]
    for s, (head, first) in enumerate(sets):
        two = (first, first + 1)
        keys = [part(1, head, c) for c in two]
        gram = dot(beside(*keys), block_diagonal(*[k.T for k in keys]))
        mix = []
        for i, c in enumerate(two):
            lanes = slice(i * LANES, (i + 1) * LANES)
            gap = col(0, head, c) - row(0, head, c)
            weight = jnp.exp(jnp.minimum(gap, 0.0)) * row(1, head, c)
            mix.append((weight * gram[:, lanes] * col(3, head, c)).astype(bf16))
        mix = beside(*mix)
        mixes[s] = mix
        eye = jnp.where(ri == ci, 1.0, 0.0)
        solves[s] = beside(eye, eye) - (mix * masks[0]).astype(f32)
    for level in range(1, levels):
        lows, mids = [], []
        for s in range(len(sets)):
            low = solves[s].astype(bf16)
            lows.append(low)
            mids.append(dot(mixes[s] * masks[level], block_diagonal(low[:, :LANES], low[:, LANES:])).astype(bf16))
        for s in range(len(sets)):
            mid = mids[s]
            solves[s] = solves[s] - dot(lows[s], block_diagonal(mid[:, :LANES], mid[:, LANES:]))
    change = {}
    for s, (head, first) in enumerate(sets):
        two = (first, first + 1)
        solve = solves[s]
        new = dot(solve.astype(bf16), block_diagonal(*[part(2, head, c) for c in two]))
        grown = beside(*[jnp.exp(row(0, head, c)) * row(3, head, c) for c in two])
        back = dot((solve * grown).astype(bf16), block_diagonal(*[part(1, head, c) for c in two]))
        for i, c in enumerate(two):
            lanes = slice(i * LANES, (i + 1) * LANES)
            both = beside(back[:, lanes], new[:, lanes])
            decay = col(0, head, c)
            tail = col(1, head, c) * jnp.exp(decay[CHUNK - 1:] - decay)
            change[head, c] = dot(part(1, head, c), (both * tail).astype(bf16), (0, 0))
            both_ref[head, c] = both.astype(bf16)
    runs = {}
    for c in range(chunks):
        for head in range(heads):
            last = jnp.exp(col(0, head, c)[CHUNK - 1:])
            if c == 0:
                runs[head] = beside(
                    jnp.where(ri == ci, last, 0.0) - change[head, c][:, :LANES], change[head, c][:, LANES:]
                )
            else:
                low = runs[head].astype(bf16)
                low_ref[head, c - 1] = low
                run = last * runs[head] - dot(change[head, c][:, :LANES].astype(bf16), low)
                runs[head] = beside(run[:, :LANES], run[:, LANES:] + change[head, c][:, LANES:])
    for head in range(heads):
        x_ref[head] = runs[head].astype(bf16)


def reach_kernel(
    heads, both_ref, low_ref, act, cols, rows_of, late0_ref, late1_ref, gate_w_ref,
    qp_ref, o_ref, gate_ref,
):
    late = jnp.concatenate([late0_ref[...], late1_ref[...]], axis=0)
    gate_ref[...] = silu(dot(late, gate_w_ref[...]))
    chunks = act.shape[1] // CHUNK
    ri, ci = grid_index((CHUNK, CHUNK))
    upto = ri >= ci
    for head in range(heads):
        for c in range(chunks):
            at = slice(c * CHUNK, (c + 1) * CHUNK)

            def col(kind):
                lane = kind * heads + head
                return cols[c, :, lane:lane + 1]

            def row(kind):
                lane = kind * heads + head
                return rows_of[c, lane:lane + 1, :]

            q = act[head, at]
            score = dot(q, act[heads + head, at], (1, 1))
            weight = jnp.exp(jnp.minimum(col(0) - row(0), 0.0)) * row(1)
            attend = jnp.where(upto, weight * score * col(2), 0.0).astype(bf16)
            inner = dot(attend, both_ref[head, c])
            eff = (jnp.exp(col(0)) * col(2)) * q.astype(f32) - inner[:, :LANES]
            if c == 0:
                qp_ref[head, at] = eff.astype(bf16)
                o_ref[head, at] = inner[:, LANES:]
            else:
                ahead = dot(eff.astype(bf16), low_ref[head, c - 1])
                qp_ref[head, at] = ahead[:, :LANES].astype(bf16)
                o_ref[head, at] = inner[:, LANES:] + ahead[:, LANES:]


def pair_kernel(share, mine_ref, other_ref, out_ref):
    core = lax.axis_index("seq") & 1
    for j in range(out_ref.shape[0]):
        head = core * out_ref.shape[0] + j if share else j
        mine, other = mine_ref[head], other_ref[head]
        first = jnp.where(core == 0, mine, other)
        second = jnp.where(core == 0, other, mine)
        both = dot(second[:, :LANES], first)
        out_ref[j, :, :LANES] = both[:, :LANES].astype(bf16)
        out_ref[j, :, LANES:] = (both[:, LANES:] + second[:, LANES:].astype(f32)).astype(bf16)


def climb_kernel(bit, inside_ref, block_ref, sent_ref, inside_out, block_out):
    upper = (lax.axis_index("seq") >> (bit + 1)) & 1
    for j in range(block_ref.shape[0]):
        sent = sent_ref[j]
        for ref, out in ((inside_ref, inside_out), (block_ref, block_out)):
            mine = ref[j]
            both = dot(mine[:, :LANES], sent)
            left = jnp.where(upper == 1, both[:, :LANES], mine[:, :LANES].astype(f32))
            right = mine[:, LANES:].astype(f32) + both[:, LANES:]
            out[j] = jnp.concatenate([left, right], axis=1).astype(bf16)


def first_kernel(block_ref, sent_ref, inside_out, block_out):
    upper = (lax.axis_index("seq") >> 1) & 1
    ri, ci = grid_index((LANES, LANES))
    eye = jnp.where(ri == ci, 1.0, 0.0)
    for j in range(block_ref.shape[0]):
        sent, mine = sent_ref[j], block_ref[j]
        both = dot(mine[:, :LANES], sent)
        left = jnp.where(upper == 1, both[:, :LANES], mine[:, :LANES].astype(f32))
        right = mine[:, LANES:].astype(f32) + both[:, LANES:]
        block_out[j] = jnp.concatenate([left, right], axis=1).astype(bf16)
        inside = jnp.where(upper == 1, sent[:, :LANES].astype(f32), eye)
        inside_out[j] = jnp.concatenate([inside.astype(bf16), sent[:, LANES:]], axis=1)


def fold_kernel(inside_ref, *refs):
    out_ref = refs[-1]
    for j in range(out_ref.shape[0]):
        state = refs[0][j]
        for ref in refs[1:-1]:
            state = state + ref[j]
        inside = inside_ref[j]
        state = inside[:, LANES:].astype(f32) + dot(inside[:, :LANES], state)
        out_ref[j] = state.astype(bf16)


def final_kernel(
    share, blocks, qp_ref, o_ref, pair_ref, mine_ref, other_ref,
    own_gate_ref, gate_ref, late_gate_ref, gain_ref, out_ref,
):
    heads, seq_rows, dim = qp_ref.shape
    rows = seq_rows // blocks
    core, me = lax.axis_index("seq") & 1, lax.axis_index("tp")
    part = mine_ref.shape[0]
    for head in range(heads):
        start = mine_ref[head % part]
        if share:
            start = jnp.where(core == head // part, start, other_ref[head % part])
        pair = pair_ref[head]
        moved = pair[:, dim:].astype(f32) + dot(pair[:, :dim], start)
        start = jnp.where(core == 0, start.astype(f32), moved).astype(bf16)
        lanes = slice(head * dim, (head + 1) * dim)
        for m in range(blocks):
            if m == 0:
                gate = own_gate_ref[:, lanes]
            elif m < blocks - 1:
                gate = gate_ref[(m - 1) * rows:m * rows, lanes]
            else:
                gate = late_gate_ref[:, lanes]
            at = pl.ds(pl.multiple_of(lax.bitwise_xor(me, m) * rows, 8), rows)
            y = o_ref[head, at] + dot(qp_ref[head, at], start)
            scale = lax.rsqrt(jnp.mean(y * y, axis=-1, keepdims=True) + EPS)
            out_ref[at, lanes] = (y * scale * gain_ref[...] * gate).astype(bf16)


def call(kernel, out, operands, flops=0, scratch=(), limit=24):
    single = not isinstance(out, tuple)
    return pl.pallas_call(
        kernel,
        out_shape=out,
        in_specs=[whole()] * len(operands),
        out_specs=whole() if single else (whole(),) * len(out),
        scratch_shapes=scratch,
        cost_estimate=pl.CostEstimate(flops=flops, transcendentals=0, bytes_accessed=1 << 20),
        compiler_params=pltpu.CompilerParams(vmem_limit_bytes=limit << 20),
    )(*operands)


def per_device(hidden, w_qkv, w_gate, w_decay_beta, conv_weight, decay_rate, dt_bias, norm_gain):
    heads = decay_rate.shape[0]
    dim = norm_gain.shape[0]
    columns = heads * dim
    blocks = lax.axis_size("tp")
    seq_count = lax.axis_size("seq")
    rows = hidden.shape[0]
    seq_rows = rows * blocks
    chunks = seq_rows // CHUNK
    shape = jax.ShapeDtypeStruct

    w_three = w_qkv.transpose(1, 0, 2)
    small = w_decay_beta.transpose(1, 2, 0)
    taps = conv_weight.transpose(1, 0, 2)
    rate, bias = decay_rate.reshape(1, heads), dt_bias.reshape(1, heads)

    early, late = gather_blocks(hidden, "tp")
    rim = rim_rows(hidden, RIM)
    weights = [w_three, w_gate, small]

    def project(tokens, count, extra=0):
        return call(
            functools.partial(project_kernel, len(tokens)),
            (
                shape((3, count + extra, columns), bf16),
                shape((count, columns), f32),
                shape((count, LANES), f32),
            ),
            [*tokens, *weights], flops=PROJECT_FLOPS, limit=20,
        )

    own_p, own_gate, own_sc = project([hidden], rows)
    mid_p, mid_gate, mid_sc = project([*early, rim], seq_rows - 2 * rows, RIM)
    own, both, low, act, cols, rows_of = call(
        functools.partial(delta_kernel, heads, blocks),
        (
            shape((heads, dim, 2 * dim), bf16),
            shape((heads, chunks, CHUNK, 2 * dim), bf16),
            shape((heads, chunks - 1, dim, 2 * dim), bf16),
            shape((3 * heads, seq_rows, dim), bf16),
            shape((chunks, CHUNK, LANES), f32),
            shape((chunks, CHUNK, LANES), f32),
        ),
        [own_p, own_sc, mid_p, mid_sc, *late, w_three, small, taps, rate, bias],
        flops=DELTA_FLOPS, limit=32,
        scratch=[
            pltpu.VMEM((3 * heads, seq_rows + RIM, dim), f32),
            pltpu.VMEM((seq_rows, LANES), f32),
            pltpu.VMEM((CHUNK.bit_length() - 1, CHUNK, 2 * CHUNK), bf16),
            pltpu.VMEM((heads * chunks // 2, CHUNK, 2 * CHUNK), bf16),
            pltpu.VMEM((heads * chunks // 2, CHUNK, 2 * CHUNK), f32),
        ],
    )
    reach, base, late_gate = call(
        functools.partial(reach_kernel, heads),
        (
            shape((heads, seq_rows, dim), bf16),
            shape((heads, seq_rows, dim), f32),
            shape((rows, columns), f32),
        ),
        [both, low, act, cols, rows_of, *late, w_gate], flops=REACH_FLOPS, limit=12,
    )

    share = heads % 2 == 0
    part = heads // 2 if share else heads
    swap = [(i, i ^ 1) for i in range(seq_count)]
    other = lax.ppermute(own, "seq", swap)
    block = call(
        functools.partial(pair_kernel, share),
        shape((part, dim, 2 * dim), bf16), [own, other], flops=SMALL_FLOPS, limit=4,
    )
    chips = seq_count // 2
    levels = chips.bit_length() - 1
    inside = None
    for level in range(levels):
        size = 1 << level
        sent = block if level < levels - 1 or level == 0 else block[:, :, dim:]
        parts = []
        for target in range(size):
            route = []
            for top in range(size - 1, chips, 2 * size):
                for c in range(2):
                    route.append((2 * top + c, 2 * (top + 1 + target) + c))
            parts.append(lax.ppermute(sent, "seq", route))
        if level == levels - 1 and level > 0:
            break
        sent = sum(parts[1:], parts[0])
        kernel, operands = first_kernel, [block, sent]
        if level > 0:
            kernel, operands = functools.partial(climb_kernel, level), [inside, block, sent]
        inside, block = call(
            kernel, (shape(block.shape, bf16),) * 2, operands, flops=SMALL_FLOPS, limit=4,
        )
    state = call(
        fold_kernel, shape((part, dim, dim), bf16), [inside, *parts],
        flops=SMALL_FLOPS, limit=4,
    )
    back = lax.ppermute(state, "seq", swap) if share else state
    return call(
        functools.partial(final_kernel, share, blocks), shape((seq_rows, columns), bf16),
        [reach, base, other, state, back, own_gate, mid_gate, late_gate, norm_gain.reshape(1, dim)],
        flops=SMALL_FLOPS, limit=12,
    )


def solution(mesh):
    return jax.shard_map(
        per_device,
        mesh=mesh,
        in_specs=(
            P(("seq", "tp"), None),
            P(None, None, "tp"),
            P(None, "tp"),
            P(None, None, "tp"),
            P(None, None, "tp"),
            P("tp"),
            P("tp"),
            P(),
        ),
        out_specs=P("seq", "tp"),
        check_vma=False,
    )
```

```python
import functools
import math

import jax
import jax.numpy as jnp
from jax import lax
from jax.experimental import pallas as pl
from jax.experimental.pallas import tpu as pltpu
from jax.sharding import PartitionSpec as P


CHUNK = 128
LANES = 128
RIM = 16
EPS = 1e-6
PROJECT_FLOPS = 3000000000
DELTA_FLOPS = 3000000000
REACH_FLOPS = 2000000000
SMALL_FLOPS = 50000000
MASKS_FLOPS = 8000000000


f32 = jnp.float32
bf16 = jnp.bfloat16


def dot(left, right, contract=(1, 0), precision=None):
    dims = (((contract[0],), (contract[1],)), ((), ()))
    return lax.dot_general(left, right, dims, precision=precision, preferred_element_type=f32)


def whole(memory=pltpu.VMEM):
    return pl.BlockSpec(memory_space=memory)


def gather_blocks(block, axis):
    count = lax.axis_size(axis)
    bits = count.bit_length() - 1
    half = block.shape[0] // 2

    def swap(value, bit):
        step = 1 << bit
        return lax.ppermute(value, axis, [(i, i ^ step) for i in range(count)])

    found = {0: block}
    for bit in range(bits):
        found[1 << bit] = swap(block, bit)
    halves = []
    for number, order in enumerate((range(bits), range(bits - 1, -1, -1))):
        part = {m: value[number * half:(number + 1) * half] for m, value in found.items()}
        for bit in order:
            for mask in list(part):
                if mask | (1 << bit) not in part:
                    part[mask | (1 << bit)] = swap(part[mask], bit)
        halves.append(part)
    early = [found[m] if m in found else (halves[0][m], halves[1][m]) for m in range(count - 1)]
    flat = []
    for item in early[1:]:
        flat.extend(item if isinstance(item, tuple) else (item,))
    return flat, [halves[0][count - 1], halves[1][count - 1]]


def rim_rows(block, count):
    seq_count, tp_count = lax.axis_size("seq"), lax.axis_size("tp")
    tail = block[-count:]
    parts = []
    for j in range(tp_count):
        route = [(s * tp_count - 1, s * tp_count + j) for s in range(1, seq_count)]
        parts.append(lax.ppermute(tail, ("seq", "tp"), route))
    route = [(i, tp_count - 1 - i) for i in range(tp_count)]
    across = lax.ppermute(tail, "tp", route)
    return parts, across


def silu(x):
    return x / (1.0 + jnp.exp(-x))


def scalar_weights(ref):
    kinds, heads, width = ref.shape
    rows = [ref[kind].astype(f32) for kind in range(kinds)]
    rows.append(jnp.zeros((LANES - kinds * heads, width), f32))
    return jnp.concatenate(rows, axis=0).astype(bf16)


def lane_row(ref):
    lane = lax.broadcasted_iota(jnp.int32, (1, LANES), 1)
    row = jnp.zeros((1, LANES), f32)
    for head in range(ref.shape[1]):
        row = jnp.where(lane == head, ref[:, head:head + 1], row)
    return row


def project_kernel(count, *refs):
    blocks = refs[:count]
    w_ref, gate_w_ref, small_ref = refs[count:count + 3]
    p_ref, gate_ref, sc_ref = refs[count + 3:count + 6]
    rows = sc_ref.shape[0]
    tokens = jnp.concatenate([ref[...] for ref in blocks], axis=0)
    sc_ref[...] = dot(tokens, scalar_weights(small_ref), (1, 1))[:rows]
    gate_ref[...] = silu(dot(tokens, gate_w_ref[...])[:rows])

    def one(branch, carry):
        p_ref[branch] = dot(tokens, w_ref[branch]).astype(bf16)
        return carry

    lax.fori_loop(0, w_ref.shape[0], one, 0)


def block_diagonal(left, right):
    hole = jnp.zeros_like(left)
    return jnp.concatenate(
        [jnp.concatenate([left, hole], axis=1), jnp.concatenate([hole, right], axis=1)], axis=0
    )


def beside(left, right):
    return jnp.concatenate([left, right], axis=1)


def grid_index(shape):
    return lax.broadcasted_iota(jnp.int32, shape, 0), lax.broadcasted_iota(jnp.int32, shape, 1)


def delta_kernel(
    heads, blocks, own_ref, own_sc_ref, p_ref, sc_ref, late0_ref, late1_ref, w_ref,
    small_ref, taps_ref, rate_ref, bias_ref, x_ref, both_ref, low_ref, act, cols, rows_of,
    xp, sc, masks, mixes, solves,
):
    seq_rows = act.shape[1]
    rows = seq_rows // blocks
    chunks = seq_rows // CHUNK
    taps = taps_ref.shape[1]
    me = lax.axis_index("tp")

    def place(m, offset=0):
        return pl.multiple_of(offset + lax.bitwise_xor(me, m) * rows, 8)

    late = jnp.concatenate([late0_ref[...], late1_ref[...]], axis=0)
    sc[pl.ds(place(blocks - 1), rows)] = dot(late, scalar_weights(small_ref), (1, 1))
    sc[pl.ds(place(0), rows)] = own_sc_ref[...]
    for m in range(1, blocks - 1):
        sc[pl.ds(place(m), rows)] = sc_ref[(m - 1) * rows:m * rows]

    def fill(branch, carry):
        made = dot(late, w_ref[branch]).astype(bf16).astype(f32)
        for head in range(heads):
            tile = branch * heads + head
            lanes = slice(head * LANES, (head + 1) * LANES)
            xp[tile, :RIM] = p_ref[branch, (blocks - 2) * rows:, lanes].astype(f32)
            xp[tile, pl.ds(place(0, RIM), rows)] = own_ref[branch, :, lanes].astype(f32)
            xp[tile, pl.ds(place(blocks - 1, RIM), rows)] = made[:, lanes]
            for m in range(1, blocks - 1):
                block = p_ref[branch, (m - 1) * rows:m * rows, lanes]
                xp[tile, pl.ds(place(m, RIM), rows)] = block.astype(f32)
        return carry

    lax.fori_loop(0, 3, fill, 0)

    ri, ci = grid_index((CHUNK, CHUNK))
    upto = ri >= ci
    lower = upto.astype(f32)
    levels = CHUNK.bit_length() - 1
    for level in range(levels):
        hit = ((ri >> (level + 1)) == (ci >> (level + 1))) & ((ri >> level) > (ci >> level))
        hit = hit.astype(f32).astype(bf16)
        masks[level] = beside(hit, hit)

    root = 1.0 / math.sqrt(LANES)
    rate, bias = -lane_row(rate_ref), lane_row(bias_ref)

    def prepare(chunk, carry):
        base = pl.multiple_of(chunk * CHUNK, CHUNK)
        raw = sc[pl.ds(base, CHUNK)]
        shifted = raw + bias
        soft = jnp.maximum(shifted, 0.0) + jnp.log1p(jnp.exp(-jnp.abs(shifted)))
        decay = dot(lower, rate * soft, precision=lax.Precision.HIGHEST)
        beta = 1.0 / (1.0 + jnp.exp(-raw))
        comb = jnp.where(ci < heads, decay, 0.0)
        for head in range(heads):
            norms = []
            for branch in range(3):
                tile = branch * heads + head
                weights = taps_ref[branch, :, head * LANES:(head + 1) * LANES].astype(f32)
                total = None
                for i in range(taps):
                    term = xp[tile, pl.ds(base + (RIM - taps + 1 + i), CHUNK)] * weights[i:i + 1]
                    total = term if total is None else total + term
                value = silu(total).astype(bf16)
                act[tile, pl.ds(base, CHUNK)] = value
                if branch < 2:
                    wide = value.astype(f32)
                    norms.append(lax.rsqrt(jnp.sum(wide * wide, axis=-1, keepdims=True) + EPS))
            scaled = beta[:, heads + head:heads + head + 1] * norms[1]
            comb = jnp.where(ci == heads + head, scaled, comb)
            comb = jnp.where(ci == 2 * heads + head, norms[0] * root, comb)
            comb = jnp.where(ci == 3 * heads + head, norms[1], comb)
        cols[chunk] = comb
        rows_of[chunk] = comb.T
        return carry

    lax.fori_loop(0, chunks, prepare, 0)

    def part(branch, head, chunk):
        return act[branch * heads + head, chunk * CHUNK:(chunk + 1) * CHUNK]

    def col(kind, head, chunk):
        lane = kind * heads + head
        return cols[chunk, :, lane:lane + 1]

    def row(kind, head, chunk):
        lane = kind * heads + head
        return rows_of[chunk, lane:lane + 1, :]

    sets = [(head, chunk) for head in range(heads) for chunk in range(0, chunks, 2)]
    for s, (head, first) in enumerate(sets):
        two = (first, first + 1)
        keys = [part(1, head, c) for c in two]
        gram = dot(beside(*keys), block_diagonal(*[k.T for k in keys]))
        mix = []
        for i, c in enumerate(two):
            lanes = slice(i * LANES, (i + 1) * LANES)
            gap = col(0, head, c) - row(0, head, c)
            weight = jnp.exp(jnp.minimum(gap, 0.0)) * row(1, head, c)
            mix.append((weight * gram[:, lanes] * col(3, head, c)).astype(bf16))
        mix = beside(*mix)
        mixes[s] = mix
        eye = jnp.where(ri == ci, 1.0, 0.0)
        solves[s] = beside(eye, eye) - (mix * masks[0]).astype(f32)
    for level in range(1, levels):
        lows, mids = [], []
        for s in range(len(sets)):
            low = solves[s].astype(bf16)
            lows.append(low)
            mids.append(dot(mixes[s] * masks[level], block_diagonal(low[:, :LANES], low[:, LANES:])).astype(bf16))
        for s in range(len(sets)):
            mid = mids[s]
            solves[s] = solves[s] - dot(lows[s], block_diagonal(mid[:, :LANES], mid[:, LANES:]))
    change = {}
    for s, (head, first) in enumerate(sets):
        two = (first, first + 1)
        solve = solves[s]
        new = dot(solve.astype(bf16), block_diagonal(*[part(2, head, c) for c in two]))
        grown = beside(*[jnp.exp(row(0, head, c)) * row(3, head, c) for c in two])
        back = dot((solve * grown).astype(bf16), block_diagonal(*[part(1, head, c) for c in two]))
        for i, c in enumerate(two):
            lanes = slice(i * LANES, (i + 1) * LANES)
            both = beside(back[:, lanes], new[:, lanes])
            decay = col(0, head, c)
            tail = col(1, head, c) * jnp.exp(decay[CHUNK - 1:] - decay)
            change[head, c] = dot(part(1, head, c), (both * tail).astype(bf16), (0, 0))
            both_ref[head, c] = both.astype(bf16)
    runs = {}
    for c in range(chunks):
        for head in range(heads):
            last = jnp.exp(col(0, head, c)[CHUNK - 1:])
            if c == 0:
                runs[head] = beside(
                    jnp.where(ri == ci, last, 0.0) - change[head, c][:, :LANES], change[head, c][:, LANES:]
                )
            else:
                low = runs[head].astype(bf16)
                low_ref[head, c - 1] = low
                run = last * runs[head] - dot(change[head, c][:, :LANES].astype(bf16), low)
                runs[head] = beside(run[:, :LANES], run[:, LANES:] + change[head, c][:, LANES:])
    for head in range(heads):
        x_ref[head] = runs[head].astype(bf16)


def reach_kernel(
    heads, both_ref, low_ref, act, cols, rows_of, late0_ref, late1_ref, gate_w_ref,
    qp_ref, o_ref, gate_ref,
):
    late = jnp.concatenate([late0_ref[...], late1_ref[...]], axis=0)
    gate_ref[...] = silu(dot(late, gate_w_ref[...]))
    chunks = act.shape[1] // CHUNK
    ri, ci = grid_index((CHUNK, CHUNK))
    upto = ri >= ci
    for head in range(heads):
        for c in range(chunks):
            at = slice(c * CHUNK, (c + 1) * CHUNK)

            def col(kind):
                lane = kind * heads + head
                return cols[c, :, lane:lane + 1]

            def row(kind):
                lane = kind * heads + head
                return rows_of[c, lane:lane + 1, :]

            q = act[head, at]
            score = dot(q, act[heads + head, at], (1, 1))
            weight = jnp.exp(jnp.minimum(col(0) - row(0), 0.0)) * row(1)
            attend = jnp.where(upto, weight * score * col(2), 0.0).astype(bf16)
            inner = dot(attend, both_ref[head, c])
            eff = (jnp.exp(col(0)) * col(2)) * q.astype(f32) - inner[:, :LANES]
            if c == 0:
                qp_ref[head, at] = eff.astype(bf16)
                o_ref[head, at] = inner[:, LANES:]
            else:
                ahead = dot(eff.astype(bf16), low_ref[head, c - 1])
                qp_ref[head, at] = ahead[:, :LANES].astype(bf16)
                o_ref[head, at] = inner[:, LANES:] + ahead[:, LANES:]


def convolve(heads, xp, base, taps_ref, raw, rate, bias, keep):
    ri, ci = grid_index((CHUNK, CHUNK))
    taps = taps_ref.shape[1]
    shifted = raw + bias
    soft = jnp.maximum(shifted, 0.0) + jnp.log1p(jnp.exp(-jnp.abs(shifted)))
    decay = dot((ri >= ci).astype(f32), rate * soft, precision=lax.Precision.HIGHEST)
    beta = 1.0 / (1.0 + jnp.exp(-raw))
    comb = jnp.where(ci < heads, decay, 0.0)
    root = 1.0 / math.sqrt(LANES)
    for head in range(heads):
        norms = []
        for branch in range(3):
            tile = branch * heads + head
            weights = taps_ref[branch, :, head * LANES:(head + 1) * LANES].astype(f32)
            total = None
            for i in range(taps):
                term = xp[tile, pl.ds(base + (RIM - taps + 1 + i), CHUNK)] * weights[i:i + 1]
                total = term if total is None else total + term
            value = silu(total).astype(bf16)
            keep(tile, value)
            if branch < 2:
                wide = value.astype(f32)
                norms.append(lax.rsqrt(jnp.sum(wide * wide, axis=-1, keepdims=True) + EPS))
        scaled = beta[:, heads + head:heads + head + 1] * norms[1]
        comb = jnp.where(ci == heads + head, scaled, comb)
        comb = jnp.where(ci == 2 * heads + head, norms[0] * root, comb)
        comb = jnp.where(ci == 3 * heads + head, norms[1], comb)
    return comb


def early_kernel(heads, blocks, *refs):
    count = blocks + 1
    tokens_refs, part_ref = refs[:blocks], refs[blocks]
    w_ref, small_ref, taps_ref, rate_ref, bias_ref = refs[count:count + 5]
    act, cols, rows_of, raw_ref, raw_sc_ref, rims_ref, xp, tails = refs[count + 5:]
    early = blocks - 1
    mid = early * CHUNK
    me = lax.axis_index("tp")
    tokens = jnp.concatenate([ref[...] for ref in tokens_refs] + [part_ref[...]], axis=0)
    raw = dot(tokens[:mid], scalar_weights(small_ref), (1, 1))
    later = [m for m in range(early) if m != 1]
    for slot, m in enumerate(later):
        raw_sc_ref[slot * CHUNK:(slot + 1) * CHUNK] = raw[m * CHUNK:(m + 1) * CHUNK]

    def fill(branch, carry):
        made = dot(tokens, w_ref[branch]).astype(bf16).astype(f32)
        for head in range(heads):
            tile = branch * heads + head
            lanes = slice(head * LANES, (head + 1) * LANES)
            for m in range(early):
                block = made[m * CHUNK:(m + 1) * CHUNK, lanes]
                if m == 1:
                    xp[tile, RIM:] = block
                else:
                    slot = later.index(m)
                    raw_ref[tile, slot * CHUNK:(slot + 1) * CHUNK] = block
                tails[m, tile] = block[CHUNK - RIM:]
            tails[early, tile] = made[mid:mid + RIM, lanes]
            tails[blocks, tile] = made[mid + RIM:, lanes]
        return carry

    lax.fori_loop(0, 3, fill, 0)
    rate, bias = -lane_row(rate_ref), lane_row(bias_ref)

    def ahead_of(m):
        index = lax.bitwise_xor(me, m)
        return jnp.where(index == 0, blocks, lax.bitwise_xor(me, jnp.maximum(index - 1, 0)))

    for slot, m in enumerate(later + [early]):
        rims_ref[slot] = tails[ahead_of(m)]
    source = ahead_of(1)
    for tile in range(3 * heads):
        xp[tile, :RIM] = tails[source, tile]

    def prepare(slot, carry):
        def keep(tile, value):
            act[tile] = value

        base = pl.multiple_of(slot * CHUNK, CHUNK)
        comb = convolve(heads, xp, base, taps_ref, raw[CHUNK:2 * CHUNK], rate, bias, keep)
        cols[0] = comb
        rows_of[0] = comb.T
        return carry

    prepare(0, 0)


def masks_kernel(out_ref):
    ri, ci = grid_index((CHUNK, CHUNK))
    for level in range(out_ref.shape[0]):
        hit = ((ri >> (level + 1)) == (ci >> (level + 1))) & ((ri >> level) > (ci >> level))
        hit = hit.astype(f32).astype(bf16)
        out_ref[level] = beside(hit, hit)


def block_delta_kernel(
    heads, blocks, act_e, cols_e, rows_e, raw_ref, raw_sc_ref, rims_ref, late0_ref, late1_ref, *refs
):
    me = lax.axis_index("tp")
    part_refs = refs[:blocks - 1]
    w_ref, small_ref, taps_ref, rate_ref, bias_ref, masks = refs[blocks - 1:blocks + 5]
    x_ref, both_ref, low_ref, act_l, cols_l, rows_l = refs[blocks + 5:blocks + 11]
    xp, sc, mixes, solves, changes, lasts = refs[blocks + 11:]
    span = RIM + CHUNK
    slots = blocks - 1
    before = part_refs[0][...].astype(f32)
    for ref in part_refs[1:]:
        before = before + ref[...].astype(f32)
    tokens = jnp.concatenate([late0_ref[...], late1_ref[...], before.astype(bf16)], axis=0)
    sc[:(slots - 1) * CHUNK] = raw_sc_ref[...]
    sc[(slots - 1) * CHUNK:] = dot(tokens[:CHUNK], scalar_weights(small_ref), (1, 1))

    def fill(branch, carry):
        made = dot(tokens, w_ref[branch]).astype(bf16).astype(f32)
        for head in range(heads):
            tile = branch * heads + head
            lanes = slice(head * LANES, (head + 1) * LANES)
            rim = made[CHUNK:, lanes]
            for slot in range(slots):
                at = slot * span
                first = me == (slot + 1 if slot else 0)
                xp[tile, at:at + RIM] = jnp.where(first, rim, rims_ref[slot, tile])
                if slot == slots - 1:
                    xp[tile, at + RIM:at + span] = made[:CHUNK, lanes]
                else:
                    xp[tile, at + RIM:at + span] = raw_ref[tile, slot * CHUNK:(slot + 1) * CHUNK]
        return carry

    lax.fori_loop(0, 3, fill, 0)
    rate, bias = -lane_row(rate_ref), lane_row(bias_ref)

    def prepare(slot, carry):
        at = pl.ds(pl.multiple_of(slot * CHUNK, CHUNK), CHUNK)

        def keep(tile, value):
            act_l[tile, at] = value

        base = pl.multiple_of(slot * span, 8)
        comb = convolve(heads, xp, base, taps_ref, sc[at], rate, bias, keep)
        cols_l[slot] = comb
        rows_l[slot] = comb.T
        return carry

    lax.fori_loop(0, slots, prepare, 0)

    ri, ci = grid_index((CHUNK, CHUNK))
    levels = masks.shape[0]

    def part(branch, head, m):
        held, slot = (act_e, 0) if m == 1 else (act_l, max(m - 1, 0))
        return held[branch * heads + head, slot * CHUNK:(slot + 1) * CHUNK]

    def col(kind, head, m):
        lane = kind * heads + head
        held, slot = (cols_e, 0) if m == 1 else (cols_l, max(m - 1, 0))
        return held[slot, :, lane:lane + 1]

    def row(kind, head, m):
        lane = kind * heads + head
        held, slot = (rows_e, 0) if m == 1 else (rows_l, max(m - 1, 0))
        return held[slot, lane:lane + 1, :]

    for m in range(blocks):
        held, slot = (cols_e, 0) if m == 1 else (cols_l, max(m - 1, 0))
        lasts[m] = jnp.exp(held[slot, CHUNK - 8:])

    sets = [(head, m) for m in range(0, blocks, 2) for head in range(heads)]
    for s, (head, first) in enumerate(sets):
        two = (first, first + 1)
        keys = [part(1, head, m) for m in two]
        gram = dot(beside(*keys), block_diagonal(*[k.T for k in keys]))
        mix = []
        for i, m in enumerate(two):
            lanes = slice(i * LANES, (i + 1) * LANES)
            gap = col(0, head, m) - row(0, head, m)
            weight = jnp.exp(jnp.minimum(gap, 0.0)) * row(1, head, m)
            mix.append((weight * gram[:, lanes] * col(3, head, m)).astype(bf16))
        mix = beside(*mix)
        mixes[s] = mix
        eye = jnp.where(ri == ci, 1.0, 0.0)
        solves[s] = beside(eye, eye) - (mix * masks[0]).astype(f32)
    for level in range(1, levels):
        lows, mids = [], []
        for s in range(len(sets)):
            low = solves[s].astype(bf16)
            lows.append(low)
            mids.append(dot(mixes[s] * masks[level], block_diagonal(low[:, :LANES], low[:, LANES:])).astype(bf16))
        for s in range(len(sets)):
            mid = mids[s]
            solves[s] = solves[s] - dot(lows[s], block_diagonal(mid[:, :LANES], mid[:, LANES:]))
    for s, (head, first) in enumerate(sets):
        two = (first, first + 1)
        solve = solves[s]
        new = dot(solve.astype(bf16), block_diagonal(*[part(2, head, m) for m in two]))
        grown = beside(*[jnp.exp(row(0, head, m)) * row(3, head, m) for m in two])
        back = dot((solve * grown).astype(bf16), block_diagonal(*[part(1, head, m) for m in two]))
        for i, m in enumerate(two):
            lanes = slice(i * LANES, (i + 1) * LANES)
            both = beside(back[:, lanes], new[:, lanes])
            decay = col(0, head, m)
            tail = col(1, head, m) * jnp.exp(decay[CHUNK - 1:] - decay)
            changes[m, head] = dot(part(1, head, m), (both * tail).astype(bf16), (0, 0))
            both_ref[head, m] = both.astype(bf16)
    eye = jnp.where(ri == ci, 1.0, 0.0)
    runs = {}
    for step in range(blocks):
        m = lax.bitwise_xor(me, step)
        for head in range(heads):
            last = lasts[m, 7:, head:head + 1]
            change = changes[m, head]
            if step == 0:
                low_ref[head, m] = beside(eye, jnp.zeros_like(eye)).astype(bf16)
                runs[head] = beside(last * eye - change[:, :LANES], change[:, LANES:])
            else:
                low = runs[head].astype(bf16)
                low_ref[head, m] = low
                run = last * runs[head] - dot(change[:, :LANES].astype(bf16), low)
                runs[head] = beside(run[:, :LANES], run[:, LANES:] + change[:, LANES:])
    for head in range(heads):
        x_ref[head] = runs[head].astype(bf16)


def block_reach_kernel(
    heads, blocks, both_ref, low_ref, act_e, cols_e, rows_e, act_l, cols_l, rows_l,
    qp_ref, o_ref,
):
    ri, ci = grid_index((CHUNK, CHUNK))
    upto = ri >= ci
    for head in range(heads):
        for m in range(blocks):
            at = slice(m * CHUNK, (m + 1) * CHUNK)
            slot = 0 if m == 1 else max(m - 1, 0)
            act, cols_of, rows_of = (act_e, cols_e, rows_e) if m == 1 else (act_l, cols_l, rows_l)
            held = slice(slot * CHUNK, (slot + 1) * CHUNK)
            cols, rows = cols_of[slot], rows_of[slot]
            q, k = act[head, held], act[heads + head, held]
            decay = cols[:, head:head + 1]
            norm = cols[:, 2 * heads + head:2 * heads + head + 1]
            gap = decay - rows[head:head + 1]
            weight = jnp.exp(jnp.minimum(gap, 0.0)) * rows[heads + head:heads + head + 1]
            attend = jnp.where(upto, weight * dot(q, k, (1, 1)) * norm, 0.0).astype(bf16)
            inner = dot(attend, both_ref[head, m])
            eff = (jnp.exp(decay) * norm) * q.astype(f32) - inner[:, :LANES]
            ahead = dot(eff.astype(bf16), low_ref[head, m])
            qp_ref[head, at] = ahead[:, :LANES].astype(bf16)
            o_ref[head, at] = inner[:, LANES:] + ahead[:, LANES:]


def gate_kernel(count, *refs):
    w_ref = refs[count]
    outs = refs[count + 1:]
    tokens = jnp.concatenate([ref[...] for ref in refs[:count]], axis=0)
    gate = silu(dot(tokens, w_ref[...]))
    start = 0
    for out in outs:
        out[...] = gate[start:start + out.shape[0]]
        start += out.shape[0]


def pair_kernel(share, mine_ref, other_ref, out_ref):
    core = lax.axis_index("seq") & 1
    for j in range(out_ref.shape[0]):
        head = core * out_ref.shape[0] + j if share else j
        mine, other = mine_ref[head], other_ref[head]
        first = jnp.where(core == 0, mine, other)
        second = jnp.where(core == 0, other, mine)
        both = dot(second[:, :LANES], first)
        out_ref[j, :, :LANES] = both[:, :LANES].astype(bf16)
        out_ref[j, :, LANES:] = (both[:, LANES:] + second[:, LANES:].astype(f32)).astype(bf16)


def climb_kernel(bit, inside_ref, block_ref, sent_ref, inside_out, block_out):
    upper = (lax.axis_index("seq") >> (bit + 1)) & 1
    for j in range(block_ref.shape[0]):
        sent = sent_ref[j]
        for ref, out in ((inside_ref, inside_out), (block_ref, block_out)):
            mine = ref[j]
            both = dot(mine[:, :LANES], sent)
            left = jnp.where(upper == 1, both[:, :LANES], mine[:, :LANES].astype(f32))
            right = mine[:, LANES:].astype(f32) + both[:, LANES:]
            out[j] = jnp.concatenate([left, right], axis=1).astype(bf16)


def first_kernel(block_ref, sent_ref, inside_out, block_out):
    upper = (lax.axis_index("seq") >> 1) & 1
    ri, ci = grid_index((LANES, LANES))
    eye = jnp.where(ri == ci, 1.0, 0.0)
    for j in range(block_ref.shape[0]):
        sent, mine = sent_ref[j], block_ref[j]
        both = dot(mine[:, :LANES], sent)
        left = jnp.where(upper == 1, both[:, :LANES], mine[:, :LANES].astype(f32))
        right = mine[:, LANES:].astype(f32) + both[:, LANES:]
        block_out[j] = jnp.concatenate([left, right], axis=1).astype(bf16)
        inside = jnp.where(upper == 1, sent[:, :LANES].astype(f32), eye)
        inside_out[j] = jnp.concatenate([inside.astype(bf16), sent[:, LANES:]], axis=1)


def fold_kernel(inside_ref, *refs):
    out_ref = refs[-1]
    for j in range(out_ref.shape[0]):
        state = refs[0][j]
        for ref in refs[1:-1]:
            state = state + ref[j]
        inside = inside_ref[j]
        state = inside[:, LANES:].astype(f32) + dot(inside[:, :LANES], state)
        out_ref[j] = state.astype(bf16)


def final_kernel(
    share, blocks, ordered, qp_ref, o_ref, pair_ref, mine_ref, other_ref,
    own_gate_ref, gate_ref, late_gate_ref, gain_ref, out_ref,
):
    heads, seq_rows, dim = qp_ref.shape
    rows = seq_rows // blocks
    core, me = lax.axis_index("seq") & 1, lax.axis_index("tp")
    part = mine_ref.shape[0]
    for head in range(heads):
        start = mine_ref[head % part]
        if share:
            start = jnp.where(core == head // part, start, other_ref[head % part])
        pair = pair_ref[head]
        moved = pair[:, dim:].astype(f32) + dot(pair[:, :dim], start)
        start = jnp.where(core == 0, start.astype(f32), moved).astype(bf16)
        lanes = slice(head * dim, (head + 1) * dim)
        for m in range(blocks):
            if m == 0:
                gate = own_gate_ref[:, lanes]
            elif m < blocks - 1:
                gate = gate_ref[(m - 1) * rows:m * rows, lanes]
            else:
                gate = late_gate_ref[:, lanes]
            at = pl.ds(pl.multiple_of(lax.bitwise_xor(me, m) * rows, 8), rows)
            held = at if ordered else slice(m * rows, (m + 1) * rows)
            y = o_ref[head, held] + dot(qp_ref[head, held], start)
            scale = lax.rsqrt(jnp.mean(y * y, axis=-1, keepdims=True) + EPS)
            out_ref[at, lanes] = (y * scale * gain_ref[...] * gate).astype(bf16)


def call(kernel, out, operands, flops=0, scratch=(), limit=24):
    single = not isinstance(out, tuple)
    return pl.pallas_call(
        kernel,
        out_shape=out,
        in_specs=[whole()] * len(operands),
        out_specs=whole() if single else (whole(),) * len(out),
        scratch_shapes=scratch,
        cost_estimate=pl.CostEstimate(flops=flops, transcendentals=0, bytes_accessed=1 << 20),
        compiler_params=pltpu.CompilerParams(vmem_limit_bytes=limit << 20),
    )(*operands)


def per_device(hidden, w_qkv, w_gate, w_decay_beta, conv_weight, decay_rate, dt_bias, norm_gain):
    heads = decay_rate.shape[0]
    dim = norm_gain.shape[0]
    columns = heads * dim
    blocks = lax.axis_size("tp")
    seq_count = lax.axis_size("seq")
    rows = hidden.shape[0]
    seq_rows = rows * blocks
    chunks = seq_rows // CHUNK
    shape = jax.ShapeDtypeStruct

    w_three = w_qkv.transpose(1, 0, 2)
    small = w_decay_beta.transpose(1, 2, 0)
    taps = conv_weight.transpose(1, 0, 2)
    rate, bias = decay_rate.reshape(1, heads), dt_bias.reshape(1, heads)

    early, late = gather_blocks(hidden, "tp")
    weights = [w_three, w_gate, small]

    def project(tokens, count, extra=0):
        return call(
            functools.partial(project_kernel, len(tokens)),
            (
                shape((3, count + extra, columns), bf16),
                shape((count, columns), f32),
                shape((count, LANES), f32),
            ),
            [*tokens, *weights], flops=PROJECT_FLOPS, limit=20,
        )

    by_block = rows == CHUNK and len(early) == blocks - 2 and blocks > 2
    if by_block:
        parts, across = rim_rows(hidden, RIM)
        masks = call(
            masks_kernel,
            shape((CHUNK.bit_length() - 1, CHUNK, 2 * CHUNK), bf16), [],
            flops=MASKS_FLOPS, limit=4,
        )
        act_e, cols_e, rows_e, raw, raw_sc, rims = call(
            functools.partial(early_kernel, heads, blocks),
            (
                shape((3 * heads, rows, dim), bf16),
                shape((1, CHUNK, LANES), f32),
                shape((1, CHUNK, LANES), f32),
                shape((3 * heads, seq_rows - 2 * rows, dim), f32),
                shape((seq_rows - 2 * rows, LANES), f32),
                shape((blocks - 1, 3 * heads, RIM, dim), f32),
            ),
            [
                hidden, *early, across, parts[1],
                w_three, small, taps, rate, bias,
            ],
            flops=PROJECT_FLOPS,
            scratch=[
                pltpu.VMEM((3 * heads, RIM + CHUNK, dim), f32),
                pltpu.VMEM((blocks + 1, 3 * heads, RIM, dim), f32),
            ],
        )
        own, both, low, act_l, cols_l, rows_l = call(
            functools.partial(block_delta_kernel, heads, blocks),
            (
                shape((heads, dim, 2 * dim), bf16),
                shape((heads, blocks, CHUNK, 2 * dim), bf16),
                shape((heads, blocks, dim, 2 * dim), bf16),
                shape((3 * heads, seq_rows - rows, dim), bf16),
                shape((blocks - 1, CHUNK, LANES), f32),
                shape((blocks - 1, CHUNK, LANES), f32),
            ),
            [
                act_e, cols_e, rows_e, raw, raw_sc, rims, *late,
                parts[0], *parts[2:], w_three, small, taps, rate, bias, masks,
            ],
            flops=DELTA_FLOPS, limit=28,
            scratch=[
                pltpu.VMEM((3 * heads, (blocks - 1) * (RIM + CHUNK), dim), f32),
                pltpu.VMEM((seq_rows - rows, LANES), f32),
                pltpu.VMEM((heads * blocks // 2, CHUNK, 2 * CHUNK), bf16),
                pltpu.VMEM((heads * blocks // 2, CHUNK, 2 * CHUNK), f32),
                pltpu.VMEM((blocks, heads, dim, 2 * dim), f32),
                pltpu.VMEM((blocks, 8, LANES), f32),
            ],
        )
        reach, base = call(
            functools.partial(block_reach_kernel, heads, blocks),
            (
                shape((heads, seq_rows, dim), bf16),
                shape((heads, seq_rows, dim), f32),
            ),
            [both, low, act_e, cols_e, rows_e, act_l, cols_l, rows_l],
            flops=REACH_FLOPS, limit=14,
        )
        tokens = [hidden, *early, *late]
        own_gate, mid_gate, late_gate = call(
            functools.partial(gate_kernel, len(tokens)),
            (
                shape((rows, columns), f32),
                shape((seq_rows - 2 * rows, columns), f32),
                shape((rows, columns), f32),
            ),
            [*tokens, w_gate], flops=PROJECT_FLOPS, limit=14,
        )
    else:
        own_p, own_gate, own_sc = project([hidden], rows)
        parts, _ = rim_rows(hidden, RIM)
        rim = sum(parts[1:], parts[0])
        mid_p, mid_gate, mid_sc = project([*early, rim], seq_rows - 2 * rows, RIM)
        own, both, low, act, cols, rows_of = call(
            functools.partial(delta_kernel, heads, blocks),
            (
                shape((heads, dim, 2 * dim), bf16),
                shape((heads, chunks, CHUNK, 2 * dim), bf16),
                shape((heads, chunks - 1, dim, 2 * dim), bf16),
                shape((3 * heads, seq_rows, dim), bf16),
                shape((chunks, CHUNK, LANES), f32),
                shape((chunks, CHUNK, LANES), f32),
            ),
            [own_p, own_sc, mid_p, mid_sc, *late, w_three, small, taps, rate, bias],
            flops=DELTA_FLOPS, limit=32,
            scratch=[
                pltpu.VMEM((3 * heads, seq_rows + RIM, dim), f32),
                pltpu.VMEM((seq_rows, LANES), f32),
                pltpu.VMEM((CHUNK.bit_length() - 1, CHUNK, 2 * CHUNK), bf16),
                pltpu.VMEM((heads * chunks // 2, CHUNK, 2 * CHUNK), bf16),
                pltpu.VMEM((heads * chunks // 2, CHUNK, 2 * CHUNK), f32),
            ],
        )
        reach, base, late_gate = call(
            functools.partial(reach_kernel, heads),
            (
                shape((heads, seq_rows, dim), bf16),
                shape((heads, seq_rows, dim), f32),
                shape((rows, columns), f32),
            ),
            [both, low, act, cols, rows_of, *late, w_gate], flops=REACH_FLOPS, limit=12,
        )

    share = heads % 2 == 0
    part = heads // 2 if share else heads
    swap = [(i, i ^ 1) for i in range(seq_count)]
    other = lax.ppermute(own, "seq", swap)
    block = call(
        functools.partial(pair_kernel, share),
        shape((part, dim, 2 * dim), bf16), [own, other], flops=SMALL_FLOPS, limit=4,
    )
    chips = seq_count // 2
    levels = chips.bit_length() - 1
    inside = None
    for level in range(levels):
        size = 1 << level
        sent = block if level < levels - 1 or level == 0 else block[:, :, dim:]
        parts = []
        for target in range(size):
            route = []
            for top in range(size - 1, chips, 2 * size):
                for c in range(2):
                    route.append((2 * top + c, 2 * (top + 1 + target) + c))
            parts.append(lax.ppermute(sent, "seq", route))
        if level == levels - 1 and level > 0:
            break
        sent = sum(parts[1:], parts[0])
        kernel, operands = first_kernel, [block, sent]
        if level > 0:
            kernel, operands = functools.partial(climb_kernel, level), [inside, block, sent]
        inside, block = call(
            kernel, (shape(block.shape, bf16),) * 2, operands, flops=SMALL_FLOPS, limit=4,
        )
    state = call(
        fold_kernel, shape((part, dim, dim), bf16), [inside, *parts],
        flops=SMALL_FLOPS, limit=4,
    )
    back = lax.ppermute(state, "seq", swap) if share else state
    return call(
        functools.partial(final_kernel, share, blocks, not by_block), shape((seq_rows, columns), bf16),
        [reach, base, other, state, back, own_gate, mid_gate, late_gate, norm_gain.reshape(1, dim)],
        flops=SMALL_FLOPS, limit=12,
    )


def solution(mesh):
    return jax.shard_map(
        per_device,
        mesh=mesh,
        in_specs=(
            P(("seq", "tp"), None),
            P(None, None, "tp"),
            P(None, "tp"),
            P(None, None, "tp"),
            P(None, None, "tp"),
            P("tp"),
            P("tp"),
            P(),
        ),
        out_specs=P("seq", "tp"),
        check_vma=False,
    )
```

```python
import functools
import math

import jax
import jax.numpy as jnp
from jax import lax
from jax.experimental import pallas as pl
from jax.experimental.pallas import tpu as pltpu
from jax.sharding import PartitionSpec as P


CHUNK = 128
LANES = 128
RIM = 8
EPS = 1e-6
PROJECT_FLOPS = 3000000000
DELTA_FLOPS = 3000000000
REACH_FLOPS = 2000000000
SMALL_FLOPS = 50000000
MASKS_FLOPS = 8000000000


f32 = jnp.float32
bf16 = jnp.bfloat16


def dot(left, right, contract=(1, 0), precision=None):
    dims = (((contract[0],), (contract[1],)), ((), ()))
    return lax.dot_general(left, right, dims, precision=precision, preferred_element_type=f32)


def whole(memory=pltpu.VMEM):
    return pl.BlockSpec(memory_space=memory)


def gather_blocks(block, axis):
    count = lax.axis_size(axis)
    bits = count.bit_length() - 1
    half = block.shape[0] // 2

    def swap(value, bit):
        step = 1 << bit
        return lax.ppermute(value, axis, [(i, i ^ step) for i in range(count)])

    found = {0: block}
    for bit in range(bits):
        found[1 << bit] = swap(block, bit)
    halves = []
    for number, order in enumerate((range(bits), range(bits - 1, -1, -1))):
        part = {m: value[number * half:(number + 1) * half] for m, value in found.items()}
        for bit in order:
            for mask in list(part):
                if mask | (1 << bit) not in part:
                    part[mask | (1 << bit)] = swap(part[mask], bit)
        halves.append(part)
    early = [found[m] if m in found else (halves[0][m], halves[1][m]) for m in range(count - 1)]
    flat = []
    for item in early[1:]:
        flat.extend(item if isinstance(item, tuple) else (item,))
    return flat, [halves[0][count - 1], halves[1][count - 1]]


def rim_rows(block, count):
    seq_count, tp_count = lax.axis_size("seq"), lax.axis_size("tp")
    tail = block[-count:]
    parts = []
    for j in range(tp_count):
        route = [(s * tp_count - 1, s * tp_count + j) for s in range(1, seq_count)]
        parts.append(lax.ppermute(tail, ("seq", "tp"), route))
    route = [(i, tp_count - 1 - i) for i in range(tp_count)]
    across = lax.ppermute(tail, "tp", route)
    return parts, across


def silu(x):
    return x / (1.0 + jnp.exp(-x))


def scalar_weights(ref):
    kinds, heads, width = ref.shape
    rows = [ref[kind].astype(f32) for kind in range(kinds)]
    rows.append(jnp.zeros((LANES - kinds * heads, width), f32))
    return jnp.concatenate(rows, axis=0).astype(bf16)


def lane_row(ref):
    lane = lax.broadcasted_iota(jnp.int32, (1, LANES), 1)
    row = jnp.zeros((1, LANES), f32)
    for head in range(ref.shape[1]):
        row = jnp.where(lane == head, ref[:, head:head + 1], row)
    return row


def project_kernel(count, *refs):
    blocks = refs[:count]
    w_ref, gate_w_ref, small_ref = refs[count:count + 3]
    p_ref, gate_ref, sc_ref = refs[count + 3:count + 6]
    rows = sc_ref.shape[0]
    tokens = jnp.concatenate([ref[...] for ref in blocks], axis=0)
    sc_ref[...] = dot(tokens, scalar_weights(small_ref), (1, 1))[:rows]
    gate_ref[...] = silu(dot(tokens, gate_w_ref[...])[:rows])

    def one(branch, carry):
        p_ref[branch] = dot(tokens, w_ref[branch]).astype(bf16)
        return carry

    lax.fori_loop(0, w_ref.shape[0], one, 0)


def block_diagonal(left, right):
    hole = jnp.zeros_like(left)
    return jnp.concatenate(
        [jnp.concatenate([left, hole], axis=1), jnp.concatenate([hole, right], axis=1)], axis=0
    )


def beside(left, right):
    return jnp.concatenate([left, right], axis=1)


def grid_index(shape):
    return lax.broadcasted_iota(jnp.int32, shape, 0), lax.broadcasted_iota(jnp.int32, shape, 1)


def delta_kernel(
    heads, blocks, own_ref, own_sc_ref, p_ref, sc_ref, late0_ref, late1_ref, w_ref,
    small_ref, taps_ref, rate_ref, bias_ref, x_ref, both_ref, low_ref, act, cols, rows_of,
    xp, sc, masks, mixes, solves,
):
    seq_rows = act.shape[1]
    rows = seq_rows // blocks
    chunks = seq_rows // CHUNK
    taps = taps_ref.shape[1]
    me = lax.axis_index("tp")

    def place(m, offset=0):
        return pl.multiple_of(offset + lax.bitwise_xor(me, m) * rows, 8)

    late = jnp.concatenate([late0_ref[...], late1_ref[...]], axis=0)
    sc[pl.ds(place(blocks - 1), rows)] = dot(late, scalar_weights(small_ref), (1, 1))
    sc[pl.ds(place(0), rows)] = own_sc_ref[...]
    for m in range(1, blocks - 1):
        sc[pl.ds(place(m), rows)] = sc_ref[(m - 1) * rows:m * rows]

    def fill(branch, carry):
        made = dot(late, w_ref[branch]).astype(bf16).astype(f32)
        for head in range(heads):
            tile = branch * heads + head
            lanes = slice(head * LANES, (head + 1) * LANES)
            xp[tile, :RIM] = p_ref[branch, (blocks - 2) * rows:, lanes].astype(f32)
            xp[tile, pl.ds(place(0, RIM), rows)] = own_ref[branch, :, lanes].astype(f32)
            xp[tile, pl.ds(place(blocks - 1, RIM), rows)] = made[:, lanes]
            for m in range(1, blocks - 1):
                block = p_ref[branch, (m - 1) * rows:m * rows, lanes]
                xp[tile, pl.ds(place(m, RIM), rows)] = block.astype(f32)
        return carry

    lax.fori_loop(0, 3, fill, 0)

    ri, ci = grid_index((CHUNK, CHUNK))
    upto = ri >= ci
    lower = upto.astype(f32)
    levels = CHUNK.bit_length() - 1
    for level in range(levels):
        hit = ((ri >> (level + 1)) == (ci >> (level + 1))) & ((ri >> level) > (ci >> level))
        hit = hit.astype(f32).astype(bf16)
        masks[level] = beside(hit, hit)

    root = 1.0 / math.sqrt(LANES)
    rate, bias = -lane_row(rate_ref), lane_row(bias_ref)

    def prepare(chunk, carry):
        base = pl.multiple_of(chunk * CHUNK, CHUNK)
        raw = sc[pl.ds(base, CHUNK)]
        shifted = raw + bias
        soft = jnp.maximum(shifted, 0.0) + jnp.log1p(jnp.exp(-jnp.abs(shifted)))
        decay = dot(lower, rate * soft, precision=lax.Precision.HIGHEST)
        beta = 1.0 / (1.0 + jnp.exp(-raw))
        comb = jnp.where(ci < heads, decay, 0.0)
        for head in range(heads):
            norms = []
            for branch in range(3):
                tile = branch * heads + head
                weights = taps_ref[branch, :, head * LANES:(head + 1) * LANES].astype(f32)
                total = None
                for i in range(taps):
                    term = xp[tile, pl.ds(base + (RIM - taps + 1 + i), CHUNK)] * weights[i:i + 1]
                    total = term if total is None else total + term
                value = silu(total).astype(bf16)
                act[tile, pl.ds(base, CHUNK)] = value
                if branch < 2:
                    wide = value.astype(f32)
                    norms.append(lax.rsqrt(jnp.sum(wide * wide, axis=-1, keepdims=True) + EPS))
            scaled = beta[:, heads + head:heads + head + 1] * norms[1]
            comb = jnp.where(ci == heads + head, scaled, comb)
            comb = jnp.where(ci == 2 * heads + head, norms[0] * root, comb)
            comb = jnp.where(ci == 3 * heads + head, norms[1], comb)
        cols[chunk] = comb
        rows_of[chunk] = comb.T
        return carry

    lax.fori_loop(0, chunks, prepare, 0)

    def part(branch, head, chunk):
        return act[branch * heads + head, chunk * CHUNK:(chunk + 1) * CHUNK]

    def col(kind, head, chunk):
        lane = kind * heads + head
        return cols[chunk, :, lane:lane + 1]

    def row(kind, head, chunk):
        lane = kind * heads + head
        return rows_of[chunk, lane:lane + 1, :]

    sets = [(head, chunk) for head in range(heads) for chunk in range(0, chunks, 2)]
    for s, (head, first) in enumerate(sets):
        two = (first, first + 1)
        keys = [part(1, head, c) for c in two]
        gram = dot(beside(*keys), block_diagonal(*[k.T for k in keys]))
        mix = []
        for i, c in enumerate(two):
            lanes = slice(i * LANES, (i + 1) * LANES)
            gap = col(0, head, c) - row(0, head, c)
            weight = jnp.exp(jnp.minimum(gap, 0.0)) * row(1, head, c)
            mix.append((weight * gram[:, lanes] * col(3, head, c)).astype(bf16))
        mix = beside(*mix)
        mixes[s] = mix
        eye = jnp.where(ri == ci, 1.0, 0.0)
        solves[s] = beside(eye, eye) - (mix * masks[0]).astype(f32)
    for level in range(1, levels):
        lows, mids = [], []
        for s in range(len(sets)):
            low = solves[s].astype(bf16)
            lows.append(low)
            mids.append(dot(mixes[s] * masks[level], block_diagonal(low[:, :LANES], low[:, LANES:])).astype(bf16))
        for s in range(len(sets)):
            mid = mids[s]
            solves[s] = solves[s] - dot(lows[s], block_diagonal(mid[:, :LANES], mid[:, LANES:]))
    change = {}
    for s, (head, first) in enumerate(sets):
        two = (first, first + 1)
        solve = solves[s]
        new = dot(solve.astype(bf16), block_diagonal(*[part(2, head, c) for c in two]))
        grown = beside(*[jnp.exp(row(0, head, c)) * row(3, head, c) for c in two])
        back = dot((solve * grown).astype(bf16), block_diagonal(*[part(1, head, c) for c in two]))
        for i, c in enumerate(two):
            lanes = slice(i * LANES, (i + 1) * LANES)
            both = beside(back[:, lanes], new[:, lanes])
            decay = col(0, head, c)
            tail = col(1, head, c) * jnp.exp(decay[CHUNK - 1:] - decay)
            change[head, c] = dot(part(1, head, c), (both * tail).astype(bf16), (0, 0))
            both_ref[head, c] = both.astype(bf16)
    runs = {}
    for c in range(chunks):
        for head in range(heads):
            last = jnp.exp(col(0, head, c)[CHUNK - 1:])
            if c == 0:
                runs[head] = beside(
                    jnp.where(ri == ci, last, 0.0) - change[head, c][:, :LANES], change[head, c][:, LANES:]
                )
            else:
                low = runs[head].astype(bf16)
                low_ref[head, c - 1] = low
                run = last * runs[head] - dot(change[head, c][:, :LANES].astype(bf16), low)
                runs[head] = beside(run[:, :LANES], run[:, LANES:] + change[head, c][:, LANES:])
    for head in range(heads):
        x_ref[head] = runs[head].astype(bf16)


def reach_kernel(
    heads, both_ref, low_ref, act, cols, rows_of, late0_ref, late1_ref, gate_w_ref,
    qp_ref, o_ref, gate_ref,
):
    late = jnp.concatenate([late0_ref[...], late1_ref[...]], axis=0)
    gate_ref[...] = silu(dot(late, gate_w_ref[...]))
    chunks = act.shape[1] // CHUNK
    ri, ci = grid_index((CHUNK, CHUNK))
    upto = ri >= ci
    for head in range(heads):
        for c in range(chunks):
            at = slice(c * CHUNK, (c + 1) * CHUNK)

            def col(kind):
                lane = kind * heads + head
                return cols[c, :, lane:lane + 1]

            def row(kind):
                lane = kind * heads + head
                return rows_of[c, lane:lane + 1, :]

            q = act[head, at]
            score = dot(q, act[heads + head, at], (1, 1))
            weight = jnp.exp(jnp.minimum(col(0) - row(0), 0.0)) * row(1)
            attend = jnp.where(upto, weight * score * col(2), 0.0).astype(bf16)
            inner = dot(attend, both_ref[head, c])
            eff = (jnp.exp(col(0)) * col(2)) * q.astype(f32) - inner[:, :LANES]
            if c == 0:
                qp_ref[head, at] = eff.astype(bf16)
                o_ref[head, at] = inner[:, LANES:]
            else:
                ahead = dot(eff.astype(bf16), low_ref[head, c - 1])
                qp_ref[head, at] = ahead[:, :LANES].astype(bf16)
                o_ref[head, at] = inner[:, LANES:] + ahead[:, LANES:]


def convolve(heads, xp, base, taps_ref, raw, rate, bias, keep):
    ri, ci = grid_index((CHUNK, CHUNK))
    taps = taps_ref.shape[1]
    shifted = raw + bias
    soft = jnp.maximum(shifted, 0.0) + jnp.log1p(jnp.exp(-jnp.abs(shifted)))
    decay = dot((ri >= ci).astype(f32), rate * soft, precision=lax.Precision.HIGHEST)
    beta = 1.0 / (1.0 + jnp.exp(-raw))
    comb = jnp.where(ci < heads, decay, 0.0)
    root = 1.0 / math.sqrt(LANES)
    for head in range(heads):
        norms = []
        for branch in range(3):
            tile = branch * heads + head
            weights = taps_ref[branch, :, head * LANES:(head + 1) * LANES].astype(f32)
            total = None
            for i in range(taps):
                term = xp[tile, pl.ds(base + (RIM - taps + 1 + i), CHUNK)] * weights[i:i + 1]
                total = term if total is None else total + term
            value = silu(total).astype(bf16)
            keep(tile, value)
            if branch < 2:
                wide = value.astype(f32)
                norms.append(lax.rsqrt(jnp.sum(wide * wide, axis=-1, keepdims=True) + EPS))
        scaled = beta[:, heads + head:heads + head + 1] * norms[1]
        comb = jnp.where(ci == heads + head, scaled, comb)
        comb = jnp.where(ci == 2 * heads + head, norms[0] * root, comb)
        comb = jnp.where(ci == 3 * heads + head, norms[1], comb)
    return comb


def early_kernel(heads, blocks, *refs):
    count = blocks + 1
    tokens_refs, part_ref = refs[:blocks], refs[blocks]
    w_ref, small_ref, taps_ref, rate_ref, bias_ref = refs[count:count + 5]
    act, cols, rows_of, raw_ref, raw_sc_ref, rims_ref, xp, tails = refs[count + 5:]
    early = blocks - 1
    mid = early * CHUNK
    me = lax.axis_index("tp")
    edge = jnp.concatenate([tokens_refs[-1][...].astype(f32), part_ref[...].astype(f32)], axis=0)
    tokens = jnp.concatenate([ref[...] for ref in tokens_refs[:-1]] + [edge.astype(bf16)], axis=0)
    raw = dot(tokens[:mid], scalar_weights(small_ref), (1, 1))
    later = [m for m in range(early) if m != 1]
    for slot, m in enumerate(later):
        raw_sc_ref[slot * CHUNK:(slot + 1) * CHUNK] = raw[m * CHUNK:(m + 1) * CHUNK]

    def fill(branch, carry):
        made = dot(tokens, w_ref[branch]).astype(bf16).astype(f32)
        for head in range(heads):
            tile = branch * heads + head
            lanes = slice(head * LANES, (head + 1) * LANES)
            for m in range(early):
                block = made[m * CHUNK:(m + 1) * CHUNK, lanes]
                if m == 1:
                    xp[tile, RIM:] = block
                else:
                    slot = later.index(m)
                    raw_ref[tile, slot * CHUNK:(slot + 1) * CHUNK] = block
                tails[m, tile] = block[CHUNK - RIM:]
            tails[early, tile] = made[mid:mid + RIM, lanes]
            tails[blocks, tile] = made[mid + RIM:, lanes]
        return carry

    lax.fori_loop(0, 3, fill, 0)
    rate, bias = -lane_row(rate_ref), lane_row(bias_ref)

    def ahead_of(m):
        index = lax.bitwise_xor(me, m)
        return jnp.where(index == 0, blocks, lax.bitwise_xor(me, jnp.maximum(index - 1, 0)))

    for slot, m in enumerate(later + [early]):
        rims_ref[slot] = tails[ahead_of(m)]
    source = ahead_of(1)
    for tile in range(3 * heads):
        xp[tile, :RIM] = tails[source, tile]

    def prepare(slot, carry):
        def keep(tile, value):
            act[tile] = value

        base = pl.multiple_of(slot * CHUNK, CHUNK)
        comb = convolve(heads, xp, base, taps_ref, raw[CHUNK:2 * CHUNK], rate, bias, keep)
        cols[0] = comb
        rows_of[0] = comb.T
        return carry

    prepare(0, 0)


def masks_kernel(out_ref):
    ri, ci = grid_index((CHUNK, CHUNK))
    for level in range(out_ref.shape[0]):
        hit = ((ri >> (level + 1)) == (ci >> (level + 1))) & ((ri >> level) > (ci >> level))
        hit = hit.astype(f32).astype(bf16)
        out_ref[level] = beside(hit, hit)


def block_delta_kernel(
    heads, blocks, act_e, cols_e, rows_e, raw_ref, raw_sc_ref, rims_ref, late0_ref, late1_ref, *refs
):
    me = lax.axis_index("tp")
    part_refs = refs[:blocks - 1]
    w_ref, small_ref, taps_ref, rate_ref, bias_ref, masks = refs[blocks - 1:blocks + 5]
    x_ref, both_ref, low_ref, act_l, cols_l, rows_l = refs[blocks + 5:blocks + 11]
    xp, sc, mixes, solves, changes, lasts = refs[blocks + 11:]
    span = RIM + CHUNK
    slots = blocks - 1
    before = part_refs[0][...].astype(f32)
    for ref in part_refs[1:]:
        before = before + ref[...].astype(f32)
    before = jnp.concatenate([before, jnp.zeros_like(before)], axis=0)
    tokens = jnp.concatenate([late0_ref[...], late1_ref[...], before.astype(bf16)], axis=0)
    sc[:(slots - 1) * CHUNK] = raw_sc_ref[...]
    sc[(slots - 1) * CHUNK:] = dot(tokens[:CHUNK], scalar_weights(small_ref), (1, 1))

    def fill(branch, carry):
        made = dot(tokens, w_ref[branch]).astype(bf16).astype(f32)
        for head in range(heads):
            tile = branch * heads + head
            lanes = slice(head * LANES, (head + 1) * LANES)
            rim = made[CHUNK:CHUNK + RIM, lanes]
            for slot in range(slots):
                at = slot * span
                first = me == (slot + 1 if slot else 0)
                xp[tile, at:at + RIM] = jnp.where(first, rim, rims_ref[slot, tile])
                if slot == slots - 1:
                    xp[tile, at + RIM:at + span] = made[:CHUNK, lanes]
                else:
                    xp[tile, at + RIM:at + span] = raw_ref[tile, slot * CHUNK:(slot + 1) * CHUNK]
        return carry

    lax.fori_loop(0, 3, fill, 0)
    rate, bias = -lane_row(rate_ref), lane_row(bias_ref)

    def prepare(slot, carry):
        at = pl.ds(pl.multiple_of(slot * CHUNK, CHUNK), CHUNK)

        def keep(tile, value):
            act_l[tile, at] = value

        base = pl.multiple_of(slot * span, 8)
        comb = convolve(heads, xp, base, taps_ref, sc[at], rate, bias, keep)
        cols_l[slot] = comb
        rows_l[slot] = comb.T
        return carry

    lax.fori_loop(0, slots, prepare, 0)

    ri, ci = grid_index((CHUNK, CHUNK))
    levels = masks.shape[0]

    def part(branch, head, m):
        held, slot = (act_e, 0) if m == 1 else (act_l, max(m - 1, 0))
        return held[branch * heads + head, slot * CHUNK:(slot + 1) * CHUNK]

    def col(kind, head, m):
        lane = kind * heads + head
        held, slot = (cols_e, 0) if m == 1 else (cols_l, max(m - 1, 0))
        return held[slot, :, lane:lane + 1]

    def row(kind, head, m):
        lane = kind * heads + head
        held, slot = (rows_e, 0) if m == 1 else (rows_l, max(m - 1, 0))
        return held[slot, lane:lane + 1, :]

    for m in range(blocks):
        held, slot = (cols_e, 0) if m == 1 else (cols_l, max(m - 1, 0))
        lasts[m] = jnp.exp(held[slot, CHUNK - 8:])

    sets = [(head, m) for m in range(0, blocks, 2) for head in range(heads)]
    for s, (head, first) in enumerate(sets):
        two = (first, first + 1)
        keys = [part(1, head, m) for m in two]
        gram = dot(beside(*keys), block_diagonal(*[k.T for k in keys]))
        mix = []
        for i, m in enumerate(two):
            lanes = slice(i * LANES, (i + 1) * LANES)
            gap = col(0, head, m) - row(0, head, m)
            weight = jnp.exp(jnp.minimum(gap, 0.0)) * row(1, head, m)
            mix.append((weight * gram[:, lanes] * col(3, head, m)).astype(bf16))
        mix = beside(*mix)
        mixes[s] = mix
        eye = jnp.where(ri == ci, 1.0, 0.0)
        solves[s] = beside(eye, eye) - (mix * masks[0]).astype(f32)
    for level in range(1, levels):
        lows, mids = [], []
        for s in range(len(sets)):
            low = solves[s].astype(bf16)
            lows.append(low)
            mids.append(dot(mixes[s] * masks[level], block_diagonal(low[:, :LANES], low[:, LANES:])).astype(bf16))
        for s in range(len(sets)):
            mid = mids[s]
            solves[s] = solves[s] - dot(lows[s], block_diagonal(mid[:, :LANES], mid[:, LANES:]))
    for s, (head, first) in enumerate(sets):
        two = (first, first + 1)
        solve = solves[s]
        new = dot(solve.astype(bf16), block_diagonal(*[part(2, head, m) for m in two]))
        grown = beside(*[jnp.exp(row(0, head, m)) * row(3, head, m) for m in two])
        back = dot((solve * grown).astype(bf16), block_diagonal(*[part(1, head, m) for m in two]))
        for i, m in enumerate(two):
            lanes = slice(i * LANES, (i + 1) * LANES)
            both = beside(back[:, lanes], new[:, lanes])
            decay = col(0, head, m)
            tail = col(1, head, m) * jnp.exp(decay[CHUNK - 1:] - decay)
            changes[m, head] = dot(part(1, head, m), (both * tail).astype(bf16), (0, 0))
            both_ref[head, m] = both.astype(bf16)
    eye = jnp.where(ri == ci, 1.0, 0.0)
    runs = {}
    for step in range(blocks):
        m = lax.bitwise_xor(me, step)
        for head in range(heads):
            last = lasts[m, 7:, head:head + 1]
            change = changes[m, head]
            if step == 0:
                low_ref[head, m] = beside(eye, jnp.zeros_like(eye)).astype(bf16)
                runs[head] = beside(last * eye - change[:, :LANES], change[:, LANES:])
            else:
                low = runs[head].astype(bf16)
                low_ref[head, m] = low
                run = last * runs[head] - dot(change[:, :LANES].astype(bf16), low)
                runs[head] = beside(run[:, :LANES], run[:, LANES:] + change[:, LANES:])
    for head in range(heads):
        x_ref[head] = runs[head].astype(bf16)


def block_reach_kernel(
    heads, blocks, both_ref, low_ref, act_e, cols_e, rows_e, act_l, cols_l, rows_l,
    qp_ref, o_ref,
):
    ri, ci = grid_index((CHUNK, CHUNK))
    upto = ri >= ci
    for head in range(heads):
        for m in range(blocks):
            at = slice(m * CHUNK, (m + 1) * CHUNK)
            slot = 0 if m == 1 else max(m - 1, 0)
            act, cols_of, rows_of = (act_e, cols_e, rows_e) if m == 1 else (act_l, cols_l, rows_l)
            held = slice(slot * CHUNK, (slot + 1) * CHUNK)
            cols, rows = cols_of[slot], rows_of[slot]
            q, k = act[head, held], act[heads + head, held]
            decay = cols[:, head:head + 1]
            norm = cols[:, 2 * heads + head:2 * heads + head + 1]
            gap = decay - rows[head:head + 1]
            weight = jnp.exp(jnp.minimum(gap, 0.0)) * rows[heads + head:heads + head + 1]
            attend = jnp.where(upto, weight * dot(q, k, (1, 1)) * norm, 0.0).astype(bf16)
            inner = dot(attend, both_ref[head, m])
            eff = (jnp.exp(decay) * norm) * q.astype(f32) - inner[:, :LANES]
            ahead = dot(eff.astype(bf16), low_ref[head, m])
            qp_ref[head, at] = ahead[:, :LANES].astype(bf16)
            o_ref[head, at] = inner[:, LANES:] + ahead[:, LANES:]


def gate_kernel(count, *refs):
    w_ref = refs[count]
    outs = refs[count + 1:]
    tokens = jnp.concatenate([ref[...] for ref in refs[:count]], axis=0)
    gate = silu(dot(tokens, w_ref[...]))
    start = 0
    for out in outs:
        out[...] = gate[start:start + out.shape[0]]
        start += out.shape[0]


def pair_kernel(share, mine_ref, other_ref, out_ref):
    core = lax.axis_index("seq") & 1
    for j in range(out_ref.shape[0]):
        head = core * out_ref.shape[0] + j if share else j
        mine, other = mine_ref[head], other_ref[head]
        first = jnp.where(core == 0, mine, other)
        second = jnp.where(core == 0, other, mine)
        both = dot(second[:, :LANES], first)
        out_ref[j, :, :LANES] = both[:, :LANES].astype(bf16)
        out_ref[j, :, LANES:] = (both[:, LANES:] + second[:, LANES:].astype(f32)).astype(bf16)


def climb_kernel(bit, inside_ref, block_ref, sent_ref, inside_out, block_out):
    upper = (lax.axis_index("seq") >> (bit + 1)) & 1
    for j in range(block_ref.shape[0]):
        sent = sent_ref[j]
        for ref, out in ((inside_ref, inside_out), (block_ref, block_out)):
            mine = ref[j]
            both = dot(mine[:, :LANES], sent)
            left = jnp.where(upper == 1, both[:, :LANES], mine[:, :LANES].astype(f32))
            right = mine[:, LANES:].astype(f32) + both[:, LANES:]
            out[j] = jnp.concatenate([left, right], axis=1).astype(bf16)


def first_kernel(block_ref, sent_ref, inside_out, block_out):
    upper = (lax.axis_index("seq") >> 1) & 1
    ri, ci = grid_index((LANES, LANES))
    eye = jnp.where(ri == ci, 1.0, 0.0)
    for j in range(block_ref.shape[0]):
        sent, mine = sent_ref[j], block_ref[j]
        both = dot(mine[:, :LANES], sent)
        left = jnp.where(upper == 1, both[:, :LANES], mine[:, :LANES].astype(f32))
        right = mine[:, LANES:].astype(f32) + both[:, LANES:]
        block_out[j] = jnp.concatenate([left, right], axis=1).astype(bf16)
        inside = jnp.where(upper == 1, sent[:, :LANES].astype(f32), eye)
        inside_out[j] = jnp.concatenate([inside.astype(bf16), sent[:, LANES:]], axis=1)


def fold_kernel(inside_ref, *refs):
    out_ref = refs[-1]
    for j in range(out_ref.shape[0]):
        state = refs[0][j]
        for ref in refs[1:-1]:
            state = state + ref[j]
        inside = inside_ref[j]
        state = inside[:, LANES:].astype(f32) + dot(inside[:, :LANES], state)
        out_ref[j] = state.astype(bf16)


def final_kernel(
    share, blocks, ordered, qp_ref, o_ref, pair_ref, mine_ref, other_ref,
    own_gate_ref, gate_ref, late_gate_ref, gain_ref, out_ref,
):
    heads, seq_rows, dim = qp_ref.shape
    rows = seq_rows // blocks
    core, me = lax.axis_index("seq") & 1, lax.axis_index("tp")
    part = mine_ref.shape[0]
    for head in range(heads):
        start = mine_ref[head % part]
        if share:
            start = jnp.where(core == head // part, start, other_ref[head % part])
        pair = pair_ref[head]
        moved = pair[:, dim:].astype(f32) + dot(pair[:, :dim], start)
        start = jnp.where(core == 0, start.astype(f32), moved).astype(bf16)
        lanes = slice(head * dim, (head + 1) * dim)
        for m in range(blocks):
            if m == 0:
                gate = own_gate_ref[:, lanes]
            elif m < blocks - 1:
                gate = gate_ref[(m - 1) * rows:m * rows, lanes]
            else:
                gate = late_gate_ref[:, lanes]
            at = pl.ds(pl.multiple_of(lax.bitwise_xor(me, m) * rows, 8), rows)
            held = at if ordered else slice(m * rows, (m + 1) * rows)
            y = o_ref[head, held] + dot(qp_ref[head, held], start)
            scale = lax.rsqrt(jnp.mean(y * y, axis=-1, keepdims=True) + EPS)
            out_ref[at, lanes] = (y * scale * gain_ref[...] * gate).astype(bf16)


def call(kernel, out, operands, flops=0, scratch=(), limit=24):
    single = not isinstance(out, tuple)
    return pl.pallas_call(
        kernel,
        out_shape=out,
        in_specs=[whole()] * len(operands),
        out_specs=whole() if single else (whole(),) * len(out),
        scratch_shapes=scratch,
        cost_estimate=pl.CostEstimate(flops=flops, transcendentals=0, bytes_accessed=1 << 20),
        compiler_params=pltpu.CompilerParams(vmem_limit_bytes=limit << 20),
    )(*operands)


def per_device(hidden, w_qkv, w_gate, w_decay_beta, conv_weight, decay_rate, dt_bias, norm_gain):
    heads = decay_rate.shape[0]
    dim = norm_gain.shape[0]
    columns = heads * dim
    blocks = lax.axis_size("tp")
    seq_count = lax.axis_size("seq")
    rows = hidden.shape[0]
    seq_rows = rows * blocks
    chunks = seq_rows // CHUNK
    shape = jax.ShapeDtypeStruct

    w_three = w_qkv.transpose(1, 0, 2)
    small = w_decay_beta.transpose(1, 2, 0)
    taps = conv_weight.transpose(1, 0, 2)
    rate, bias = decay_rate.reshape(1, heads), dt_bias.reshape(1, heads)

    early, late = gather_blocks(hidden, "tp")
    weights = [w_three, w_gate, small]

    def project(tokens, count, extra=0):
        return call(
            functools.partial(project_kernel, len(tokens)),
            (
                shape((3, count + extra, columns), bf16),
                shape((count, columns), f32),
                shape((count, LANES), f32),
            ),
            [*tokens, *weights], flops=PROJECT_FLOPS, limit=20,
        )

    by_block = rows == CHUNK and len(early) == blocks - 2 and blocks > 2
    if by_block:
        parts, across = rim_rows(hidden, RIM)
        masks = call(
            masks_kernel,
            shape((CHUNK.bit_length() - 1, CHUNK, 2 * CHUNK), bf16), [],
            flops=MASKS_FLOPS, limit=4,
        )
        act_e, cols_e, rows_e, raw, raw_sc, rims = call(
            functools.partial(early_kernel, heads, blocks),
            (
                shape((3 * heads, rows, dim), bf16),
                shape((1, CHUNK, LANES), f32),
                shape((1, CHUNK, LANES), f32),
                shape((3 * heads, seq_rows - 2 * rows, dim), f32),
                shape((seq_rows - 2 * rows, LANES), f32),
                shape((blocks - 1, 3 * heads, RIM, dim), f32),
            ),
            [
                hidden, *early, across, parts[1],
                w_three, small, taps, rate, bias,
            ],
            flops=PROJECT_FLOPS,
            scratch=[
                pltpu.VMEM((3 * heads, RIM + CHUNK, dim), f32),
                pltpu.VMEM((blocks + 1, 3 * heads, RIM, dim), f32),
            ],
        )
        own, both, low, act_l, cols_l, rows_l = call(
            functools.partial(block_delta_kernel, heads, blocks),
            (
                shape((heads, dim, 2 * dim), bf16),
                shape((heads, blocks, CHUNK, 2 * dim), bf16),
                shape((heads, blocks, dim, 2 * dim), bf16),
                shape((3 * heads, seq_rows - rows, dim), bf16),
                shape((blocks - 1, CHUNK, LANES), f32),
                shape((blocks - 1, CHUNK, LANES), f32),
            ),
            [
                act_e, cols_e, rows_e, raw, raw_sc, rims, *late,
                parts[0], *parts[2:], w_three, small, taps, rate, bias, masks,
            ],
            flops=DELTA_FLOPS, limit=28,
            scratch=[
                pltpu.VMEM((3 * heads, (blocks - 1) * (RIM + CHUNK), dim), f32),
                pltpu.VMEM((seq_rows - rows, LANES), f32),
                pltpu.VMEM((heads * blocks // 2, CHUNK, 2 * CHUNK), bf16),
                pltpu.VMEM((heads * blocks // 2, CHUNK, 2 * CHUNK), f32),
                pltpu.VMEM((blocks, heads, dim, 2 * dim), f32),
                pltpu.VMEM((blocks, 8, LANES), f32),
            ],
        )
        reach, base = call(
            functools.partial(block_reach_kernel, heads, blocks),
            (
                shape((heads, seq_rows, dim), bf16),
                shape((heads, seq_rows, dim), f32),
            ),
            [both, low, act_e, cols_e, rows_e, act_l, cols_l, rows_l],
            flops=REACH_FLOPS, limit=14,
        )
        tokens = [hidden, *early, *late]
        own_gate, mid_gate, late_gate = call(
            functools.partial(gate_kernel, len(tokens)),
            (
                shape((rows, columns), f32),
                shape((seq_rows - 2 * rows, columns), f32),
                shape((rows, columns), f32),
            ),
            [*tokens, w_gate], flops=PROJECT_FLOPS, limit=14,
        )
    else:
        own_p, own_gate, own_sc = project([hidden], rows)
        parts, _ = rim_rows(hidden, RIM)
        rim = sum(parts[1:], parts[0])
        mid_p, mid_gate, mid_sc = project([*early, rim], seq_rows - 2 * rows, RIM)
        own, both, low, act, cols, rows_of = call(
            functools.partial(delta_kernel, heads, blocks),
            (
                shape((heads, dim, 2 * dim), bf16),
                shape((heads, chunks, CHUNK, 2 * dim), bf16),
                shape((heads, chunks - 1, dim, 2 * dim), bf16),
                shape((3 * heads, seq_rows, dim), bf16),
                shape((chunks, CHUNK, LANES), f32),
                shape((chunks, CHUNK, LANES), f32),
            ),
            [own_p, own_sc, mid_p, mid_sc, *late, w_three, small, taps, rate, bias],
            flops=DELTA_FLOPS, limit=32,
            scratch=[
                pltpu.VMEM((3 * heads, seq_rows + RIM, dim), f32),
                pltpu.VMEM((seq_rows, LANES), f32),
                pltpu.VMEM((CHUNK.bit_length() - 1, CHUNK, 2 * CHUNK), bf16),
                pltpu.VMEM((heads * chunks // 2, CHUNK, 2 * CHUNK), bf16),
                pltpu.VMEM((heads * chunks // 2, CHUNK, 2 * CHUNK), f32),
            ],
        )
        reach, base, late_gate = call(
            functools.partial(reach_kernel, heads),
            (
                shape((heads, seq_rows, dim), bf16),
                shape((heads, seq_rows, dim), f32),
                shape((rows, columns), f32),
            ),
            [both, low, act, cols, rows_of, *late, w_gate], flops=REACH_FLOPS, limit=12,
        )

    share = heads % 2 == 0
    part = heads // 2 if share else heads
    swap = [(i, i ^ 1) for i in range(seq_count)]
    other = lax.ppermute(own, "seq", swap)
    block = call(
        functools.partial(pair_kernel, share),
        shape((part, dim, 2 * dim), bf16), [own, other], flops=SMALL_FLOPS, limit=4,
    )
    chips = seq_count // 2
    levels = chips.bit_length() - 1
    inside = None
    for level in range(levels):
        size = 1 << level
        sent = block if level < levels - 1 or level == 0 else block[:, :, dim:]
        parts = []
        for target in range(size):
            route = []
            for top in range(size - 1, chips, 2 * size):
                for c in range(2):
                    route.append((2 * top + c, 2 * (top + 1 + target) + c))
            parts.append(lax.ppermute(sent, "seq", route))
        if level == levels - 1 and level > 0:
            break
        sent = sum(parts[1:], parts[0])
        kernel, operands = first_kernel, [block, sent]
        if level > 0:
            kernel, operands = functools.partial(climb_kernel, level), [inside, block, sent]
        inside, block = call(
            kernel, (shape(block.shape, bf16),) * 2, operands, flops=SMALL_FLOPS, limit=4,
        )
    state = call(
        fold_kernel, shape((part, dim, dim), bf16), [inside, *parts],
        flops=SMALL_FLOPS, limit=4,
    )
    back = lax.ppermute(state, "seq", swap) if share else state
    return call(
        functools.partial(final_kernel, share, blocks, not by_block), shape((seq_rows, columns), bf16),
        [reach, base, other, state, back, own_gate, mid_gate, late_gate, norm_gain.reshape(1, dim)],
        flops=SMALL_FLOPS, limit=12,
    )


def solution(mesh):
    return jax.shard_map(
        per_device,
        mesh=mesh,
        in_specs=(
            P(("seq", "tp"), None),
            P(None, None, "tp"),
            P(None, "tp"),
            P(None, None, "tp"),
            P(None, None, "tp"),
            P("tp"),
            P("tp"),
            P(),
        ),
        out_specs=P("seq", "tp"),
        check_vma=False,
    )
```

```python
import functools
import math

import jax
import jax.numpy as jnp
from jax import lax
from jax.experimental import pallas as pl
from jax.experimental.pallas import tpu as pltpu
from jax.sharding import PartitionSpec as P


CHUNK = 128
LANES = 128
RIM = 8
EPS = 1e-6
PROJECT_FLOPS = 3000000000
DELTA_FLOPS = 3000000000
REACH_FLOPS = 2000000000
SMALL_FLOPS = 50000000
MASKS_FLOPS = 8000000000


f32 = jnp.float32
bf16 = jnp.bfloat16


def dot(left, right, contract=(1, 0), precision=None):
    dims = (((contract[0],), (contract[1],)), ((), ()))
    return lax.dot_general(left, right, dims, precision=precision, preferred_element_type=f32)


def whole(memory=pltpu.VMEM):
    return pl.BlockSpec(memory_space=memory)


def gather_blocks(block, axis):
    count = lax.axis_size(axis)
    bits = count.bit_length() - 1
    half = block.shape[0] // 2

    def swap(value, bit):
        step = 1 << bit
        return lax.ppermute(value, axis, [(i, i ^ step) for i in range(count)])

    found = {0: block}
    for bit in range(bits):
        found[1 << bit] = swap(block, bit)
    halves = []
    for number, order in enumerate((range(bits), range(bits - 1, -1, -1))):
        part = {m: value[number * half:(number + 1) * half] for m, value in found.items()}
        for bit in order:
            for mask in list(part):
                if mask | (1 << bit) not in part:
                    part[mask | (1 << bit)] = swap(part[mask], bit)
        halves.append(part)
    early = [found[m] if m in found else (halves[0][m], halves[1][m]) for m in range(count - 1)]
    flat = []
    for item in early[1:]:
        flat.extend(item if isinstance(item, tuple) else (item,))
    return flat, [halves[0][count - 1], halves[1][count - 1]]


def rim_rows(block, count):
    seq_count, tp_count = lax.axis_size("seq"), lax.axis_size("tp")
    tail = block[-count:]
    parts = []
    for j in range(tp_count):
        route = [(s * tp_count - 1, s * tp_count + j) for s in range(1, seq_count)]
        parts.append(lax.ppermute(tail, ("seq", "tp"), route))
    route = [(i, tp_count - 1 - i) for i in range(tp_count)]
    across = lax.ppermute(tail, "tp", route)
    return parts, across


def silu(x):
    return x / (1.0 + jnp.exp(-x))


def scalar_weights(ref):
    kinds, heads, width = ref.shape
    rows = [ref[kind].astype(f32) for kind in range(kinds)]
    rows.append(jnp.zeros((LANES - kinds * heads, width), f32))
    return jnp.concatenate(rows, axis=0).astype(bf16)


def lane_row(ref):
    lane = lax.broadcasted_iota(jnp.int32, (1, LANES), 1)
    row = jnp.zeros((1, LANES), f32)
    for head in range(ref.shape[1]):
        row = jnp.where(lane == head, ref[:, head:head + 1], row)
    return row


def project_kernel(count, *refs):
    blocks = refs[:count]
    w_ref, gate_w_ref, small_ref = refs[count:count + 3]
    p_ref, gate_ref, sc_ref = refs[count + 3:count + 6]
    rows = sc_ref.shape[0]
    tokens = jnp.concatenate([ref[...] for ref in blocks], axis=0)
    sc_ref[...] = dot(tokens, scalar_weights(small_ref), (1, 1))[:rows]
    gate_ref[...] = silu(dot(tokens, gate_w_ref[...])[:rows])

    def one(branch, carry):
        p_ref[branch] = dot(tokens, w_ref[branch]).astype(bf16)
        return carry

    lax.fori_loop(0, w_ref.shape[0], one, 0)


def block_diagonal(left, right):
    hole = jnp.zeros_like(left)
    return jnp.concatenate(
        [jnp.concatenate([left, hole], axis=1), jnp.concatenate([hole, right], axis=1)], axis=0
    )


def beside(left, right):
    return jnp.concatenate([left, right], axis=1)


def grid_index(shape):
    return lax.broadcasted_iota(jnp.int32, shape, 0), lax.broadcasted_iota(jnp.int32, shape, 1)


def delta_kernel(
    heads, blocks, own_ref, own_sc_ref, p_ref, sc_ref, late0_ref, late1_ref, w_ref,
    small_ref, taps_ref, rate_ref, bias_ref, x_ref, both_ref, low_ref, act, cols, rows_of,
    xp, sc, masks, mixes, solves,
):
    seq_rows = act.shape[1]
    rows = seq_rows // blocks
    chunks = seq_rows // CHUNK
    taps = taps_ref.shape[1]
    me = lax.axis_index("tp")

    def place(m, offset=0):
        return pl.multiple_of(offset + lax.bitwise_xor(me, m) * rows, 8)

    late = jnp.concatenate([late0_ref[...], late1_ref[...]], axis=0)
    sc[pl.ds(place(blocks - 1), rows)] = dot(late, scalar_weights(small_ref), (1, 1))
    sc[pl.ds(place(0), rows)] = own_sc_ref[...]
    for m in range(1, blocks - 1):
        sc[pl.ds(place(m), rows)] = sc_ref[(m - 1) * rows:m * rows]

    def fill(branch, carry):
        made = dot(late, w_ref[branch]).astype(bf16).astype(f32)
        for head in range(heads):
            tile = branch * heads + head
            lanes = slice(head * LANES, (head + 1) * LANES)
            xp[tile, :RIM] = p_ref[branch, (blocks - 2) * rows:, lanes].astype(f32)
            xp[tile, pl.ds(place(0, RIM), rows)] = own_ref[branch, :, lanes].astype(f32)
            xp[tile, pl.ds(place(blocks - 1, RIM), rows)] = made[:, lanes]
            for m in range(1, blocks - 1):
                block = p_ref[branch, (m - 1) * rows:m * rows, lanes]
                xp[tile, pl.ds(place(m, RIM), rows)] = block.astype(f32)
        return carry

    lax.fori_loop(0, 3, fill, 0)

    ri, ci = grid_index((CHUNK, CHUNK))
    upto = ri >= ci
    lower = upto.astype(f32)
    levels = CHUNK.bit_length() - 1
    for level in range(levels):
        hit = ((ri >> (level + 1)) == (ci >> (level + 1))) & ((ri >> level) > (ci >> level))
        hit = hit.astype(f32).astype(bf16)
        masks[level] = beside(hit, hit)

    root = 1.0 / math.sqrt(LANES)
    rate, bias = -lane_row(rate_ref), lane_row(bias_ref)

    def prepare(chunk, carry):
        base = pl.multiple_of(chunk * CHUNK, CHUNK)
        raw = sc[pl.ds(base, CHUNK)]
        shifted = raw + bias
        soft = jnp.maximum(shifted, 0.0) + jnp.log1p(jnp.exp(-jnp.abs(shifted)))
        decay = dot(lower, rate * soft, precision=lax.Precision.HIGHEST)
        beta = 1.0 / (1.0 + jnp.exp(-raw))
        comb = jnp.where(ci < heads, decay, 0.0)
        for head in range(heads):
            norms = []
            for branch in range(3):
                tile = branch * heads + head
                weights = taps_ref[branch, :, head * LANES:(head + 1) * LANES].astype(f32)
                total = None
                for i in range(taps):
                    term = xp[tile, pl.ds(base + (RIM - taps + 1 + i), CHUNK)] * weights[i:i + 1]
                    total = term if total is None else total + term
                value = silu(total).astype(bf16)
                act[tile, pl.ds(base, CHUNK)] = value
                if branch < 2:
                    wide = value.astype(f32)
                    norms.append(lax.rsqrt(jnp.sum(wide * wide, axis=-1, keepdims=True) + EPS))
            scaled = beta[:, heads + head:heads + head + 1] * norms[1]
            comb = jnp.where(ci == heads + head, scaled, comb)
            comb = jnp.where(ci == 2 * heads + head, norms[0] * root, comb)
            comb = jnp.where(ci == 3 * heads + head, norms[1], comb)
        cols[chunk] = comb
        rows_of[chunk] = comb.T
        return carry

    lax.fori_loop(0, chunks, prepare, 0)

    def part(branch, head, chunk):
        return act[branch * heads + head, chunk * CHUNK:(chunk + 1) * CHUNK]

    def col(kind, head, chunk):
        lane = kind * heads + head
        return cols[chunk, :, lane:lane + 1]

    def row(kind, head, chunk):
        lane = kind * heads + head
        return rows_of[chunk, lane:lane + 1, :]

    sets = [(head, chunk) for head in range(heads) for chunk in range(0, chunks, 2)]
    for s, (head, first) in enumerate(sets):
        two = (first, first + 1)
        keys = [part(1, head, c) for c in two]
        gram = dot(beside(*keys), block_diagonal(*[k.T for k in keys]))
        mix = []
        for i, c in enumerate(two):
            lanes = slice(i * LANES, (i + 1) * LANES)
            gap = col(0, head, c) - row(0, head, c)
            weight = jnp.exp(jnp.minimum(gap, 0.0)) * row(1, head, c)
            mix.append((weight * gram[:, lanes] * col(3, head, c)).astype(bf16))
        mix = beside(*mix)
        mixes[s] = mix
        eye = jnp.where(ri == ci, 1.0, 0.0)
        solves[s] = beside(eye, eye) - (mix * masks[0]).astype(f32)
    for level in range(1, levels):
        lows, mids = [], []
        for s in range(len(sets)):
            low = solves[s].astype(bf16)
            lows.append(low)
            mids.append(dot(mixes[s] * masks[level], block_diagonal(low[:, :LANES], low[:, LANES:])).astype(bf16))
        for s in range(len(sets)):
            mid = mids[s]
            solves[s] = solves[s] - dot(lows[s], block_diagonal(mid[:, :LANES], mid[:, LANES:]))
    change = {}
    for s, (head, first) in enumerate(sets):
        two = (first, first + 1)
        solve = solves[s]
        new = dot(solve.astype(bf16), block_diagonal(*[part(2, head, c) for c in two]))
        grown = beside(*[jnp.exp(row(0, head, c)) * row(3, head, c) for c in two])
        back = dot((solve * grown).astype(bf16), block_diagonal(*[part(1, head, c) for c in two]))
        for i, c in enumerate(two):
            lanes = slice(i * LANES, (i + 1) * LANES)
            both = beside(back[:, lanes], new[:, lanes])
            decay = col(0, head, c)
            tail = col(1, head, c) * jnp.exp(decay[CHUNK - 1:] - decay)
            change[head, c] = dot(part(1, head, c), (both * tail).astype(bf16), (0, 0))
            both_ref[head, c] = both.astype(bf16)
    runs = {}
    for c in range(chunks):
        for head in range(heads):
            last = jnp.exp(col(0, head, c)[CHUNK - 1:])
            if c == 0:
                runs[head] = beside(
                    jnp.where(ri == ci, last, 0.0) - change[head, c][:, :LANES], change[head, c][:, LANES:]
                )
            else:
                low = runs[head].astype(bf16)
                low_ref[head, c - 1] = low
                run = last * runs[head] - dot(change[head, c][:, :LANES].astype(bf16), low)
                runs[head] = beside(run[:, :LANES], run[:, LANES:] + change[head, c][:, LANES:])
    for head in range(heads):
        x_ref[head] = runs[head].astype(bf16)


def reach_kernel(
    heads, both_ref, low_ref, act, cols, rows_of, late0_ref, late1_ref, gate_w_ref,
    qp_ref, o_ref, gate_ref,
):
    late = jnp.concatenate([late0_ref[...], late1_ref[...]], axis=0)
    gate_ref[...] = silu(dot(late, gate_w_ref[...]))
    chunks = act.shape[1] // CHUNK
    ri, ci = grid_index((CHUNK, CHUNK))
    upto = ri >= ci
    for head in range(heads):
        for c in range(chunks):
            at = slice(c * CHUNK, (c + 1) * CHUNK)

            def col(kind):
                lane = kind * heads + head
                return cols[c, :, lane:lane + 1]

            def row(kind):
                lane = kind * heads + head
                return rows_of[c, lane:lane + 1, :]

            q = act[head, at]
            score = dot(q, act[heads + head, at], (1, 1))
            weight = jnp.exp(jnp.minimum(col(0) - row(0), 0.0)) * row(1)
            attend = jnp.where(upto, weight * score * col(2), 0.0).astype(bf16)
            inner = dot(attend, both_ref[head, c])
            eff = (jnp.exp(col(0)) * col(2)) * q.astype(f32) - inner[:, :LANES]
            if c == 0:
                qp_ref[head, at] = eff.astype(bf16)
                o_ref[head, at] = inner[:, LANES:]
            else:
                ahead = dot(eff.astype(bf16), low_ref[head, c - 1])
                qp_ref[head, at] = ahead[:, :LANES].astype(bf16)
                o_ref[head, at] = inner[:, LANES:] + ahead[:, LANES:]


def convolve(heads, xp, base, taps_ref, raw, rate, bias, keep):
    ri, ci = grid_index((CHUNK, CHUNK))
    taps = taps_ref.shape[1]
    shifted = raw + bias
    soft = jnp.maximum(shifted, 0.0) + jnp.log1p(jnp.exp(-jnp.abs(shifted)))
    decay = dot((ri >= ci).astype(f32), rate * soft, precision=lax.Precision.HIGHEST)
    beta = 1.0 / (1.0 + jnp.exp(-raw))
    comb = jnp.where(ci < heads, decay, 0.0)
    root = 1.0 / math.sqrt(LANES)
    for head in range(heads):
        norms = []
        for branch in range(3):
            tile = branch * heads + head
            weights = taps_ref[branch, :, head * LANES:(head + 1) * LANES].astype(f32)
            total = None
            for i in range(taps):
                term = xp[tile, pl.ds(base + (RIM - taps + 1 + i), CHUNK)] * weights[i:i + 1]
                total = term if total is None else total + term
            value = silu(total).astype(bf16)
            keep(tile, value)
            if branch < 2:
                wide = value.astype(f32)
                norms.append(lax.rsqrt(jnp.sum(wide * wide, axis=-1, keepdims=True) + EPS))
        scaled = beta[:, heads + head:heads + head + 1] * norms[1]
        comb = jnp.where(ci == heads + head, scaled, comb)
        comb = jnp.where(ci == 2 * heads + head, norms[0] * root, comb)
        comb = jnp.where(ci == 3 * heads + head, norms[1], comb)
    return comb


def early_kernel(heads, blocks, *refs):
    count = 2 * blocks - 2
    tokens_refs = refs[:blocks]
    part_refs = refs[blocks:count]
    w_ref, small_ref, taps_ref, rate_ref, bias_ref = refs[count:count + 5]
    act, cols, rows_of, own_ref, own_sc_ref, own_rim_ref, late_rim_ref, xp, sc, tails = refs[count + 5:]
    early = blocks - 1
    span = RIM + CHUNK
    mid = early * CHUNK
    me = lax.axis_index("tp")
    before = part_refs[0][...].astype(f32)
    for ref in part_refs[1:]:
        before = before + ref[...].astype(f32)
    edge = jnp.concatenate([tokens_refs[-1][...].astype(f32), before], axis=0)
    tokens = jnp.concatenate([ref[...] for ref in tokens_refs[:-1]] + [edge.astype(bf16)], axis=0)
    raw = dot(tokens[:mid], scalar_weights(small_ref), (1, 1))
    own_sc_ref[...] = raw[:CHUNK]
    sc[...] = raw[CHUNK:]

    def fill(branch, carry):
        made = dot(tokens, w_ref[branch]).astype(bf16).astype(f32)
        for head in range(heads):
            tile = branch * heads + head
            lanes = slice(head * LANES, (head + 1) * LANES)
            own_ref[tile] = made[:CHUNK, lanes]
            for m in range(early):
                block = made[m * CHUNK:(m + 1) * CHUNK, lanes]
                if m > 0:
                    at = (m - 1) * span
                    xp[tile, at + RIM:at + span] = block
                tails[m, tile] = block[CHUNK - RIM:]
            tails[early, tile] = made[mid:mid + RIM, lanes]
            tails[blocks, tile] = made[mid + RIM:, lanes]
        return carry

    lax.fori_loop(0, 3, fill, 0)
    rate, bias = -lane_row(rate_ref), lane_row(bias_ref)

    def ahead_of(m):
        index = lax.bitwise_xor(me, m)
        return jnp.where(index == 0, blocks, lax.bitwise_xor(me, jnp.maximum(index - 1, 0)))

    own_rim_ref[...] = tails[ahead_of(0)]
    late_rim_ref[...] = tails[ahead_of(early)]

    def prepare(slot, carry):
        at = pl.ds(pl.multiple_of(slot * CHUNK, CHUNK), CHUNK)
        base = pl.multiple_of(slot * span, 8)
        source = ahead_of(slot + 1)
        for tile in range(3 * heads):
            xp[tile, pl.ds(base, RIM)] = tails[source, tile]

        def keep(tile, value):
            act[tile, at] = value

        comb = convolve(heads, xp, base, taps_ref, sc[at], rate, bias, keep)
        cols[slot] = comb
        rows_of[slot] = comb.T
        return carry

    lax.fori_loop(0, early - 1, prepare, 0)


def masks_kernel(out_ref):
    ri, ci = grid_index((CHUNK, CHUNK))
    for level in range(out_ref.shape[0]):
        hit = ((ri >> (level + 1)) == (ci >> (level + 1))) & ((ri >> level) > (ci >> level))
        hit = hit.astype(f32).astype(bf16)
        out_ref[level] = beside(hit, hit)


def block_delta_kernel(
    heads, blocks, act_e, cols_e, rows_e, own_ref, own_sc_ref, own_rim_ref, late_rim_ref,
    late0_ref, late1_ref, part0_ref, part1_ref, w_ref, small_ref, taps_ref, rate_ref, bias_ref,
    masks, x_ref, both_ref, low_ref, act_l, cols_l, rows_l, xp, sc, mixes, solves, changes, lasts,
):
    me = lax.axis_index("tp")
    span = RIM + CHUNK
    before = part0_ref[...].astype(f32) + part1_ref[...].astype(f32)
    before = jnp.concatenate([before, jnp.zeros_like(before)], axis=0)
    tokens = jnp.concatenate([late0_ref[...], late1_ref[...], before.astype(bf16)], axis=0)
    sc[:CHUNK] = own_sc_ref[...]
    sc[CHUNK:] = dot(tokens[:CHUNK], scalar_weights(small_ref), (1, 1))

    def fill(branch, carry):
        made = dot(tokens, w_ref[branch]).astype(bf16).astype(f32)
        for head in range(heads):
            tile = branch * heads + head
            lanes = slice(head * LANES, (head + 1) * LANES)
            rim = made[CHUNK:CHUNK + RIM, lanes]
            xp[tile, :RIM] = jnp.where(me == 0, rim, own_rim_ref[tile])
            xp[tile, RIM:span] = own_ref[tile]
            xp[tile, span:span + RIM] = jnp.where(me == blocks - 1, rim, late_rim_ref[tile])
            xp[tile, span + RIM:] = made[:CHUNK, lanes]
        return carry

    lax.fori_loop(0, 3, fill, 0)
    rate, bias = -lane_row(rate_ref), lane_row(bias_ref)

    def prepare(slot, carry):
        at = pl.ds(pl.multiple_of(slot * CHUNK, CHUNK), CHUNK)

        def keep(tile, value):
            act_l[tile, at] = value

        base = pl.multiple_of(slot * span, 8)
        comb = convolve(heads, xp, base, taps_ref, sc[at], rate, bias, keep)
        cols_l[slot] = comb
        rows_l[slot] = comb.T
        return carry

    lax.fori_loop(0, 2, prepare, 0)

    ri, ci = grid_index((CHUNK, CHUNK))
    levels = masks.shape[0]

    def part(branch, head, m):
        held, slot = (act_e, m - 1) if 0 < m < blocks - 1 else (act_l, min(m, 1))
        return held[branch * heads + head, slot * CHUNK:(slot + 1) * CHUNK]

    def col(kind, head, m):
        lane = kind * heads + head
        held, slot = (cols_e, m - 1) if 0 < m < blocks - 1 else (cols_l, min(m, 1))
        return held[slot, :, lane:lane + 1]

    def row(kind, head, m):
        lane = kind * heads + head
        held, slot = (rows_e, m - 1) if 0 < m < blocks - 1 else (rows_l, min(m, 1))
        return held[slot, lane:lane + 1, :]

    for m in range(blocks):
        held, slot = (cols_e, m - 1) if 0 < m < blocks - 1 else (cols_l, min(m, 1))
        lasts[m] = jnp.exp(held[slot, CHUNK - 8:])

    sets = [(head, m) for m in range(0, blocks, 2) for head in range(heads)]
    for s, (head, first) in enumerate(sets):
        two = (first, first + 1)
        keys = [part(1, head, m) for m in two]
        gram = dot(beside(*keys), block_diagonal(*[k.T for k in keys]))
        mix = []
        for i, m in enumerate(two):
            lanes = slice(i * LANES, (i + 1) * LANES)
            gap = col(0, head, m) - row(0, head, m)
            weight = jnp.exp(jnp.minimum(gap, 0.0)) * row(1, head, m)
            mix.append((weight * gram[:, lanes] * col(3, head, m)).astype(bf16))
        mix = beside(*mix)
        mixes[s] = mix
        eye = jnp.where(ri == ci, 1.0, 0.0)
        solves[s] = beside(eye, eye) - (mix * masks[0]).astype(f32)
    for level in range(1, levels):
        lows, mids = [], []
        for s in range(len(sets)):
            low = solves[s].astype(bf16)
            lows.append(low)
            mids.append(dot(mixes[s] * masks[level], block_diagonal(low[:, :LANES], low[:, LANES:])).astype(bf16))
        for s in range(len(sets)):
            mid = mids[s]
            solves[s] = solves[s] - dot(lows[s], block_diagonal(mid[:, :LANES], mid[:, LANES:]))
    for s, (head, first) in enumerate(sets):
        two = (first, first + 1)
        solve = solves[s]
        new = dot(solve.astype(bf16), block_diagonal(*[part(2, head, m) for m in two]))
        grown = beside(*[jnp.exp(row(0, head, m)) * row(3, head, m) for m in two])
        back = dot((solve * grown).astype(bf16), block_diagonal(*[part(1, head, m) for m in two]))
        for i, m in enumerate(two):
            lanes = slice(i * LANES, (i + 1) * LANES)
            both = beside(back[:, lanes], new[:, lanes])
            decay = col(0, head, m)
            tail = col(1, head, m) * jnp.exp(decay[CHUNK - 1:] - decay)
            changes[m, head] = dot(part(1, head, m), (both * tail).astype(bf16), (0, 0))
            both_ref[head, m] = both.astype(bf16)
    eye = jnp.where(ri == ci, 1.0, 0.0)
    runs = {}
    for step in range(blocks):
        m = lax.bitwise_xor(me, step)
        for head in range(heads):
            last = lasts[m, 7:, head:head + 1]
            change = changes[m, head]
            if step == 0:
                low_ref[head, m] = beside(eye, jnp.zeros_like(eye)).astype(bf16)
                runs[head] = beside(last * eye - change[:, :LANES], change[:, LANES:])
            else:
                low = runs[head].astype(bf16)
                low_ref[head, m] = low
                run = last * runs[head] - dot(change[:, :LANES].astype(bf16), low)
                runs[head] = beside(run[:, :LANES], run[:, LANES:] + change[:, LANES:])
    for head in range(heads):
        x_ref[head] = runs[head].astype(bf16)


def block_reach_kernel(
    heads, blocks, both_ref, low_ref, act_e, cols_e, rows_e, act_l, cols_l, rows_l,
    qp_ref, o_ref,
):
    ri, ci = grid_index((CHUNK, CHUNK))
    upto = ri >= ci
    for head in range(heads):
        for m in range(blocks):
            at = slice(m * CHUNK, (m + 1) * CHUNK)
            middle = 0 < m < blocks - 1
            slot = m - 1 if middle else min(m, 1)
            act, cols_of, rows_of = (act_e, cols_e, rows_e) if middle else (act_l, cols_l, rows_l)
            held = slice(slot * CHUNK, (slot + 1) * CHUNK)
            cols, rows = cols_of[slot], rows_of[slot]
            q, k = act[head, held], act[heads + head, held]
            decay = cols[:, head:head + 1]
            norm = cols[:, 2 * heads + head:2 * heads + head + 1]
            gap = decay - rows[head:head + 1]
            weight = jnp.exp(jnp.minimum(gap, 0.0)) * rows[heads + head:heads + head + 1]
            attend = jnp.where(upto, weight * dot(q, k, (1, 1)) * norm, 0.0).astype(bf16)
            inner = dot(attend, both_ref[head, m])
            eff = (jnp.exp(decay) * norm) * q.astype(f32) - inner[:, :LANES]
            ahead = dot(eff.astype(bf16), low_ref[head, m])
            qp_ref[head, at] = ahead[:, :LANES].astype(bf16)
            o_ref[head, at] = inner[:, LANES:] + ahead[:, LANES:]


def gate_kernel(count, *refs):
    w_ref = refs[count]
    outs = refs[count + 1:]
    tokens = jnp.concatenate([ref[...] for ref in refs[:count]], axis=0)
    gate = silu(dot(tokens, w_ref[...]))
    start = 0
    for out in outs:
        out[...] = gate[start:start + out.shape[0]]
        start += out.shape[0]


def pair_kernel(share, mine_ref, other_ref, out_ref):
    core = lax.axis_index("seq") & 1
    for j in range(out_ref.shape[0]):
        head = core * out_ref.shape[0] + j if share else j
        mine, other = mine_ref[head], other_ref[head]
        first = jnp.where(core == 0, mine, other)
        second = jnp.where(core == 0, other, mine)
        both = dot(second[:, :LANES], first)
        out_ref[j, :, :LANES] = both[:, :LANES].astype(bf16)
        out_ref[j, :, LANES:] = (both[:, LANES:] + second[:, LANES:].astype(f32)).astype(bf16)


def climb_kernel(bit, inside_ref, block_ref, sent_ref, inside_out, block_out):
    upper = (lax.axis_index("seq") >> (bit + 1)) & 1
    for j in range(block_ref.shape[0]):
        sent = sent_ref[j]
        for ref, out in ((inside_ref, inside_out), (block_ref, block_out)):
            mine = ref[j]
            both = dot(mine[:, :LANES], sent)
            left = jnp.where(upper == 1, both[:, :LANES], mine[:, :LANES].astype(f32))
            right = mine[:, LANES:].astype(f32) + both[:, LANES:]
            out[j] = jnp.concatenate([left, right], axis=1).astype(bf16)


def first_kernel(block_ref, sent_ref, inside_out, block_out):
    upper = (lax.axis_index("seq") >> 1) & 1
    ri, ci = grid_index((LANES, LANES))
    eye = jnp.where(ri == ci, 1.0, 0.0)
    for j in range(block_ref.shape[0]):
        sent, mine = sent_ref[j], block_ref[j]
        both = dot(mine[:, :LANES], sent)
        left = jnp.where(upper == 1, both[:, :LANES], mine[:, :LANES].astype(f32))
        right = mine[:, LANES:].astype(f32) + both[:, LANES:]
        block_out[j] = jnp.concatenate([left, right], axis=1).astype(bf16)
        inside = jnp.where(upper == 1, sent[:, :LANES].astype(f32), eye)
        inside_out[j] = jnp.concatenate([inside.astype(bf16), sent[:, LANES:]], axis=1)


def fold_kernel(inside_ref, *refs):
    out_ref = refs[-1]
    for j in range(out_ref.shape[0]):
        state = refs[0][j]
        for ref in refs[1:-1]:
            state = state + ref[j]
        inside = inside_ref[j]
        state = inside[:, LANES:].astype(f32) + dot(inside[:, :LANES], state)
        out_ref[j] = state.astype(bf16)


def final_kernel(
    share, blocks, ordered, qp_ref, o_ref, pair_ref, mine_ref, other_ref,
    own_gate_ref, gate_ref, late_gate_ref, gain_ref, out_ref,
):
    heads, seq_rows, dim = qp_ref.shape
    rows = seq_rows // blocks
    core, me = lax.axis_index("seq") & 1, lax.axis_index("tp")
    part = mine_ref.shape[0]
    for head in range(heads):
        start = mine_ref[head % part]
        if share:
            start = jnp.where(core == head // part, start, other_ref[head % part])
        pair = pair_ref[head]
        moved = pair[:, dim:].astype(f32) + dot(pair[:, :dim], start)
        start = jnp.where(core == 0, start.astype(f32), moved).astype(bf16)
        lanes = slice(head * dim, (head + 1) * dim)
        for m in range(blocks):
            if m == 0:
                gate = own_gate_ref[:, lanes]
            elif m < blocks - 1:
                gate = gate_ref[(m - 1) * rows:m * rows, lanes]
            else:
                gate = late_gate_ref[:, lanes]
            at = pl.ds(pl.multiple_of(lax.bitwise_xor(me, m) * rows, 8), rows)
            held = at if ordered else slice(m * rows, (m + 1) * rows)
            y = o_ref[head, held] + dot(qp_ref[head, held], start)
            scale = lax.rsqrt(jnp.mean(y * y, axis=-1, keepdims=True) + EPS)
            out_ref[at, lanes] = (y * scale * gain_ref[...] * gate).astype(bf16)


def call(kernel, out, operands, flops=0, scratch=(), limit=24):
    single = not isinstance(out, tuple)
    return pl.pallas_call(
        kernel,
        out_shape=out,
        in_specs=[whole()] * len(operands),
        out_specs=whole() if single else (whole(),) * len(out),
        scratch_shapes=scratch,
        cost_estimate=pl.CostEstimate(flops=flops, transcendentals=0, bytes_accessed=1 << 20),
        compiler_params=pltpu.CompilerParams(vmem_limit_bytes=limit << 20),
    )(*operands)


def per_device(hidden, w_qkv, w_gate, w_decay_beta, conv_weight, decay_rate, dt_bias, norm_gain):
    heads = decay_rate.shape[0]
    dim = norm_gain.shape[0]
    columns = heads * dim
    blocks = lax.axis_size("tp")
    seq_count = lax.axis_size("seq")
    rows = hidden.shape[0]
    seq_rows = rows * blocks
    chunks = seq_rows // CHUNK
    shape = jax.ShapeDtypeStruct

    w_three = w_qkv.transpose(1, 0, 2)
    small = w_decay_beta.transpose(1, 2, 0)
    taps = conv_weight.transpose(1, 0, 2)
    rate, bias = decay_rate.reshape(1, heads), dt_bias.reshape(1, heads)

    early, late = gather_blocks(hidden, "tp")
    weights = [w_three, w_gate, small]

    def project(tokens, count, extra=0):
        return call(
            functools.partial(project_kernel, len(tokens)),
            (
                shape((3, count + extra, columns), bf16),
                shape((count, columns), f32),
                shape((count, LANES), f32),
            ),
            [*tokens, *weights], flops=PROJECT_FLOPS, limit=20,
        )

    by_block = rows == CHUNK and len(early) == blocks - 2 and blocks > 2
    if by_block:
        parts, across = rim_rows(hidden, RIM)
        masks = call(
            masks_kernel,
            shape((CHUNK.bit_length() - 1, CHUNK, 2 * CHUNK), bf16), [],
            flops=MASKS_FLOPS, limit=4,
        )
        act_e, cols_e, rows_e, own_f, own_sc, own_rim, late_rim = call(
            functools.partial(early_kernel, heads, blocks),
            (
                shape((3 * heads, seq_rows - 2 * rows, dim), bf16),
                shape((blocks - 2, CHUNK, LANES), f32),
                shape((blocks - 2, CHUNK, LANES), f32),
                shape((3 * heads, rows, dim), f32),
                shape((rows, LANES), f32),
                shape((3 * heads, RIM, dim), f32),
                shape((3 * heads, RIM, dim), f32),
            ),
            [
                hidden, *early, across, *parts[1:-1],
                w_three, small, taps, rate, bias,
            ],
            flops=PROJECT_FLOPS,
            scratch=[
                pltpu.VMEM((3 * heads, (blocks - 2) * (RIM + CHUNK), dim), f32),
                pltpu.VMEM((seq_rows - 2 * rows, LANES), f32),
                pltpu.VMEM((blocks + 1, 3 * heads, RIM, dim), f32),
            ],
        )
        own, both, low, act_l, cols_l, rows_l = call(
            functools.partial(block_delta_kernel, heads, blocks),
            (
                shape((heads, dim, 2 * dim), bf16),
                shape((heads, blocks, CHUNK, 2 * dim), bf16),
                shape((heads, blocks, dim, 2 * dim), bf16),
                shape((3 * heads, 2 * rows, dim), bf16),
                shape((2, CHUNK, LANES), f32),
                shape((2, CHUNK, LANES), f32),
            ),
            [
                act_e, cols_e, rows_e, own_f, own_sc, own_rim, late_rim, *late,
                parts[0], parts[-1], w_three, small, taps, rate, bias, masks,
            ],
            flops=DELTA_FLOPS, limit=28,
            scratch=[
                pltpu.VMEM((3 * heads, 2 * (RIM + CHUNK), dim), f32),
                pltpu.VMEM((2 * rows, LANES), f32),
                pltpu.VMEM((heads * blocks // 2, CHUNK, 2 * CHUNK), bf16),
                pltpu.VMEM((heads * blocks // 2, CHUNK, 2 * CHUNK), f32),
                pltpu.VMEM((blocks, heads, dim, 2 * dim), f32),
                pltpu.VMEM((blocks, 8, LANES), f32),
            ],
        )
        reach, base = call(
            functools.partial(block_reach_kernel, heads, blocks),
            (
                shape((heads, seq_rows, dim), bf16),
                shape((heads, seq_rows, dim), f32),
            ),
            [both, low, act_e, cols_e, rows_e, act_l, cols_l, rows_l],
            flops=REACH_FLOPS, limit=14,
        )
        tokens = [hidden, *early, *late]
        own_gate, mid_gate, late_gate = call(
            functools.partial(gate_kernel, len(tokens)),
            (
                shape((rows, columns), f32),
                shape((seq_rows - 2 * rows, columns), f32),
                shape((rows, columns), f32),
            ),
            [*tokens, w_gate], flops=PROJECT_FLOPS, limit=14,
        )
    else:
        own_p, own_gate, own_sc = project([hidden], rows)
        parts, _ = rim_rows(hidden, RIM)
        rim = sum(parts[1:], parts[0])
        mid_p, mid_gate, mid_sc = project([*early, rim], seq_rows - 2 * rows, RIM)
        own, both, low, act, cols, rows_of = call(
            functools.partial(delta_kernel, heads, blocks),
            (
                shape((heads, dim, 2 * dim), bf16),
                shape((heads, chunks, CHUNK, 2 * dim), bf16),
                shape((heads, chunks - 1, dim, 2 * dim), bf16),
                shape((3 * heads, seq_rows, dim), bf16),
                shape((chunks, CHUNK, LANES), f32),
                shape((chunks, CHUNK, LANES), f32),
            ),
            [own_p, own_sc, mid_p, mid_sc, *late, w_three, small, taps, rate, bias],
            flops=DELTA_FLOPS, limit=32,
            scratch=[
                pltpu.VMEM((3 * heads, seq_rows + RIM, dim), f32),
                pltpu.VMEM((seq_rows, LANES), f32),
                pltpu.VMEM((CHUNK.bit_length() - 1, CHUNK, 2 * CHUNK), bf16),
                pltpu.VMEM((heads * chunks // 2, CHUNK, 2 * CHUNK), bf16),
                pltpu.VMEM((heads * chunks // 2, CHUNK, 2 * CHUNK), f32),
            ],
        )
        reach, base, late_gate = call(
            functools.partial(reach_kernel, heads),
            (
                shape((heads, seq_rows, dim), bf16),
                shape((heads, seq_rows, dim), f32),
                shape((rows, columns), f32),
            ),
            [both, low, act, cols, rows_of, *late, w_gate], flops=REACH_FLOPS, limit=12,
        )

    share = heads % 2 == 0
    part = heads // 2 if share else heads
    swap = [(i, i ^ 1) for i in range(seq_count)]
    other = lax.ppermute(own, "seq", swap)
    block = call(
        functools.partial(pair_kernel, share),
        shape((part, dim, 2 * dim), bf16), [own, other], flops=SMALL_FLOPS, limit=4,
    )
    chips = seq_count // 2
    levels = chips.bit_length() - 1
    inside = None
    for level in range(levels):
        size = 1 << level
        sent = block if level < levels - 1 or level == 0 else block[:, :, dim:]
        parts = []
        for target in range(size):
            route = []
            for top in range(size - 1, chips, 2 * size):
                for c in range(2):
                    route.append((2 * top + c, 2 * (top + 1 + target) + c))
            parts.append(lax.ppermute(sent, "seq", route))
        if level == levels - 1 and level > 0:
            break
        sent = sum(parts[1:], parts[0])
        kernel, operands = first_kernel, [block, sent]
        if level > 0:
            kernel, operands = functools.partial(climb_kernel, level), [inside, block, sent]
        inside, block = call(
            kernel, (shape(block.shape, bf16),) * 2, operands, flops=SMALL_FLOPS, limit=4,
        )
    state = call(
        fold_kernel, shape((part, dim, dim), bf16), [inside, *parts],
        flops=SMALL_FLOPS, limit=4,
    )
    back = lax.ppermute(state, "seq", swap) if share else state
    return call(
        functools.partial(final_kernel, share, blocks, not by_block), shape((seq_rows, columns), bf16),
        [reach, base, other, state, back, own_gate, mid_gate, late_gate, norm_gain.reshape(1, dim)],
        flops=SMALL_FLOPS, limit=12,
    )


def solution(mesh):
    return jax.shard_map(
        per_device,
        mesh=mesh,
        in_specs=(
            P(("seq", "tp"), None),
            P(None, None, "tp"),
            P(None, "tp"),
            P(None, None, "tp"),
            P(None, None, "tp"),
            P("tp"),
            P("tp"),
            P(),
        ),
        out_specs=P("seq", "tp"),
        check_vma=False,
    )
```

```python
import functools
import math

import jax
import jax.numpy as jnp
from jax import lax
from jax.experimental import pallas as pl
from jax.experimental.pallas import tpu as pltpu
from jax.sharding import PartitionSpec as P


CHUNK = 128
LANES = 128
RIM = 8
EPS = 1e-6
PROJECT_FLOPS = 3000000000
DELTA_FLOPS = 3000000000
REACH_FLOPS = 2000000000
SMALL_FLOPS = 50000000
MASKS_FLOPS = 8000000000


f32 = jnp.float32
bf16 = jnp.bfloat16


def dot(left, right, contract=(1, 0), precision=None):
    dims = (((contract[0],), (contract[1],)), ((), ()))
    return lax.dot_general(left, right, dims, precision=precision, preferred_element_type=f32)


def whole(memory=pltpu.VMEM):
    return pl.BlockSpec(memory_space=memory)


def gather_blocks(block, axis):
    count = lax.axis_size(axis)
    bits = count.bit_length() - 1
    half = block.shape[0] // 2

    def swap(value, bit):
        step = 1 << bit
        return lax.ppermute(value, axis, [(i, i ^ step) for i in range(count)])

    found = {0: block}
    for bit in range(bits):
        found[1 << bit] = swap(block, bit)
    halves = []
    for number, order in enumerate((range(bits), range(bits - 1, -1, -1))):
        part = {m: value[number * half:(number + 1) * half] for m, value in found.items()}
        for bit in order:
            for mask in list(part):
                if mask | (1 << bit) not in part:
                    part[mask | (1 << bit)] = swap(part[mask], bit)
        halves.append(part)
    early = [found[m] if m in found else (halves[0][m], halves[1][m]) for m in range(count - 1)]
    flat = []
    for item in early[1:]:
        flat.extend(item if isinstance(item, tuple) else (item,))
    return flat, [halves[0][count - 1], halves[1][count - 1]]


def rim_rows(block, count):
    seq_count, tp_count = lax.axis_size("seq"), lax.axis_size("tp")
    tail = block[-count:]
    parts = []
    for j in range(tp_count):
        route = [(s * tp_count - 1, s * tp_count + j) for s in range(1, seq_count)]
        parts.append(lax.ppermute(tail, ("seq", "tp"), route))
    route = [(i, tp_count - 1 - i) for i in range(tp_count)]
    across = lax.ppermute(tail, "tp", route)
    return parts, across


def silu(x):
    return x / (1.0 + jnp.exp(-x))


def scalar_weights(ref):
    kinds, heads, width = ref.shape
    rows = [ref[kind].astype(f32) for kind in range(kinds)]
    rows.append(jnp.zeros((LANES - kinds * heads, width), f32))
    return jnp.concatenate(rows, axis=0).astype(bf16)


def lane_row(ref):
    lane = lax.broadcasted_iota(jnp.int32, (1, LANES), 1)
    row = jnp.zeros((1, LANES), f32)
    for head in range(ref.shape[1]):
        row = jnp.where(lane == head, ref[:, head:head + 1], row)
    return row


def project_kernel(count, *refs):
    blocks = refs[:count]
    w_ref, gate_w_ref, small_ref = refs[count:count + 3]
    p_ref, gate_ref, sc_ref = refs[count + 3:count + 6]
    rows = sc_ref.shape[0]
    tokens = jnp.concatenate([ref[...] for ref in blocks], axis=0)
    sc_ref[...] = dot(tokens, scalar_weights(small_ref), (1, 1))[:rows]
    gate_ref[...] = silu(dot(tokens, gate_w_ref[...])[:rows])

    def one(branch, carry):
        p_ref[branch] = dot(tokens, w_ref[branch]).astype(bf16)
        return carry

    lax.fori_loop(0, w_ref.shape[0], one, 0)


def block_diagonal(left, right):
    hole = jnp.zeros_like(left)
    return jnp.concatenate(
        [jnp.concatenate([left, hole], axis=1), jnp.concatenate([hole, right], axis=1)], axis=0
    )


def beside(left, right):
    return jnp.concatenate([left, right], axis=1)


def grid_index(shape):
    return lax.broadcasted_iota(jnp.int32, shape, 0), lax.broadcasted_iota(jnp.int32, shape, 1)


def delta_kernel(
    heads, blocks, own_ref, own_sc_ref, p_ref, sc_ref, late0_ref, late1_ref, w_ref,
    small_ref, taps_ref, rate_ref, bias_ref, x_ref, both_ref, low_ref, act, cols, rows_of,
    xp, sc, masks, mixes, solves,
):
    seq_rows = act.shape[1]
    rows = seq_rows // blocks
    chunks = seq_rows // CHUNK
    taps = taps_ref.shape[1]
    me = lax.axis_index("tp")

    def place(m, offset=0):
        return pl.multiple_of(offset + lax.bitwise_xor(me, m) * rows, 8)

    late = jnp.concatenate([late0_ref[...], late1_ref[...]], axis=0)
    sc[pl.ds(place(blocks - 1), rows)] = dot(late, scalar_weights(small_ref), (1, 1))
    sc[pl.ds(place(0), rows)] = own_sc_ref[...]
    for m in range(1, blocks - 1):
        sc[pl.ds(place(m), rows)] = sc_ref[(m - 1) * rows:m * rows]

    def fill(branch, carry):
        made = dot(late, w_ref[branch]).astype(bf16).astype(f32)
        for head in range(heads):
            tile = branch * heads + head
            lanes = slice(head * LANES, (head + 1) * LANES)
            xp[tile, :RIM] = p_ref[branch, (blocks - 2) * rows:, lanes].astype(f32)
            xp[tile, pl.ds(place(0, RIM), rows)] = own_ref[branch, :, lanes].astype(f32)
            xp[tile, pl.ds(place(blocks - 1, RIM), rows)] = made[:, lanes]
            for m in range(1, blocks - 1):
                block = p_ref[branch, (m - 1) * rows:m * rows, lanes]
                xp[tile, pl.ds(place(m, RIM), rows)] = block.astype(f32)
        return carry

    lax.fori_loop(0, 3, fill, 0)

    ri, ci = grid_index((CHUNK, CHUNK))
    upto = ri >= ci
    lower = upto.astype(f32)
    levels = CHUNK.bit_length() - 1
    for level in range(levels):
        hit = ((ri >> (level + 1)) == (ci >> (level + 1))) & ((ri >> level) > (ci >> level))
        hit = hit.astype(f32).astype(bf16)
        masks[level] = beside(hit, hit)

    root = 1.0 / math.sqrt(LANES)
    rate, bias = -lane_row(rate_ref), lane_row(bias_ref)

    def prepare(chunk, carry):
        base = pl.multiple_of(chunk * CHUNK, CHUNK)
        raw = sc[pl.ds(base, CHUNK)]
        shifted = raw + bias
        soft = jnp.maximum(shifted, 0.0) + jnp.log1p(jnp.exp(-jnp.abs(shifted)))
        decay = dot(lower, rate * soft, precision=lax.Precision.HIGHEST)
        beta = 1.0 / (1.0 + jnp.exp(-raw))
        comb = jnp.where(ci < heads, decay, 0.0)
        for head in range(heads):
            norms = []
            for branch in range(3):
                tile = branch * heads + head
                weights = taps_ref[branch, :, head * LANES:(head + 1) * LANES].astype(f32)
                total = None
                for i in range(taps):
                    term = xp[tile, pl.ds(base + (RIM - taps + 1 + i), CHUNK)] * weights[i:i + 1]
                    total = term if total is None else total + term
                value = silu(total).astype(bf16)
                act[tile, pl.ds(base, CHUNK)] = value
                if branch < 2:
                    wide = value.astype(f32)
                    norms.append(lax.rsqrt(jnp.sum(wide * wide, axis=-1, keepdims=True) + EPS))
            scaled = beta[:, heads + head:heads + head + 1] * norms[1]
            comb = jnp.where(ci == heads + head, scaled, comb)
            comb = jnp.where(ci == 2 * heads + head, norms[0] * root, comb)
            comb = jnp.where(ci == 3 * heads + head, norms[1], comb)
        cols[chunk] = comb
        rows_of[chunk] = comb.T
        return carry

    lax.fori_loop(0, chunks, prepare, 0)

    def part(branch, head, chunk):
        return act[branch * heads + head, chunk * CHUNK:(chunk + 1) * CHUNK]

    def col(kind, head, chunk):
        lane = kind * heads + head
        return cols[chunk, :, lane:lane + 1]

    def row(kind, head, chunk):
        lane = kind * heads + head
        return rows_of[chunk, lane:lane + 1, :]

    sets = [(head, chunk) for head in range(heads) for chunk in range(0, chunks, 2)]
    for s, (head, first) in enumerate(sets):
        two = (first, first + 1)
        keys = [part(1, head, c) for c in two]
        gram = dot(beside(*keys), block_diagonal(*[k.T for k in keys]))
        mix = []
        for i, c in enumerate(two):
            lanes = slice(i * LANES, (i + 1) * LANES)
            gap = col(0, head, c) - row(0, head, c)
            weight = jnp.exp(jnp.minimum(gap, 0.0)) * row(1, head, c)
            mix.append((weight * gram[:, lanes] * col(3, head, c)).astype(bf16))
        mix = beside(*mix)
        mixes[s] = mix
        eye = jnp.where(ri == ci, 1.0, 0.0)
        solves[s] = beside(eye, eye) - (mix * masks[0]).astype(f32)
    for level in range(1, levels):
        lows, mids = [], []
        for s in range(len(sets)):
            low = solves[s].astype(bf16)
            lows.append(low)
            mids.append(dot(mixes[s] * masks[level], block_diagonal(low[:, :LANES], low[:, LANES:])).astype(bf16))
        for s in range(len(sets)):
            mid = mids[s]
            solves[s] = solves[s] - dot(lows[s], block_diagonal(mid[:, :LANES], mid[:, LANES:]))
    change = {}
    for s, (head, first) in enumerate(sets):
        two = (first, first + 1)
        solve = solves[s]
        new = dot(solve.astype(bf16), block_diagonal(*[part(2, head, c) for c in two]))
        grown = beside(*[jnp.exp(row(0, head, c)) * row(3, head, c) for c in two])
        back = dot((solve * grown).astype(bf16), block_diagonal(*[part(1, head, c) for c in two]))
        for i, c in enumerate(two):
            lanes = slice(i * LANES, (i + 1) * LANES)
            both = beside(back[:, lanes], new[:, lanes])
            decay = col(0, head, c)
            tail = col(1, head, c) * jnp.exp(decay[CHUNK - 1:] - decay)
            change[head, c] = dot(part(1, head, c), (both * tail).astype(bf16), (0, 0))
            both_ref[head, c] = both.astype(bf16)
    runs = {}
    for c in range(chunks):
        for head in range(heads):
            last = jnp.exp(col(0, head, c)[CHUNK - 1:])
            if c == 0:
                runs[head] = beside(
                    jnp.where(ri == ci, last, 0.0) - change[head, c][:, :LANES], change[head, c][:, LANES:]
                )
            else:
                low = runs[head].astype(bf16)
                low_ref[head, c - 1] = low
                run = last * runs[head] - dot(change[head, c][:, :LANES].astype(bf16), low)
                runs[head] = beside(run[:, :LANES], run[:, LANES:] + change[head, c][:, LANES:])
    for head in range(heads):
        x_ref[head] = runs[head].astype(bf16)


def reach_kernel(
    heads, both_ref, low_ref, act, cols, rows_of, late0_ref, late1_ref, gate_w_ref,
    qp_ref, o_ref, gate_ref,
):
    late = jnp.concatenate([late0_ref[...], late1_ref[...]], axis=0)
    gate_ref[...] = silu(dot(late, gate_w_ref[...]))
    chunks = act.shape[1] // CHUNK
    ri, ci = grid_index((CHUNK, CHUNK))
    upto = ri >= ci
    for head in range(heads):
        for c in range(chunks):
            at = slice(c * CHUNK, (c + 1) * CHUNK)

            def col(kind):
                lane = kind * heads + head
                return cols[c, :, lane:lane + 1]

            def row(kind):
                lane = kind * heads + head
                return rows_of[c, lane:lane + 1, :]

            q = act[head, at]
            score = dot(q, act[heads + head, at], (1, 1))
            weight = jnp.exp(jnp.minimum(col(0) - row(0), 0.0)) * row(1)
            attend = jnp.where(upto, weight * score * col(2), 0.0).astype(bf16)
            inner = dot(attend, both_ref[head, c])
            eff = (jnp.exp(col(0)) * col(2)) * q.astype(f32) - inner[:, :LANES]
            if c == 0:
                qp_ref[head, at] = eff.astype(bf16)
                o_ref[head, at] = inner[:, LANES:]
            else:
                ahead = dot(eff.astype(bf16), low_ref[head, c - 1])
                qp_ref[head, at] = ahead[:, :LANES].astype(bf16)
                o_ref[head, at] = inner[:, LANES:] + ahead[:, LANES:]


def convolve(heads, xp, base, taps_ref, raw, rate, bias, keep):
    ri, ci = grid_index((CHUNK, CHUNK))
    taps = taps_ref.shape[1]
    shifted = raw + bias
    soft = jnp.maximum(shifted, 0.0) + jnp.log1p(jnp.exp(-jnp.abs(shifted)))
    decay = dot((ri >= ci).astype(f32), rate * soft, precision=lax.Precision.HIGHEST)
    beta = 1.0 / (1.0 + jnp.exp(-raw))
    comb = jnp.where(ci < heads, decay, 0.0)
    root = 1.0 / math.sqrt(LANES)
    for head in range(heads):
        norms = []
        for branch in range(3):
            tile = branch * heads + head
            weights = taps_ref[branch, :, head * LANES:(head + 1) * LANES].astype(f32)
            total = None
            for i in range(taps):
                term = xp[tile, pl.ds(base + (RIM - taps + 1 + i), CHUNK)] * weights[i:i + 1]
                total = term if total is None else total + term
            value = silu(total).astype(bf16)
            keep(tile, value)
            if branch < 2:
                wide = value.astype(f32)
                norms.append(lax.rsqrt(jnp.sum(wide * wide, axis=-1, keepdims=True) + EPS))
        scaled = beta[:, heads + head:heads + head + 1] * norms[1]
        comb = jnp.where(ci == heads + head, scaled, comb)
        comb = jnp.where(ci == 2 * heads + head, norms[0] * root, comb)
        comb = jnp.where(ci == 3 * heads + head, norms[1], comb)
    return comb


def early_kernel(heads, blocks, *refs):
    count = 2 * blocks
    tokens_refs = refs[:blocks]
    part_refs = refs[blocks:count]
    w_ref, small_ref, taps_ref, rate_ref, bias_ref = refs[count:count + 5]
    act, cols, rows_of, rim_ref, xp, sc, tails = refs[count + 5:]
    early = blocks - 1
    span = RIM + CHUNK
    mid = early * CHUNK
    me = lax.axis_index("tp")
    before = part_refs[0][...].astype(f32)
    for ref in part_refs[1:]:
        before = before + ref[...].astype(f32)
    edge = jnp.concatenate([tokens_refs[-1][...].astype(f32), before], axis=0)
    tokens = jnp.concatenate([ref[...] for ref in tokens_refs[:-1]] + [edge.astype(bf16)], axis=0)
    sc[...] = dot(tokens[:mid], scalar_weights(small_ref), (1, 1))

    def fill(branch, carry):
        made = dot(tokens, w_ref[branch]).astype(bf16).astype(f32)
        for head in range(heads):
            tile = branch * heads + head
            lanes = slice(head * LANES, (head + 1) * LANES)
            for m in range(early):
                at = m * span
                block = made[m * CHUNK:(m + 1) * CHUNK, lanes]
                xp[tile, at + RIM:at + span] = block
                tails[m, tile] = block[CHUNK - RIM:]
            tails[early, tile] = made[mid:mid + RIM, lanes]
            tails[blocks, tile] = made[mid + RIM:, lanes]
        return carry

    lax.fori_loop(0, 3, fill, 0)
    rate, bias = -lane_row(rate_ref), lane_row(bias_ref)

    def ahead_of(m):
        index = lax.bitwise_xor(me, m)
        return jnp.where(index == 0, blocks, lax.bitwise_xor(me, jnp.maximum(index - 1, 0)))

    rim_ref[...] = tails[ahead_of(early)]

    def prepare(m, carry):
        at = pl.ds(pl.multiple_of(m * CHUNK, CHUNK), CHUNK)
        base = pl.multiple_of(m * span, 8)
        source = ahead_of(m)
        for tile in range(3 * heads):
            xp[tile, pl.ds(base, RIM)] = tails[source, tile]

        def keep(tile, value):
            act[tile, at] = value

        comb = convolve(heads, xp, base, taps_ref, sc[at], rate, bias, keep)
        cols[m] = comb
        rows_of[m] = comb.T
        return carry

    lax.fori_loop(0, early, prepare, 0)


def masks_kernel(out_ref):
    ri, ci = grid_index((CHUNK, CHUNK))
    for level in range(out_ref.shape[0]):
        hit = ((ri >> (level + 1)) == (ci >> (level + 1))) & ((ri >> level) > (ci >> level))
        hit = hit.astype(f32).astype(bf16)
        out_ref[level] = beside(hit, hit)


def block_delta_kernel(
    heads, blocks, act_e, cols_e, rows_e, rim_ref, late0_ref, late1_ref, w_ref, small_ref,
    taps_ref, rate_ref, bias_ref, masks, x_ref, both_ref, low_ref, act_l, cols_l, rows_l,
    xp, mixes, solves, changes, lasts,
):
    me = lax.axis_index("tp")
    late = jnp.concatenate([late0_ref[...], late1_ref[...]], axis=0)
    raw = dot(late, scalar_weights(small_ref), (1, 1))

    def fill(branch, carry):
        made = dot(late, w_ref[branch]).astype(bf16).astype(f32)
        for head in range(heads):
            tile = branch * heads + head
            lanes = slice(head * LANES, (head + 1) * LANES)
            xp[tile, :RIM] = rim_ref[tile]
            xp[tile, RIM:] = made[:, lanes]
        return carry

    lax.fori_loop(0, 3, fill, 0)

    def keep(tile, value):
        act_l[tile] = value

    comb = convolve(
        heads, xp, 0, taps_ref, raw, -lane_row(rate_ref), lane_row(bias_ref), keep
    )
    cols_l[0] = comb
    rows_l[0] = comb.T

    ri, ci = grid_index((CHUNK, CHUNK))
    levels = masks.shape[0]

    def part(branch, head, m):
        tile = branch * heads + head
        if m == blocks - 1:
            return act_l[tile]
        return act_e[tile, m * CHUNK:(m + 1) * CHUNK]

    def col(kind, head, m):
        lane = kind * heads + head
        if m == blocks - 1:
            return cols_l[0, :, lane:lane + 1]
        return cols_e[m, :, lane:lane + 1]

    def row(kind, head, m):
        lane = kind * heads + head
        if m == blocks - 1:
            return rows_l[0, lane:lane + 1, :]
        return rows_e[m, lane:lane + 1, :]

    for m in range(blocks):
        source = cols_l[0] if m == blocks - 1 else cols_e[m]
        lasts[m] = jnp.exp(source[CHUNK - 8:])

    sets = [(head, m) for m in range(0, blocks, 2) for head in range(heads)]
    for s, (head, first) in enumerate(sets):
        two = (first, first + 1)
        keys = [part(1, head, m) for m in two]
        gram = dot(beside(*keys), block_diagonal(*[k.T for k in keys]))
        mix = []
        for i, m in enumerate(two):
            lanes = slice(i * LANES, (i + 1) * LANES)
            gap = col(0, head, m) - row(0, head, m)
            weight = jnp.exp(jnp.minimum(gap, 0.0)) * row(1, head, m)
            mix.append((weight * gram[:, lanes] * col(3, head, m)).astype(bf16))
        mix = beside(*mix)
        mixes[s] = mix
        eye = jnp.where(ri == ci, 1.0, 0.0)
        solves[s] = beside(eye, eye) - (mix * masks[0]).astype(f32)
    for level in range(1, levels):
        lows, mids = [], []
        for s in range(len(sets)):
            low = solves[s].astype(bf16)
            lows.append(low)
            mids.append(dot(mixes[s] * masks[level], block_diagonal(low[:, :LANES], low[:, LANES:])).astype(bf16))
        for s in range(len(sets)):
            mid = mids[s]
            solves[s] = solves[s] - dot(lows[s], block_diagonal(mid[:, :LANES], mid[:, LANES:]))
    for s, (head, first) in enumerate(sets):
        two = (first, first + 1)
        solve = solves[s]
        new = dot(solve.astype(bf16), block_diagonal(*[part(2, head, m) for m in two]))
        grown = beside(*[jnp.exp(row(0, head, m)) * row(3, head, m) for m in two])
        back = dot((solve * grown).astype(bf16), block_diagonal(*[part(1, head, m) for m in two]))
        for i, m in enumerate(two):
            lanes = slice(i * LANES, (i + 1) * LANES)
            both = beside(back[:, lanes], new[:, lanes])
            decay = col(0, head, m)
            tail = col(1, head, m) * jnp.exp(decay[CHUNK - 1:] - decay)
            changes[m, head] = dot(part(1, head, m), (both * tail).astype(bf16), (0, 0))
            both_ref[head, m] = both.astype(bf16)
    eye = jnp.where(ri == ci, 1.0, 0.0)
    runs = {}
    for step in range(blocks):
        m = lax.bitwise_xor(me, step)
        for head in range(heads):
            last = lasts[m, 7:, head:head + 1]
            change = changes[m, head]
            if step == 0:
                low_ref[head, m] = beside(eye, jnp.zeros_like(eye)).astype(bf16)
                runs[head] = beside(last * eye - change[:, :LANES], change[:, LANES:])
            else:
                low = runs[head].astype(bf16)
                low_ref[head, m] = low
                run = last * runs[head] - dot(change[:, :LANES].astype(bf16), low)
                runs[head] = beside(run[:, :LANES], run[:, LANES:] + change[:, LANES:])
    for head in range(heads):
        x_ref[head] = runs[head].astype(bf16)


def block_reach_kernel(
    heads, blocks, both_ref, low_ref, act_e, cols_e, rows_e, act_l, cols_l, rows_l,
    qp_ref, o_ref,
):
    ri, ci = grid_index((CHUNK, CHUNK))
    upto = ri >= ci
    for head in range(heads):
        for m in range(blocks):
            at = slice(m * CHUNK, (m + 1) * CHUNK)
            final = m == blocks - 1
            cols = cols_l[0] if final else cols_e[m]
            rows = rows_l[0] if final else rows_e[m]
            q = act_l[head] if final else act_e[head, at]
            k = act_l[heads + head] if final else act_e[heads + head, at]
            decay = cols[:, head:head + 1]
            norm = cols[:, 2 * heads + head:2 * heads + head + 1]
            gap = decay - rows[head:head + 1]
            weight = jnp.exp(jnp.minimum(gap, 0.0)) * rows[heads + head:heads + head + 1]
            attend = jnp.where(upto, weight * dot(q, k, (1, 1)) * norm, 0.0).astype(bf16)
            inner = dot(attend, both_ref[head, m])
            eff = (jnp.exp(decay) * norm) * q.astype(f32) - inner[:, :LANES]
            ahead = dot(eff.astype(bf16), low_ref[head, m])
            qp_ref[head, at] = ahead[:, :LANES].astype(bf16)
            o_ref[head, at] = inner[:, LANES:] + ahead[:, LANES:]


def gate_kernel(count, *refs):
    w_ref = refs[count]
    outs = refs[count + 1:]
    tokens = jnp.concatenate([ref[...] for ref in refs[:count]], axis=0)
    gate = silu(dot(tokens, w_ref[...]))
    start = 0
    for out in outs:
        out[...] = gate[start:start + out.shape[0]]
        start += out.shape[0]


def pair_kernel(share, mine_ref, other_ref, out_ref):
    core = lax.axis_index("seq") & 1
    for j in range(out_ref.shape[0]):
        head = core * out_ref.shape[0] + j if share else j
        mine, other = mine_ref[head], other_ref[head]
        first = jnp.where(core == 0, mine, other)
        second = jnp.where(core == 0, other, mine)
        both = dot(second[:, :LANES], first)
        out_ref[j, :, :LANES] = both[:, :LANES].astype(bf16)
        out_ref[j, :, LANES:] = (both[:, LANES:] + second[:, LANES:].astype(f32)).astype(bf16)


def climb_kernel(bit, inside_ref, block_ref, sent_ref, inside_out, block_out):
    upper = (lax.axis_index("seq") >> (bit + 1)) & 1
    for j in range(block_ref.shape[0]):
        sent = sent_ref[j]
        for ref, out in ((inside_ref, inside_out), (block_ref, block_out)):
            mine = ref[j]
            both = dot(mine[:, :LANES], sent)
            left = jnp.where(upper == 1, both[:, :LANES], mine[:, :LANES].astype(f32))
            right = mine[:, LANES:].astype(f32) + both[:, LANES:]
            out[j] = jnp.concatenate([left, right], axis=1).astype(bf16)


def first_kernel(block_ref, sent_ref, inside_out, block_out):
    upper = (lax.axis_index("seq") >> 1) & 1
    ri, ci = grid_index((LANES, LANES))
    eye = jnp.where(ri == ci, 1.0, 0.0)
    for j in range(block_ref.shape[0]):
        sent, mine = sent_ref[j], block_ref[j]
        both = dot(mine[:, :LANES], sent)
        left = jnp.where(upper == 1, both[:, :LANES], mine[:, :LANES].astype(f32))
        right = mine[:, LANES:].astype(f32) + both[:, LANES:]
        block_out[j] = jnp.concatenate([left, right], axis=1).astype(bf16)
        inside = jnp.where(upper == 1, sent[:, :LANES].astype(f32), eye)
        inside_out[j] = jnp.concatenate([inside.astype(bf16), sent[:, LANES:]], axis=1)


def fold_kernel(inside_ref, *refs):
    out_ref = refs[-1]
    for j in range(out_ref.shape[0]):
        state = refs[0][j]
        for ref in refs[1:-1]:
            state = state + ref[j]
        inside = inside_ref[j]
        state = inside[:, LANES:].astype(f32) + dot(inside[:, :LANES], state)
        out_ref[j] = state.astype(bf16)


def final_kernel(
    share, blocks, ordered, qp_ref, o_ref, pair_ref, mine_ref, other_ref,
    own_gate_ref, gate_ref, late_gate_ref, gain_ref, out_ref,
):
    heads, seq_rows, dim = qp_ref.shape
    rows = seq_rows // blocks
    core, me = lax.axis_index("seq") & 1, lax.axis_index("tp")
    part = mine_ref.shape[0]
    for head in range(heads):
        start = mine_ref[head % part]
        if share:
            start = jnp.where(core == head // part, start, other_ref[head % part])
        pair = pair_ref[head]
        moved = pair[:, dim:].astype(f32) + dot(pair[:, :dim], start)
        start = jnp.where(core == 0, start.astype(f32), moved).astype(bf16)
        lanes = slice(head * dim, (head + 1) * dim)
        for m in range(blocks):
            if m == 0:
                gate = own_gate_ref[:, lanes]
            elif m < blocks - 1:
                gate = gate_ref[(m - 1) * rows:m * rows, lanes]
            else:
                gate = late_gate_ref[:, lanes]
            at = pl.ds(pl.multiple_of(lax.bitwise_xor(me, m) * rows, 8), rows)
            held = at if ordered else slice(m * rows, (m + 1) * rows)
            y = o_ref[head, held] + dot(qp_ref[head, held], start)
            scale = lax.rsqrt(jnp.mean(y * y, axis=-1, keepdims=True) + EPS)
            out_ref[at, lanes] = (y * scale * gain_ref[...] * gate).astype(bf16)


def call(kernel, out, operands, flops=0, scratch=(), limit=24):
    single = not isinstance(out, tuple)
    return pl.pallas_call(
        kernel,
        out_shape=out,
        in_specs=[whole()] * len(operands),
        out_specs=whole() if single else (whole(),) * len(out),
        scratch_shapes=scratch,
        cost_estimate=pl.CostEstimate(flops=flops, transcendentals=0, bytes_accessed=1 << 20),
        compiler_params=pltpu.CompilerParams(vmem_limit_bytes=limit << 20),
    )(*operands)


def per_device(hidden, w_qkv, w_gate, w_decay_beta, conv_weight, decay_rate, dt_bias, norm_gain):
    heads = decay_rate.shape[0]
    dim = norm_gain.shape[0]
    columns = heads * dim
    blocks = lax.axis_size("tp")
    seq_count = lax.axis_size("seq")
    rows = hidden.shape[0]
    seq_rows = rows * blocks
    chunks = seq_rows // CHUNK
    shape = jax.ShapeDtypeStruct

    w_three = w_qkv.transpose(1, 0, 2)
    small = w_decay_beta.transpose(1, 2, 0)
    taps = conv_weight.transpose(1, 0, 2)
    rate, bias = decay_rate.reshape(1, heads), dt_bias.reshape(1, heads)

    early, late = gather_blocks(hidden, "tp")
    weights = [w_three, w_gate, small]

    def project(tokens, count, extra=0):
        return call(
            functools.partial(project_kernel, len(tokens)),
            (
                shape((3, count + extra, columns), bf16),
                shape((count, columns), f32),
                shape((count, LANES), f32),
            ),
            [*tokens, *weights], flops=PROJECT_FLOPS, limit=20,
        )

    by_block = rows == CHUNK and len(early) == blocks - 2 and blocks % 2 == 0
    if by_block:
        parts, across = rim_rows(hidden, RIM)
        masks = call(
            masks_kernel,
            shape((CHUNK.bit_length() - 1, CHUNK, 2 * CHUNK), bf16), [],
            flops=MASKS_FLOPS, limit=4,
        )
        act_e, cols_e, rows_e, late_rim = call(
            functools.partial(early_kernel, heads, blocks),
            (
                shape((3 * heads, seq_rows - rows, dim), bf16),
                shape((blocks - 1, CHUNK, LANES), f32),
                shape((blocks - 1, CHUNK, LANES), f32),
                shape((3 * heads, RIM, dim), f32),
            ),
            [
                hidden, *early, across, *parts,
                w_three, small, taps, rate, bias,
            ],
            flops=PROJECT_FLOPS,
            scratch=[
                pltpu.VMEM((3 * heads, (blocks - 1) * (RIM + CHUNK), dim), f32),
                pltpu.VMEM((seq_rows - rows, LANES), f32),
                pltpu.VMEM((blocks + 1, 3 * heads, RIM, dim), f32),
            ],
        )
        own, both, low, act_l, cols_l, rows_l = call(
            functools.partial(block_delta_kernel, heads, blocks),
            (
                shape((heads, dim, 2 * dim), bf16),
                shape((heads, blocks, CHUNK, 2 * dim), bf16),
                shape((heads, blocks, dim, 2 * dim), bf16),
                shape((3 * heads, rows, dim), bf16),
                shape((1, CHUNK, LANES), f32),
                shape((1, CHUNK, LANES), f32),
            ),
            [act_e, cols_e, rows_e, late_rim, *late, w_three, small, taps, rate, bias, masks],
            flops=DELTA_FLOPS, limit=28,
            scratch=[
                pltpu.VMEM((3 * heads, RIM + CHUNK, dim), f32),
                pltpu.VMEM((heads * blocks // 2, CHUNK, 2 * CHUNK), bf16),
                pltpu.VMEM((heads * blocks // 2, CHUNK, 2 * CHUNK), f32),
                pltpu.VMEM((blocks, heads, dim, 2 * dim), f32),
                pltpu.VMEM((blocks, 8, LANES), f32),
            ],
        )
        reach, base = call(
            functools.partial(block_reach_kernel, heads, blocks),
            (
                shape((heads, seq_rows, dim), bf16),
                shape((heads, seq_rows, dim), f32),
            ),
            [both, low, act_e, cols_e, rows_e, act_l, cols_l, rows_l],
            flops=REACH_FLOPS, limit=14,
        )
        tokens = [hidden, *early, *late]
        own_gate, mid_gate, late_gate = call(
            functools.partial(gate_kernel, len(tokens)),
            (
                shape((rows, columns), f32),
                shape((seq_rows - 2 * rows, columns), f32),
                shape((rows, columns), f32),
            ),
            [*tokens, w_gate], flops=PROJECT_FLOPS, limit=14,
        )
    else:
        own_p, own_gate, own_sc = project([hidden], rows)
        parts, _ = rim_rows(hidden, RIM)
        rim = sum(parts[1:], parts[0])
        mid_p, mid_gate, mid_sc = project([*early, rim], seq_rows - 2 * rows, RIM)
        own, both, low, act, cols, rows_of = call(
            functools.partial(delta_kernel, heads, blocks),
            (
                shape((heads, dim, 2 * dim), bf16),
                shape((heads, chunks, CHUNK, 2 * dim), bf16),
                shape((heads, chunks - 1, dim, 2 * dim), bf16),
                shape((3 * heads, seq_rows, dim), bf16),
                shape((chunks, CHUNK, LANES), f32),
                shape((chunks, CHUNK, LANES), f32),
            ),
            [own_p, own_sc, mid_p, mid_sc, *late, w_three, small, taps, rate, bias],
            flops=DELTA_FLOPS, limit=32,
            scratch=[
                pltpu.VMEM((3 * heads, seq_rows + RIM, dim), f32),
                pltpu.VMEM((seq_rows, LANES), f32),
                pltpu.VMEM((CHUNK.bit_length() - 1, CHUNK, 2 * CHUNK), bf16),
                pltpu.VMEM((heads * chunks // 2, CHUNK, 2 * CHUNK), bf16),
                pltpu.VMEM((heads * chunks // 2, CHUNK, 2 * CHUNK), f32),
            ],
        )
        reach, base, late_gate = call(
            functools.partial(reach_kernel, heads),
            (
                shape((heads, seq_rows, dim), bf16),
                shape((heads, seq_rows, dim), f32),
                shape((rows, columns), f32),
            ),
            [both, low, act, cols, rows_of, *late, w_gate], flops=REACH_FLOPS, limit=12,
        )

    share = heads % 2 == 0
    part = heads // 2 if share else heads
    swap = [(i, i ^ 1) for i in range(seq_count)]
    other = lax.ppermute(own, "seq", swap)
    block = call(
        functools.partial(pair_kernel, share),
        shape((part, dim, 2 * dim), bf16), [own, other], flops=SMALL_FLOPS, limit=4,
    )
    chips = seq_count // 2
    levels = chips.bit_length() - 1
    inside = None
    for level in range(levels):
        size = 1 << level
        sent = block if level < levels - 1 or level == 0 else block[:, :, dim:]
        parts = []
        for target in range(size):
            route = []
            for top in range(size - 1, chips, 2 * size):
                for c in range(2):
                    route.append((2 * top + c, 2 * (top + 1 + target) + c))
            parts.append(lax.ppermute(sent, "seq", route))
        if level == levels - 1 and level > 0:
            break
        sent = sum(parts[1:], parts[0])
        kernel, operands = first_kernel, [block, sent]
        if level > 0:
            kernel, operands = functools.partial(climb_kernel, level), [inside, block, sent]
        inside, block = call(
            kernel, (shape(block.shape, bf16),) * 2, operands, flops=SMALL_FLOPS, limit=4,
        )
    state = call(
        fold_kernel, shape((part, dim, dim), bf16), [inside, *parts],
        flops=SMALL_FLOPS, limit=4,
    )
    back = lax.ppermute(state, "seq", swap) if share else state
    return call(
        functools.partial(final_kernel, share, blocks, not by_block), shape((seq_rows, columns), bf16),
        [reach, base, other, state, back, own_gate, mid_gate, late_gate, norm_gain.reshape(1, dim)],
        flops=SMALL_FLOPS, limit=12,
    )


def solution(mesh):
    return jax.shard_map(
        per_device,
        mesh=mesh,
        in_specs=(
            P(("seq", "tp"), None),
            P(None, None, "tp"),
            P(None, "tp"),
            P(None, None, "tp"),
            P(None, None, "tp"),
            P("tp"),
            P("tp"),
            P(),
        ),
        out_specs=P("seq", "tp"),
        check_vma=False,
    )
```
